8 devices in a mesh: data: 1 (over z), ffn: 2 (over y), hid: 4 (over x, core).
Axes of the slice: x: 2, y: 2, z: 1, core: 2. Of those that a mesh axis runs over, the one named last changes fastest.
Arguments:
- x_in: bfloat16 [64, 4096], P('data', 'hid')
- gain_one: float32 [4096], P('hid')
- gain_two: float32 [4096], P('hid')
- w_gate: bfloat16 [4096, 14336], P('hid', 'ffn')
- w_up: bfloat16 [4096, 14336], P('hid', 'ffn')
- w_down: bfloat16 [14336, 4096], P('ffn', 'hid')
- w_qkv: bfloat16 [4096, 6144], P('hid', 'ffn')
- dx_out: bfloat16 [64, 4096], P('data', 'hid')
- d_qkv: bfloat16 [64, 6144], P('data', 'ffn')
Outputs:
- output 1: bfloat16 [64, 4096], P('data', 'hid')
- output 2: bfloat16 [4096, 14336], P(('data', 'hid'), 'ffn')
- output 3: bfloat16 [4096, 14336], P(('data', 'hid'), 'ffn')
- output 4: bfloat16 [14336, 4096], P(('data', 'ffn'), 'hid')
- output 5: bfloat16 [4096, 6144], P(('data', 'hid'), 'ffn')
- output 6: float32 [4096], P(('data', 'hid'))
- output 7: float32 [4096], P(('data', 'hid'))
All inputs are finite; a program needn't handle non-finite values.
Results may differ from the reference program's by a relative error of at most 0.00512244.
Values are sent between devices in bfloat16 or wider.
A program may use at most 1 GiB of HBM per device.

```python
import jax
import jax.numpy as jnp
from jax import lax

D_MODEL = 4096
D_FF = 14336
Q_HEADS = 32
KV_HEADS = 8
HEAD_DIM = 128
TOKENS = 64
QKV_WIDTH = (Q_HEADS + 2 * KV_HEADS) * HEAD_DIM
NORM_EPS = 1e-6


def norm_forward(z_val, gain_vec):
    inv_rms = lax.rsqrt(jnp.sum(z_val * z_val, axis=-1, keepdims=True) / D_MODEL + NORM_EPS)
    return inv_rms, (z_val * inv_rms * gain_vec).astype(jnp.bfloat16)


def norm_backward(z_val, gain_vec, inv_rms, d_norm):
    g_dn = gain_vec * d_norm
    dot_tok = jnp.sum(g_dn * z_val, axis=-1, keepdims=True)
    d_input = inv_rms * g_dn - z_val * (inv_rms ** 3) * (dot_tok / D_MODEL)
    d_gain = jnp.sum(d_norm * z_val * inv_rms, axis=0)
    return d_input, d_gain


def forward_states(x_in, gain_one, gain_two, w_gate, w_up, w_down):
    x_f32 = x_in.astype(jnp.float32)
    inv_one, normed_one = norm_forward(x_f32, gain_one)
    gate_pre = jnp.dot(normed_one, w_gate, preferred_element_type=jnp.float32)
    up_pre = jnp.dot(normed_one, w_up, preferred_element_type=jnp.float32)
    act_bf = (jax.nn.silu(gate_pre) * up_pre).astype(jnp.bfloat16)
    down_out = jnp.dot(act_bf, w_down, preferred_element_type=jnp.float32)
    resid_f32 = (x_f32 + down_out).astype(jnp.bfloat16).astype(jnp.float32)
    inv_two, normed_two = norm_forward(resid_f32, gain_two)
    return x_f32, inv_one, normed_one, gate_pre, up_pre, act_bf, resid_f32, inv_two, normed_two


def setup_inputs(seed: int = 0, part: int = 0) -> dict:
    shared_keys = jax.random.split(jax.random.key(seed), 6)
    part_keys = jax.random.split(jax.random.fold_in(jax.random.key(seed + 1), part), 6)
    positions = jnp.arange(D_MODEL, dtype=jnp.float32) / D_MODEL
    row_scale = jnp.exp(jax.random.uniform(part_keys[0], (TOKENS, 1), minval=-1.0, maxval=1.0))
    amplitude = jax.random.uniform(part_keys[1], (TOKENS, 1), minval=0.6, maxval=1.2)
    phase_off = jax.random.uniform(part_keys[2], (TOKENS, 1))
    profile = jnp.exp(amplitude * jnp.sin(2.0 * jnp.pi * (positions + phase_off)))
    x_in = (jax.random.normal(part_keys[3], (TOKENS, D_MODEL)) * row_scale * profile).astype(jnp.bfloat16)
    gain_one = jax.random.uniform(shared_keys[0], (D_MODEL,), minval=0.5, maxval=1.5)
    gain_two = jax.random.uniform(shared_keys[1], (D_MODEL,), minval=0.5, maxval=1.5)
    w_gate = (jax.random.normal(shared_keys[2], (D_MODEL, D_FF)) * D_MODEL ** -0.5).astype(jnp.bfloat16)
    w_up = (jax.random.normal(shared_keys[3], (D_MODEL, D_FF)) * D_MODEL ** -0.5).astype(jnp.bfloat16)
    w_down = (jax.random.normal(shared_keys[4], (D_FF, D_MODEL)) * D_FF ** -0.5).astype(jnp.bfloat16)
    w_qkv = (jax.random.normal(shared_keys[5], (D_MODEL, QKV_WIDTH)) * D_MODEL ** -0.5).astype(jnp.bfloat16)
    states = forward_states(x_in, gain_one, gain_two, w_gate, w_up, w_down)
    qkv_est = jnp.dot(states[8], w_qkv, preferred_element_type=jnp.float32)
    d_qkv = (qkv_est + 0.5 * jax.random.normal(part_keys[4], (TOKENS, QKV_WIDTH))).astype(jnp.bfloat16)
    dx_out = (3.0 * (states[6] - states[0]) + 0.5 * jax.random.normal(part_keys[5], (TOKENS, D_MODEL))).astype(jnp.bfloat16)
    return {"x_in": x_in, "gain_one": gain_one, "gain_two": gain_two, "w_gate": w_gate, "w_up": w_up, "w_down": w_down, "w_qkv": w_qkv, "dx_out": dx_out, "d_qkv": d_qkv}


def reference(x_in, gain_one, gain_two, w_gate, w_up, w_down, w_qkv, dx_out, d_qkv):
    x_f32, inv_one, normed_one, gate_pre, up_pre, act_bf, resid_f32, inv_two, normed_two = forward_states(x_in, gain_one, gain_two, w_gate, w_up, w_down)
    dw_qkv = jnp.dot(normed_two.T, d_qkv, preferred_element_type=jnp.float32).astype(jnp.bfloat16)
    d_normed_two = jnp.dot(d_qkv, w_qkv.T, preferred_element_type=jnp.float32)
    d_resid, d_gain_two = norm_backward(resid_f32, gain_two, inv_two, d_normed_two)
    d_res_tot = dx_out.astype(jnp.float32) + d_resid
    d_res_bf = d_res_tot.astype(jnp.bfloat16)
    dw_down = jnp.dot(act_bf.T, d_res_bf, preferred_element_type=jnp.float32).astype(jnp.bfloat16)
    d_act = jnp.dot(d_res_bf, w_down.T, preferred_element_type=jnp.float32)
    gate_sig = jax.nn.sigmoid(gate_pre)
    d_gate = (d_act * up_pre * gate_sig * (1.0 + gate_pre * (1.0 - gate_sig))).astype(jnp.bfloat16)
    d_up = (d_act * jax.nn.silu(gate_pre)).astype(jnp.bfloat16)
    dw_gate = jnp.dot(normed_one.T, d_gate, preferred_element_type=jnp.float32).astype(jnp.bfloat16)
    dw_up = jnp.dot(normed_one.T, d_up, preferred_element_type=jnp.float32).astype(jnp.bfloat16)
    d_normed_one = jnp.dot(d_gate, w_gate.T, preferred_element_type=jnp.float32) + jnp.dot(d_up, w_up.T, preferred_element_type=jnp.float32)
    d_in, d_gain_one = norm_backward(x_f32, gain_one, inv_one, d_normed_one)
    dx_in = (d_res_tot + d_in).astype(jnp.bfloat16)
    return (dx_in, dw_gate, dw_up, dw_down, dw_qkv, d_gain_one, d_gain_two)
```

```python
import functools

import jax
import jax.numpy as jnp
from jax import lax
from jax.experimental import pallas as pl
from jax.experimental.pallas import tpu as pltpu
from jax.sharding import PartitionSpec as P

NORM_EPS = 1e-6
BF = jnp.bfloat16
F32 = jnp.float32
MESH_ID = pl.DeviceIdType.MESH
ANY = pl.BlockSpec(memory_space=pl.ANY)
VMEM_LIMIT = 67043328

CHUNK = 1024
LAG_PAIR = 1
LAG_ACT = 2
LAG_FWD = 3
LAG_DOT = 4

PAIR, XRED, GX, GP, FW = range(5)


def nn_dot(a_mat, b_mat):
    return jnp.dot(a_mat, b_mat, preferred_element_type=F32)


def nt_dot(a_mat, b_mat):
    return lax.dot_general(a_mat, b_mat, (((1,), (1,)), ((), ())), preferred_element_type=F32)


def pack_stats(cols):
    tok = cols[0].shape[0]
    lane = lax.broadcasted_iota(jnp.int32, (tok, 128), 1)
    wide = jnp.zeros((tok, 128), F32)
    for i, col in enumerate(cols):
        wide = jnp.where(lane == i, col, wide)
    full = jnp.concatenate([wide, jnp.zeros((128 - tok, 128), F32)], axis=0)
    return full.T[0:8, :]


def unpack_stats(tile, tok, count):
    full = jnp.concatenate([tile, jnp.zeros((120, 128), F32)], axis=0).T
    return [full[0:tok, i : i + 1] for i in range(count)]


def comm_kernel(
    dims,
    x_h, g1_h, g2_h, wg_h, wu_h, wd_h, wq_h, dx_h, dq_h,
    n1_o, n2_o, eb_o, a_o, dgu_o, dxin_o, dg1_o, dg2_o,
    wg, wu, wd, wq, dq, x_s, dx_s, g1, g2, n1, n2, eb, e_s, x2_s,
    acc, part, r1, r2, xs, xr, xs2, xr2, gu, a_f, dgu_f, ys, yr, st_s, st_r, dxin_s, dg_s,
    ld, wld, out_sem, st_sem, y_sem, sems,
):
    tok, hd, ff, qw = dims
    c_w = CHUNK
    nc = ff // c_w
    half = c_w // 2
    quart = c_w // 4
    d_model = hd * 4
    zc, yc, h = lax.axis_index("data"), lax.axis_index("ffn"), lax.axis_index("hid")
    xc = h // 2
    core = lax.rem(h, 2)
    pair = (zc, yc, xc * 2 + 1 - core)
    xnb = (zc, yc, (1 - xc) * 2 + core)
    ynb = (zc, 1 - yc, h)

    def load(src, dst, sem):
        return pltpu.make_async_copy(src, dst, sem)

    small = [
        load(x_h, x_s, ld.at[0]), load(g1_h, g1, ld.at[1]), load(dq_h, dq, ld.at[2]),
        load(g2_h, g2, ld.at[3]), load(dx_h, dx_s, ld.at[4]),
    ]
    qn = qw // 1024

    def wq_load(i):
        cols = pl.ds(pl.multiple_of(i * 1024, 1024), 1024)
        return load(wq_h.at[:, cols], wq.at[:, cols], wld.at[3, i])

    def w_load(i, c):
        cols = pl.ds(pl.multiple_of(c * c_w, c_w), c_w)
        if i == 2:
            return load(wd_h.at[cols, :], wd.at[cols, :], wld.at[2, c])
        src, dst = ((wg_h, wg), (wu_h, wu))[i]
        return load(src.at[:, cols], dst.at[:, cols], wld.at[i, c])

    for cp in small:
        cp.start()
    for i in range(qn):
        wq_load(i).start()
    for c in range(nc):
        w_load(0, c).start()
        w_load(1, c).start()
    for c in range(nc):
        w_load(2, c).start()

    bar = pltpu.get_barrier_semaphore()
    for j in (1, 2, 3):
        pl.semaphore_signal(bar, inc=1, device_id=(zc, yc, lax.rem(h + j, 4)), device_id_type=MESH_ID)
    pl.semaphore_signal(bar, inc=1, device_id=ynb, device_id_type=MESH_ID)
    pl.semaphore_wait(bar, 4)

    def stat_copy(n, j):
        return pltpu.make_async_remote_copy(
            src_ref=st_s.at[n], dst_ref=st_r.at[n, h], send_sem=st_sem.at[n, 0, j], recv_sem=st_sem.at[n, 1, j],
            device_id=(zc, yc, lax.rem(h + j, 4)), device_id_type=MESH_ID,
        )

    def stat_send(n, cols):
        tile = pack_stats(cols)
        st_s[n] = tile
        st_r[n, h] = tile
        for j in (1, 2, 3):
            stat_copy(n, j).start()

    def stat_recv(n, count):
        for j in (1, 2, 3):
            stat_copy(n, j).wait()
        return unpack_stats(st_r[n, 0] + st_r[n, 1] + st_r[n, 2] + st_r[n, 3], tok, count)

    def y_copy(n):
        return pltpu.make_async_remote_copy(
            src_ref=ys.at[n], dst_ref=yr.at[n], send_sem=y_sem.at[n, 0], recv_sem=y_sem.at[n, 1],
            device_id=ynb, device_id_type=MESH_ID,
        )

    def y_sum(n):
        y_copy(n).wait()
        return ys[n].astype(F32) + yr[n].astype(F32)

    small[0].wait()
    x_f = x_s[...].astype(F32)
    stat_send(0, [jnp.sum(x_f * x_f, axis=-1, keepdims=True)])
    small[2].wait()
    acc[...] = jnp.zeros_like(acc)

    def qkv_step(i, carry):
        wq_load(i).wait()
        cols = pl.ds(pl.multiple_of(i * 1024, 1024), 1024)
        acc[...] += nt_dot(dq[:, cols], wq[:, cols])
        return carry

    lax.fori_loop(0, qn, qkv_step, 0)
    ys[0] = acc[...].astype(BF)
    y_copy(0).start()
    small[1].wait()
    (sq,) = stat_recv(0, 1)
    inv1 = lax.rsqrt(sq / d_model + NORM_EPS)
    n1[...] = (x_s[...].astype(F32) * inv1 * g1[...]).astype(BF)
    n1_out = load(n1, n1_o, out_sem.at[0])
    n1_out.start()
    acc[...] = jnp.zeros_like(acc)

    def pair_copy(ph, c):
        slot = lax.rem(c, 2)
        src = part.at[slot, 1 - core] if ph == 0 else part.at[slot, 1 - core, 0]
        return pltpu.make_async_remote_copy(
            src_ref=src, dst_ref=(r1 if ph == 0 else r2).at[c],
            send_sem=sems.at[ph, 2 * PAIR, c], recv_sem=sems.at[ph, 2 * PAIR + 1, c],
            device_id=pair, device_id_type=MESH_ID,
        )

    def x_copy(ph, c):
        src, dst = ((xs, xr), (xs2, xr2))[ph]
        return pltpu.make_async_remote_copy(
            src_ref=src.at[c], dst_ref=dst.at[c],
            send_sem=sems.at[ph, 2 * XRED, c], recv_sem=sems.at[ph, 2 * XRED + 1, c],
            device_id=xnb, device_id_type=MESH_ID,
        )

    own_q = core * 2 + xc
    xnb_q = core * 2 + 1 - xc

    def block(ph, c, q):
        cols = pl.ds(pl.multiple_of(c * c_w + q * quart, quart), quart)
        return a_f.at[:, cols] if ph == 0 else dgu_f.at[:, :, cols]

    def g_copy(ph, c, kind):
        ref = block(ph, c, xnb_q if kind == FW else own_q)
        return pltpu.make_async_remote_copy(
            src_ref=ref, dst_ref=ref,
            send_sem=sems.at[ph, 2 * kind, c], recv_sem=sems.at[ph, 2 * kind + 1, c],
            device_id=xnb if kind == GX else pair, device_id_type=MESH_ID,
        )

    own_cols = pl.ds(pl.multiple_of(xc * quart, quart), quart)
    oth_cols = pl.ds(pl.multiple_of((1 - xc) * quart, quart), quart)

    def pipeline(ph, partial, activate, consume):
        def step(t, carry):
            @pl.when(t < nc)
            def _():
                c = t

                @pl.when(c >= 2)
                def _():
                    pair_copy(ph, c - 2).wait_send()

                partial(c, 1 - core)
                pair_copy(ph, c).start()
                partial(c, core)

            @pl.when((t >= LAG_PAIR) & (t < nc + LAG_PAIR))
            def _():
                c = t - LAG_PAIR
                slot = lax.rem(c, 2)
                pair_copy(ph, c).wait_recv()
                if ph == 0:
                    xs[c] = (part[slot, core, :, :, oth_cols] + r1[c, :, :, oth_cols]).astype(BF)
                    x_copy(ph, c).start()
                    gu[c] = part[slot, core, :, :, own_cols] + r1[c, :, :, own_cols]
                else:
                    xs2[c] = (part[slot, core, 0, :, oth_cols] + r2[c, :, oth_cols]).astype(BF)
                    x_copy(ph, c).start()
                    r2[c, :, own_cols] = part[slot, core, 0, :, own_cols] + r2[c, :, own_cols]

            @pl.when((t >= LAG_ACT) & (t < nc + LAG_ACT))
            def _():
                c = t - LAG_ACT
                x_copy(ph, c).wait_recv()
                activate(c)
                g_copy(ph, c, GX).start()
                g_copy(ph, c, GP).start()

            @pl.when((t >= LAG_FWD) & (t < nc + LAG_FWD))
            def _():
                c = t - LAG_FWD
                g_copy(ph, c, GX).wait_recv()
                g_copy(ph, c, FW).start()

            @pl.when((t >= LAG_DOT) & (t < nc + LAG_DOT))
            def _():
                c = t - LAG_DOT
                g_copy(ph, c, GP).wait_recv()
                g_copy(ph, c, FW).wait_recv()
                consume(c)
                x_copy(ph, c).wait_send()
                g_copy(ph, c, GX).wait_send()
                g_copy(ph, c, GP).wait_send()
                g_copy(ph, c, FW).wait_send()

            return carry

        lax.fori_loop(0, nc + LAG_DOT, step, 0)
        pair_copy(ph, nc - 2).wait_send()
        pair_copy(ph, nc - 1).wait_send()

    def gu_partial(c, which):
        @pl.when(which != core)
        def _():
            w_load(0, c).wait()
            w_load(1, c).wait()

        cols = pl.ds(pl.multiple_of(c * c_w + which * half, half), half)
        slot = lax.rem(c, 2)
        part[slot, which, 0] = nn_dot(n1[...], wg[:, cols])
        part[slot, which, 1] = nn_dot(n1[...], wu[:, cols])

    def act_forward(c):
        gate = gu[c, 0] + xr[c, 0].astype(F32)
        up = gu[c, 1] + xr[c, 1].astype(F32)
        gu[c, 0] = gate
        gu[c, 1] = up
        cols = pl.ds(pl.multiple_of(c * c_w + own_q * quart, quart), quart)
        a_f[:, cols] = (jax.nn.silu(gate) * up).astype(BF)

    def down_dot(c):
        w_load(2, c).wait()
        rows = pl.ds(pl.multiple_of(c * c_w, c_w), c_w)
        acc[...] += nn_dot(a_f[:, rows], wd[rows, :])

    pipeline(0, gu_partial, act_forward, down_dot)
    ys[1] = acc[...].astype(BF)
    y_copy(1).start()
    a_out = load(a_f, a_o, out_sem.at[1])
    a_out.start()

    small[3].wait()
    small[4].wait()
    dn2 = y_sum(0)
    acc[...] = dn2
    x2_s[...] = (x_s[...].astype(F32) + y_sum(1)).astype(BF)
    x2 = x2_s[...].astype(F32)
    stat_send(1, [
        jnp.sum(x2 * x2, axis=-1, keepdims=True),
        jnp.sum(g2[...] * acc[...] * x2, axis=-1, keepdims=True),
    ])
    sq2, dot2 = stat_recv(1, 2)
    inv2 = lax.rsqrt(sq2 / d_model + NORM_EPS)
    x2 = x2_s[...].astype(F32)
    dz2 = inv2 * (g2[...] * acc[...]) - x2 * (inv2 * inv2 * inv2) * (dot2 / d_model)
    e_val = dx_s[...].astype(F32) + dz2
    e_s[...] = e_val
    eb[...] = e_val.astype(BF)
    n2[...] = (x2_s[...].astype(F32) * inv2 * g2[...]).astype(BF)
    dg_s[0:1, :] = jnp.sum(acc[...] * x2_s[...].astype(F32) * inv2, axis=0, keepdims=True)
    outs = [load(eb, eb_o, out_sem.at[2]), load(n2, n2_o, out_sem.at[3])]
    for cp in outs:
        cp.start()
    acc[...] = jnp.zeros_like(acc)

    def da_partial(c, which):
        rows = pl.ds(pl.multiple_of(c * c_w + which * half, half), half)
        part[lax.rem(c, 2), which, 0] = nt_dot(eb[...], wd[rows, :])

    def act_backward(c):
        d_act = r2[c, :, own_cols] + xr2[c].astype(F32)
        gate, up = gu[c, 0], gu[c, 1]
        sig = jax.nn.sigmoid(gate)
        cols = pl.ds(pl.multiple_of(c * c_w + own_q * quart, quart), quart)
        dgu_f[0, :, cols] = (d_act * up * sig * (1.0 + gate * (1.0 - sig))).astype(BF)
        dgu_f[1, :, cols] = (d_act * (gate * sig)).astype(BF)

    def dn1_dot(c):
        cols = pl.ds(pl.multiple_of(c * c_w, c_w), c_w)
        acc[...] += nt_dot(dgu_f[0, :, cols], wg[:, cols]) + nt_dot(dgu_f[1, :, cols], wu[:, cols])

    pipeline(1, da_partial, act_backward, dn1_dot)
    dgu_out = load(dgu_f, dgu_o, out_sem.at[4])
    dgu_out.start()
    ys[2] = acc[...].astype(BF)
    y_copy(2).start()

    acc[...] = y_sum(2)
    stat_send(2, [jnp.sum(g1[...] * acc[...] * x_s[...].astype(F32), axis=-1, keepdims=True)])
    dg_s[1:2, :] = jnp.sum(acc[...] * x_s[...].astype(F32) * inv1, axis=0, keepdims=True)
    (dot1,) = stat_recv(2, 1)
    dz1 = inv1 * (g1[...] * acc[...]) - x_s[...].astype(F32) * (inv1 * inv1 * inv1) * (dot1 / d_model)
    dxin_s[...] = (e_s[...] + dz1).astype(BF)
    tail = [
        load(dxin_s, dxin_o, out_sem.at[5]),
        load(dg_s.at[0:1, :], dg2_o, out_sem.at[6]),
        load(dg_s.at[1:2, :], dg1_o, out_sem.at[7]),
    ]
    for cp in tail:
        cp.start()
    for cp in (n1_out, a_out, *outs, dgu_out, *tail):
        cp.wait()


def comm_call(x_in, gain_one, gain_two, w_gate, w_up, w_down, w_qkv, dx_out, d_qkv):
    tok, hd = x_in.shape
    ff = w_gate.shape[1]
    qw = w_qkv.shape[1]
    nc = ff // CHUNK
    half, quart = CHUNK // 2, CHUNK // 4
    out = lambda shape, dtype: jax.ShapeDtypeStruct(shape, dtype)
    vm = lambda *shape_dtype: pltpu.VMEM(shape_dtype[:-1], shape_dtype[-1])
    dma = pltpu.SemaphoreType.DMA
    return pl.pallas_call(
        functools.partial(comm_kernel, (tok, hd, ff, qw)),
        out_shape=(
            out((tok, hd), BF), out((tok, hd), BF), out((tok, hd), BF), out((tok, ff), BF), out((2, tok, ff), BF),
            out((tok, hd), BF), out((1, hd), F32), out((1, hd), F32),
        ),
        in_specs=[ANY] * 9,
        out_specs=[ANY] * 8,
        scratch_shapes=[
            vm(hd, ff, BF), vm(hd, ff, BF), vm(ff, hd, BF), vm(hd, qw, BF), vm(tok, qw, BF),
            vm(tok, hd, BF), vm(tok, hd, BF), vm(1, hd, F32), vm(1, hd, F32),
            vm(tok, hd, BF), vm(tok, hd, BF), vm(tok, hd, BF), vm(tok, hd, F32), vm(tok, hd, BF),
            vm(tok, hd, F32), vm(2, 2, 2, tok, half, F32), vm(nc, 2, tok, half, F32), vm(nc, tok, half, F32),
            vm(nc, 2, tok, quart, BF), vm(nc, 2, tok, quart, BF), vm(nc, tok, quart, BF), vm(nc, tok, quart, BF),
            vm(nc, 2, tok, quart, F32), vm(tok, ff, BF), vm(2, tok, ff, BF),
            vm(3, tok, hd, BF), vm(3, tok, hd, BF), vm(3, 8, 128, F32), vm(3, 4, 8, 128, F32),
            vm(tok, hd, BF), vm(8, hd, F32),
            dma((5,)), dma((4, nc)), dma((8,)), dma((3, 2, 4)), dma((3, 2)), dma((2, 10, nc)),
        ],
        compiler_params=pltpu.CompilerParams(
            collective_id=0, has_side_effects=True, vmem_limit_bytes=VMEM_LIMIT
        ),
        name="block_comm",
    )(x_in, gain_one, gain_two, w_gate, w_up, w_down, w_qkv, dx_out, d_qkv)


TILE = 512
SLOTS = 3


def grad_kernel(dims, n1, n2, eb, a_f, dgu, dq, dwg_o, dwu_o, dwd_o, dwq_o, n1_t, n2_t, bg, bu, bd, sem):
    hd, ff, qw = dims
    nt, nq = ff // TILE, qw // TILE
    n1_t[...] = n1[...].astype(F32).T.astype(BF)
    n2_t[...] = n2[...].astype(F32).T.astype(BF)

    def cols_of(i):
        return pl.ds(pl.multiple_of(i * TILE, TILE), TILE)

    def q_copy(i):
        slot = lax.rem(i, SLOTS)
        return pltpu.make_async_copy(bg.at[slot], dwq_o.at[:, cols_of(i)], sem.at[0, slot])

    def g_copy(i):
        slot = lax.rem(i, SLOTS)
        return pltpu.make_async_copy(bg.at[slot], dwg_o.at[:, cols_of(i)], sem.at[0, slot])

    def u_copy(i):
        slot = lax.rem(i, SLOTS)
        return pltpu.make_async_copy(bu.at[slot], dwu_o.at[:, cols_of(i)], sem.at[1, slot])

    def d_copy(i):
        slot = lax.rem(i, SLOTS)
        return pltpu.make_async_copy(bd.at[slot], dwd_o.at[cols_of(i), :], sem.at[2, slot])

    def q_step(i, carry):
        @pl.when(i >= SLOTS)
        def _():
            q_copy(i - SLOTS).wait()

        bg[lax.rem(i, SLOTS)] = nn_dot(n2_t[...], dq[:, cols_of(i)]).astype(BF)
        q_copy(i).start()
        return carry

    lax.fori_loop(0, nq, q_step, 0)
    for i in range(nq - SLOTS, nq):
        q_copy(i).wait()

    def step(i, carry):
        slot = lax.rem(i, SLOTS)

        @pl.when(i >= SLOTS)
        def _():
            g_copy(i - SLOTS).wait()
            u_copy(i - SLOTS).wait()
            d_copy(i - SLOTS).wait()

        bd[slot] = nn_dot(a_f[:, cols_of(i)].astype(F32).T.astype(BF), eb[...]).astype(BF)
        d_copy(i).start()
        bg[slot] = nn_dot(n1_t[...], dgu[0, :, cols_of(i)]).astype(BF)
        g_copy(i).start()
        bu[slot] = nn_dot(n1_t[...], dgu[1, :, cols_of(i)]).astype(BF)
        u_copy(i).start()
        return carry

    lax.fori_loop(0, nt, step, 0)
    for i in range(nt - SLOTS, nt):
        g_copy(i).wait()
        u_copy(i).wait()
        d_copy(i).wait()


def grad_call(n1, n2, eb, a_full, dgu, d_qkv):
    tok, hd = n1.shape
    ff, qw = a_full.shape[1], d_qkv.shape[1]
    out = lambda *shape: jax.ShapeDtypeStruct(shape, BF)
    return pl.pallas_call(
        functools.partial(grad_kernel, (hd, ff, qw)),
        out_shape=(out(hd, ff), out(hd, ff), out(ff, hd), out(hd, qw)),
        in_specs=[pl.BlockSpec(memory_space=pltpu.VMEM)] * 6,
        out_specs=[ANY] * 4,
        scratch_shapes=[
            pltpu.VMEM((hd, tok), BF), pltpu.VMEM((hd, tok), BF),
            pltpu.VMEM((SLOTS, hd, TILE), BF), pltpu.VMEM((SLOTS, hd, TILE), BF), pltpu.VMEM((SLOTS, TILE, hd), BF),
            pltpu.SemaphoreType.DMA((3, SLOTS)),
        ],
        compiler_params=pltpu.CompilerParams(vmem_limit_bytes=VMEM_LIMIT),
        name="weight_grads",
    )(n1, n2, eb, a_full, dgu, d_qkv)


def solution(mesh):
    def local_step(x_in, gain_one, gain_two, w_gate, w_up, w_down, w_qkv, dx_out, d_qkv):
        hd = x_in.shape[1]
        n1, n2, eb, a_full, dgu, dx_in, dg1, dg2 = comm_call(
            x_in, gain_one.reshape(1, hd), gain_two.reshape(1, hd), w_gate, w_up, w_down, w_qkv, dx_out, d_qkv
        )
        dw_gate, dw_up, dw_down, dw_qkv = grad_call(n1, n2, eb, a_full, dgu, d_qkv)
        return dx_in, dw_gate, dw_up, dw_down, dw_qkv, dg1.reshape(hd), dg2.reshape(hd)

    tok_spec = P("data", "hid")
    in_specs = (tok_spec, P("hid"), P("hid"), P("hid", "ffn"), P("hid", "ffn"), P("ffn", "hid"), P("hid", "ffn"), tok_spec, P("data", "ffn"))
    out_specs = (tok_spec, P(("data", "hid"), "ffn"), P(("data", "hid"), "ffn"), P(("data", "ffn"), "hid"), P(("data", "hid"), "ffn"), P(("data", "hid")), P(("data", "hid")))
    return jax.shard_map(local_step, mesh=mesh, in_specs=in_specs, out_specs=out_specs, check_vma=False)
```

```python
import functools

import jax
import jax.numpy as jnp
from jax import lax
from jax.experimental import pallas as pl
from jax.experimental.pallas import tpu as pltpu
from jax.sharding import PartitionSpec as P

NORM_EPS = 1e-6
BF = jnp.bfloat16
F32 = jnp.float32
MESH_ID = pl.DeviceIdType.MESH
ANY = pl.BlockSpec(memory_space=pl.ANY)
VMEM_LIMIT = 67043328

CHUNK = 1024
LAGS = ((1, 3, 5, 6), (1, 3, 5, 6))

PAIR, XRED, GX, GP, FW = range(5)


def nn_dot(a_mat, b_mat):
    return jnp.dot(a_mat, b_mat, preferred_element_type=F32)


def nt_dot(a_mat, b_mat):
    return lax.dot_general(a_mat, b_mat, (((1,), (1,)), ((), ())), preferred_element_type=F32)


def pack_stats(cols):
    tok = cols[0].shape[0]
    lane = lax.broadcasted_iota(jnp.int32, (tok, 128), 1)
    wide = jnp.zeros((tok, 128), F32)
    for i, col in enumerate(cols):
        wide = jnp.where(lane == i, col, wide)
    full = jnp.concatenate([wide, jnp.zeros((128 - tok, 128), F32)], axis=0)
    return full.T[0:8, :]


def unpack_stats(tile, tok, count):
    full = jnp.concatenate([tile, jnp.zeros((120, 128), F32)], axis=0).T
    return [full[0:tok, i : i + 1] for i in range(count)]


def comm_kernel(
    dims,
    x_h, g1_h, g2_h, wg_h, wu_h, wd_h, wq_h, dx_h, dq_h,
    n1_o, n2_o, eb_o, a_o, dgu_o, dxin_o, dg1_o, dg2_o,
    wg, wu, wd, wq, dq, x_s, dx_s, g1, g2, n1, n2, eb, e_s, x2_s,
    acc, part, r1, r2, xs, xr, xs2, xr2, gu, a_f, dgu_f, y32, ys, yr, st_s, st_r, dxin_s, dg_s,
    ld, wld, out_sem, st_sem, y_sem, sems,
):
    tok, hd, ff, qw = dims
    c_w = CHUNK
    nc = ff // c_w
    half = c_w // 2
    quart = c_w // 4
    d_model = hd * 4
    zc, yc, h = lax.axis_index("data"), lax.axis_index("ffn"), lax.axis_index("hid")
    xc = h // 2
    core = lax.rem(h, 2)
    pair = (zc, yc, xc * 2 + 1 - core)
    xnb = (zc, yc, (1 - xc) * 2 + core)
    ynb = (zc, 1 - yc, h)

    def load(src, dst, sem):
        return pltpu.make_async_copy(src, dst, sem)

    small = [
        load(x_h, x_s, ld.at[0]), load(g1_h, g1, ld.at[1]), load(dq_h, dq, ld.at[2]),
        load(g2_h, g2, ld.at[3]), load(dx_h, dx_s, ld.at[4]),
    ]
    qn = qw // 1024

    def wq_load(i):
        cols = pl.ds(pl.multiple_of(i * 1024, 1024), 1024)
        return load(wq_h.at[:, cols], wq.at[:, cols], wld.at[3, i])

    def w_load(i, c):
        cols = pl.ds(pl.multiple_of(c * c_w, c_w), c_w)
        if i == 2:
            return load(wd_h.at[cols, :], wd.at[cols, :], wld.at[2, c])
        src, dst = ((wg_h, wg), (wu_h, wu))[i]
        return load(src.at[:, cols], dst.at[:, cols], wld.at[i, c])

    def gu_load_start(c):
        w_load(0, c).start()
        w_load(1, c).start()

    for cp in small:
        cp.start()
    for i in range(qn):
        wq_load(i).start()

    bar = pltpu.get_barrier_semaphore()
    for j in (1, 2, 3):
        pl.semaphore_signal(bar, inc=1, device_id=(zc, yc, lax.rem(h + j, 4)), device_id_type=MESH_ID)
    pl.semaphore_signal(bar, inc=1, device_id=ynb, device_id_type=MESH_ID)
    small[0].wait()
    gu_load_start(0)
    x_f = x_s[...].astype(F32)
    sq_part = jnp.sum(x_f * x_f, axis=-1, keepdims=True)
    with jax.named_scope("barrier"):
        pl.semaphore_wait(bar, 4)

    def stat_copy(n, j):
        return pltpu.make_async_remote_copy(
            src_ref=st_s.at[n], dst_ref=st_r.at[n, h], send_sem=st_sem.at[n, 0, j], recv_sem=st_sem.at[n, 1, j],
            device_id=(zc, yc, lax.rem(h + j, 4)), device_id_type=MESH_ID,
        )

    def stat_send(n, cols):
        tile = pack_stats(cols)
        st_s[n] = tile
        st_r[n, h] = tile
        for j in (1, 2, 3):
            stat_copy(n, j).start()

    def stat_recv(n, count):
        for j in (1, 2, 3):
            stat_copy(n, j).wait()
        return unpack_stats(st_r[n, 0] + st_r[n, 1] + st_r[n, 2] + st_r[n, 3], tok, count)

    def y_copy(n):
        src, dst = (y32.at[0], y32.at[1]) if n == 0 else (ys.at[n - 1], yr.at[n - 1])
        return pltpu.make_async_remote_copy(
            src_ref=src, dst_ref=dst, send_sem=y_sem.at[n, 0], recv_sem=y_sem.at[n, 1],
            device_id=ynb, device_id_type=MESH_ID,
        )

    def y_sum(n):
        with jax.named_scope(f"ywait{n}"):
            y_copy(n).wait()
        if n == 0:
            return y32[0] + y32[1]
        return ys[n - 1].astype(F32) + yr[n - 1].astype(F32)

    stat_send(0, [sq_part])
    gu_load_start(1)
    small[2].wait()
    acc[...] = jnp.zeros_like(acc)

    def qkv_step(i, carry):
        wq_load(i).wait()
        cols = pl.ds(pl.multiple_of(i * 1024, 1024), 1024)
        acc[...] += nt_dot(dq[:, cols], wq[:, cols])
        return carry

    with jax.named_scope("qkv"):
        lax.fori_loop(0, qn, qkv_step, 0)
    gu_load_start(2)
    y32[0] = acc[...]
    y_copy(0).start()
    small[1].wait()
    with jax.named_scope("stat0"):
        (sq,) = stat_recv(0, 1)
    inv1 = lax.rsqrt(sq / d_model + NORM_EPS)
    n1[...] = (x_s[...].astype(F32) * inv1 * g1[...]).astype(BF)
    n1_out = load(n1, n1_o, out_sem.at[0])
    n1_out.start()
    acc[...] = jnp.zeros_like(acc)

    def pair_copy(ph, c):
        slot = lax.rem(c, 2)
        src = part.at[slot, 1 - core] if ph == 0 else part.at[slot, 1 - core, 0]
        return pltpu.make_async_remote_copy(
            src_ref=src, dst_ref=(r1 if ph == 0 else r2).at[c],
            send_sem=sems.at[ph, 2 * PAIR, c], recv_sem=sems.at[ph, 2 * PAIR + 1, c],
            device_id=pair, device_id_type=MESH_ID,
        )

    def x_copy(ph, c):
        src, dst = ((xs, xr), (xs2, xr2))[ph]
        return pltpu.make_async_remote_copy(
            src_ref=src.at[c], dst_ref=dst.at[c],
            send_sem=sems.at[ph, 2 * XRED, c], recv_sem=sems.at[ph, 2 * XRED + 1, c],
            device_id=xnb, device_id_type=MESH_ID,
        )

    own_q = core * 2 + xc
    xnb_q = core * 2 + 1 - xc

    def block(ph, c, q):
        cols = pl.ds(pl.multiple_of(c * c_w + q * quart, quart), quart)
        return a_f.at[:, cols] if ph == 0 else dgu_f.at[:, :, cols]

    def g_copy(ph, c, kind):
        ref = block(ph, c, xnb_q if kind == FW else own_q)
        return pltpu.make_async_remote_copy(
            src_ref=ref, dst_ref=ref,
            send_sem=sems.at[ph, 2 * kind, c], recv_sem=sems.at[ph, 2 * kind + 1, c],
            device_id=xnb if kind == GX else pair, device_id_type=MESH_ID,
        )

    own_cols = pl.ds(pl.multiple_of(xc * quart, quart), quart)
    oth_cols = pl.ds(pl.multiple_of((1 - xc) * quart, quart), quart)

    def pipeline(ph, partial, activate, consume):
        lag_pair, lag_act, lag_fwd, lag_dot = LAGS[ph]

        def step(t, carry):
            if ph == 0:

                @pl.when(t < nc - 3)
                def _():
                    gu_load_start(t + 3)

                @pl.when((t >= 2) & (t < nc + 2))
                def _():
                    w_load(2, t - 2).start()

            @pl.when(t < nc)
            def _():
                c = t

                @pl.when(c >= 2)
                def _():
                    pair_copy(ph, c - 2).wait_send()

                with jax.named_scope(f"part{ph}"):
                    partial(c, 1 - core)
                    pair_copy(ph, c).start()
                    partial(c, core)

            @pl.when((t >= lag_pair) & (t < nc + lag_pair))
            def _():
                c = t - lag_pair
                slot = lax.rem(c, 2)
                with jax.named_scope(f"pairwait{ph}"):
                    pair_copy(ph, c).wait_recv()
                if ph == 0:
                    xs[c] = (part[slot, core, :, :, oth_cols] + r1[c, :, :, oth_cols]).astype(BF)
                    x_copy(ph, c).start()
                    gu[c] = part[slot, core, :, :, own_cols] + r1[c, :, :, own_cols]
                else:
                    xs2[c] = (part[slot, core, 0, :, oth_cols] + r2[c, :, oth_cols]).astype(BF)
                    x_copy(ph, c).start()
                    r2[c, :, own_cols] = part[slot, core, 0, :, own_cols] + r2[c, :, own_cols]

            @pl.when((t >= lag_act) & (t < nc + lag_act))
            def _():
                c = t - lag_act
                with jax.named_scope(f"xwait{ph}"):
                    x_copy(ph, c).wait_recv()
                with jax.named_scope(f"act{ph}"):
                    activate(c)
                g_copy(ph, c, GX).start()
                g_copy(ph, c, GP).start()

            @pl.when((t >= lag_fwd) & (t < nc + lag_fwd))
            def _():
                c = t - lag_fwd
                with jax.named_scope(f"gxwait{ph}"):
                    g_copy(ph, c, GX).wait_recv()
                g_copy(ph, c, FW).start()

            @pl.when((t >= lag_dot) & (t < nc + lag_dot))
            def _():
                c = t - lag_dot
                with jax.named_scope(f"gpwait{ph}"):
                    g_copy(ph, c, GP).wait_recv()
                    g_copy(ph, c, FW).wait_recv()
                with jax.named_scope(f"dot{ph}"):
                    consume(c)
                x_copy(ph, c).wait_send()
                g_copy(ph, c, GX).wait_send()
                g_copy(ph, c, GP).wait_send()
                g_copy(ph, c, FW).wait_send()

            return carry

        lax.fori_loop(0, nc + lag_dot, step, 0)
        pair_copy(ph, nc - 2).wait_send()
        pair_copy(ph, nc - 1).wait_send()

    def gu_partial(c, which):
        @pl.when(which != core)
        def _():
            w_load(0, c).wait()
            w_load(1, c).wait()

        cols = pl.ds(pl.multiple_of(c * c_w + which * half, half), half)
        slot = lax.rem(c, 2)
        part[slot, which, 0] = nn_dot(n1[...], wg[:, cols])
        part[slot, which, 1] = nn_dot(n1[...], wu[:, cols])

    def act_forward(c):
        gate = gu[c, 0] + xr[c, 0].astype(F32)
        up = gu[c, 1] + xr[c, 1].astype(F32)
        gu[c, 0] = gate
        gu[c, 1] = up
        cols = pl.ds(pl.multiple_of(c * c_w + own_q * quart, quart), quart)
        a_f[:, cols] = (jax.nn.silu(gate) * up).astype(BF)

    def down_dot(c):
        w_load(2, c).wait()
        rows = pl.ds(pl.multiple_of(c * c_w, c_w), c_w)
        acc[...] += nn_dot(a_f[:, rows], wd[rows, :])

    pipeline(0, gu_partial, act_forward, down_dot)
    ys[0] = acc[...].astype(BF)
    y_copy(1).start()
    a_out = load(a_f, a_o, out_sem.at[1])
    a_out.start()

    small[3].wait()
    small[4].wait()
    dn2 = y_sum(0)
    acc[...] = dn2
    x2_s[...] = (x_s[...].astype(F32) + y_sum(1)).astype(BF)
    x2 = x2_s[...].astype(F32)
    stat_send(1, [
        jnp.sum(x2 * x2, axis=-1, keepdims=True),
        jnp.sum(g2[...] * acc[...] * x2, axis=-1, keepdims=True),
    ])
    with jax.named_scope("stat1"):
        sq2, dot2 = stat_recv(1, 2)
    inv2 = lax.rsqrt(sq2 / d_model + NORM_EPS)
    x2 = x2_s[...].astype(F32)
    dz2 = inv2 * (g2[...] * acc[...]) - x2 * (inv2 * inv2 * inv2) * (dot2 / d_model)
    e_val = dx_s[...].astype(F32) + dz2
    e_s[...] = e_val
    eb[...] = e_val.astype(BF)
    n2[...] = (x2_s[...].astype(F32) * inv2 * g2[...]).astype(BF)
    dg_s[0:1, :] = jnp.sum(acc[...] * x2_s[...].astype(F32) * inv2, axis=0, keepdims=True)
    outs = [load(eb, eb_o, out_sem.at[2]), load(n2, n2_o, out_sem.at[3])]
    for cp in outs:
        cp.start()
    acc[...] = jnp.zeros_like(acc)

    def da_partial(c, which):
        rows = pl.ds(pl.multiple_of(c * c_w + which * half, half), half)
        part[lax.rem(c, 2), which, 0] = nt_dot(eb[...], wd[rows, :])

    def act_backward(c):
        d_act = r2[c, :, own_cols] + xr2[c].astype(F32)
        gate, up = gu[c, 0], gu[c, 1]
        sig = jax.nn.sigmoid(gate)
        cols = pl.ds(pl.multiple_of(c * c_w + own_q * quart, quart), quart)
        dgu_f[0, :, cols] = (d_act * up * sig * (1.0 + gate * (1.0 - sig))).astype(BF)
        dgu_f[1, :, cols] = (d_act * (gate * sig)).astype(BF)

    def dn1_dot(c):
        cols = pl.ds(pl.multiple_of(c * c_w, c_w), c_w)
        acc[...] += nt_dot(dgu_f[0, :, cols], wg[:, cols]) + nt_dot(dgu_f[1, :, cols], wu[:, cols])

    pipeline(1, da_partial, act_backward, dn1_dot)
    dgu_out = load(dgu_f, dgu_o, out_sem.at[4])
    dgu_out.start()
    ys[1] = acc[...].astype(BF)
    y_copy(2).start()

    acc[...] = y_sum(2)
    stat_send(2, [jnp.sum(g1[...] * acc[...] * x_s[...].astype(F32), axis=-1, keepdims=True)])
    dg_s[1:2, :] = jnp.sum(acc[...] * x_s[...].astype(F32) * inv1, axis=0, keepdims=True)
    with jax.named_scope("stat2"):
        (dot1,) = stat_recv(2, 1)
    dz1 = inv1 * (g1[...] * acc[...]) - x_s[...].astype(F32) * (inv1 * inv1 * inv1) * (dot1 / d_model)
    dxin_s[...] = (e_s[...] + dz1).astype(BF)
    tail = [
        load(dxin_s, dxin_o, out_sem.at[5]),
        load(dg_s.at[0:1, :], dg2_o, out_sem.at[6]),
        load(dg_s.at[1:2, :], dg1_o, out_sem.at[7]),
    ]
    for cp in tail:
        cp.start()
    for cp in (n1_out, a_out, *outs, dgu_out, *tail):
        cp.wait()


def comm_call(x_in, gain_one, gain_two, w_gate, w_up, w_down, w_qkv, dx_out, d_qkv):
    tok, hd = x_in.shape
    ff = w_gate.shape[1]
    qw = w_qkv.shape[1]
    nc = ff // CHUNK
    half, quart = CHUNK // 2, CHUNK // 4
    out = lambda shape, dtype: jax.ShapeDtypeStruct(shape, dtype)
    vm = lambda *shape_dtype: pltpu.VMEM(shape_dtype[:-1], shape_dtype[-1])
    dma = pltpu.SemaphoreType.DMA
    return pl.pallas_call(
        functools.partial(comm_kernel, (tok, hd, ff, qw)),
        out_shape=(
            out((tok, hd), BF), out((tok, hd), BF), out((tok, hd), BF), out((tok, ff), BF), out((2, tok, ff), BF),
            out((tok, hd), BF), out((1, hd), F32), out((1, hd), F32),
        ),
        in_specs=[ANY] * 9,
        out_specs=[ANY] * 8,
        scratch_shapes=[
            vm(hd, ff, BF), vm(hd, ff, BF), vm(ff, hd, BF), vm(hd, qw, BF), vm(tok, qw, BF),
            vm(tok, hd, BF), vm(tok, hd, BF), vm(1, hd, F32), vm(1, hd, F32),
            vm(tok, hd, BF), vm(tok, hd, BF), vm(tok, hd, BF), vm(tok, hd, F32), vm(tok, hd, BF),
            vm(tok, hd, F32), vm(2, 2, 2, tok, half, F32), vm(nc, 2, tok, half, F32), vm(nc, tok, half, F32),
            vm(nc, 2, tok, quart, BF), vm(nc, 2, tok, quart, BF), vm(nc, tok, quart, BF), vm(nc, tok, quart, BF),
            vm(nc, 2, tok, quart, F32), vm(tok, ff, BF), vm(2, tok, ff, BF),
            vm(2, tok, hd, F32), vm(2, tok, hd, BF), vm(2, tok, hd, BF), vm(3, 8, 128, F32), vm(3, 4, 8, 128, F32),
            vm(tok, hd, BF), vm(8, hd, F32),
            dma((5,)), dma((4, nc)), dma((8,)), dma((3, 2, 4)), dma((3, 2)), dma((2, 10, nc)),
        ],
        compiler_params=pltpu.CompilerParams(
            collective_id=0, has_side_effects=True, vmem_limit_bytes=VMEM_LIMIT
        ),
        name="block_comm",
    )(x_in, gain_one, gain_two, w_gate, w_up, w_down, w_qkv, dx_out, d_qkv)


TILE = 512
SLOTS = 3


def grad_kernel(dims, n1, n2, eb, a_f, dgu, dq, dx, dg1, dg2, dwg_o, dwu_o, dwd_o, dwq_o, dx_o, dg1_o, dg2_o, n1_t, n2_t, bg, bu, bd, sem):
    hd, ff, qw = dims
    nt, nq = ff // TILE, qw // TILE
    dx_o[...] = dx[...]
    dg1_o[...] = dg1[...]
    dg2_o[...] = dg2[...]
    n1_t[...] = n1[...].astype(F32).T.astype(BF)
    n2_t[...] = n2[...].astype(F32).T.astype(BF)

    def cols_of(i):
        return pl.ds(pl.multiple_of(i * TILE, TILE), TILE)

    def q_copy(i):
        slot = lax.rem(i, SLOTS)
        return pltpu.make_async_copy(bg.at[slot], dwq_o.at[:, cols_of(i)], sem.at[0, slot])

    def g_copy(i):
        slot = lax.rem(i, SLOTS)
        return pltpu.make_async_copy(bg.at[slot], dwg_o.at[:, cols_of(i)], sem.at[0, slot])

    def u_copy(i):
        slot = lax.rem(i, SLOTS)
        return pltpu.make_async_copy(bu.at[slot], dwu_o.at[:, cols_of(i)], sem.at[1, slot])

    def d_copy(i):
        slot = lax.rem(i, SLOTS)
        return pltpu.make_async_copy(bd.at[slot], dwd_o.at[cols_of(i), :], sem.at[2, slot])

    def q_step(i, carry):
        @pl.when(i >= SLOTS)
        def _():
            q_copy(i - SLOTS).wait()

        bg[lax.rem(i, SLOTS)] = nn_dot(n2_t[...], dq[:, cols_of(i)]).astype(BF)
        q_copy(i).start()
        return carry

    lax.fori_loop(0, nq, q_step, 0)
    for i in range(nq - SLOTS, nq):
        q_copy(i).wait()

    def step(i, carry):
        slot = lax.rem(i, SLOTS)

        @pl.when(i >= SLOTS)
        def _():
            g_copy(i - SLOTS).wait()
            u_copy(i - SLOTS).wait()
            d_copy(i - SLOTS).wait()

        bd[slot] = nn_dot(a_f[:, cols_of(i)].astype(F32).T.astype(BF), eb[...]).astype(BF)
        d_copy(i).start()
        bg[slot] = nn_dot(n1_t[...], dgu[0, :, cols_of(i)]).astype(BF)
        g_copy(i).start()
        bu[slot] = nn_dot(n1_t[...], dgu[1, :, cols_of(i)]).astype(BF)
        u_copy(i).start()
        return carry

    lax.fori_loop(0, nt, step, 0)
    for i in range(nt - SLOTS, nt):
        g_copy(i).wait()
        u_copy(i).wait()
        d_copy(i).wait()


def grad_call(n1, n2, eb, a_full, dgu, d_qkv, dx_in, dg1, dg2):
    tok, hd = n1.shape
    ff, qw = a_full.shape[1], d_qkv.shape[1]
    out = lambda *shape: jax.ShapeDtypeStruct(shape, BF)
    return pl.pallas_call(
        functools.partial(grad_kernel, (hd, ff, qw)),
        out_shape=(
            out(hd, ff), out(hd, ff), out(ff, hd), out(hd, qw),
            out(tok, hd), jax.ShapeDtypeStruct((1, hd), F32), jax.ShapeDtypeStruct((1, hd), F32),
        ),
        in_specs=[pl.BlockSpec(memory_space=pltpu.VMEM)] * 9,
        out_specs=[ANY] * 4 + [pl.BlockSpec(memory_space=pltpu.VMEM)] * 3,
        scratch_shapes=[
            pltpu.VMEM((hd, tok), BF), pltpu.VMEM((hd, tok), BF),
            pltpu.VMEM((SLOTS, hd, TILE), BF), pltpu.VMEM((SLOTS, hd, TILE), BF), pltpu.VMEM((SLOTS, TILE, hd), BF),
            pltpu.SemaphoreType.DMA((3, SLOTS)),
        ],
        compiler_params=pltpu.CompilerParams(vmem_limit_bytes=VMEM_LIMIT),
        name="weight_grads",
    )(n1, n2, eb, a_full, dgu, d_qkv, dx_in, dg1, dg2)


def solution(mesh):
    def local_step(x_in, gain_one, gain_two, w_gate, w_up, w_down, w_qkv, dx_out, d_qkv):
        hd = x_in.shape[1]
        n1, n2, eb, a_full, dgu, dx_in, dg1, dg2 = comm_call(
            x_in, gain_one.reshape(1, hd), gain_two.reshape(1, hd), w_gate, w_up, w_down, w_qkv, dx_out, d_qkv
        )
        dw_gate, dw_up, dw_down, dw_qkv, dx_in, dg1, dg2 = grad_call(
            n1, n2, eb, a_full, dgu, d_qkv, dx_in, dg1, dg2
        )
        return dx_in, dw_gate, dw_up, dw_down, dw_qkv, dg1.reshape(hd), dg2.reshape(hd)

    tok_spec = P("data", "hid")
    in_specs = (tok_spec, P("hid"), P("hid"), P("hid", "ffn"), P("hid", "ffn"), P("ffn", "hid"), P("hid", "ffn"), tok_spec, P("data", "ffn"))
    out_specs = (tok_spec, P(("data", "hid"), "ffn"), P(("data", "hid"), "ffn"), P(("data", "ffn"), "hid"), P(("data", "hid"), "ffn"), P(("data", "hid")), P(("data", "hid")))
    return jax.shard_map(local_step, mesh=mesh, in_specs=in_specs, out_specs=out_specs, check_vma=False)
```

```python
import functools

import jax
import jax.numpy as jnp
from jax import lax
from jax.experimental import pallas as pl
from jax.experimental.pallas import tpu as pltpu
from jax.sharding import PartitionSpec as P

NORM_EPS = 1e-6
BF = jnp.bfloat16
F32 = jnp.float32
MESH_ID = pl.DeviceIdType.MESH
ANY = pl.BlockSpec(memory_space=pl.ANY)
VMEM_LIMIT = 67043328

CHUNK = 1024
LATE = 2
F_STEPS = (0, 3)
PIECES = (0, 1, 2, 4)
DIRECT_LAST = 1
DIRECT_FIRST = 1
LAGS = ((1, 3, 5, 6), (1, 3, 5, 6))

PAIR, XRED, GX, GP, FW, DG = range(6)

PEERS = tuple((dy, j) for dy in range(2) for j in range(4) if dy or j)
ROW_PEERS = PEERS[:3]


def nn_dot(a_mat, b_mat):
    return jnp.dot(a_mat, b_mat, preferred_element_type=F32)


def nt_dot(a_mat, b_mat):
    return lax.dot_general(a_mat, b_mat, (((1,), (1,)), ((), ())), preferred_element_type=F32)


def pack_stats(cols):
    tok = cols[0].shape[0]
    lane = lax.broadcasted_iota(jnp.int32, (tok, 128), 1)
    wide = jnp.zeros((tok, 128), F32)
    for i, col in enumerate(cols):
        wide = jnp.where(lane == i, col, wide)
    full = jnp.concatenate([wide, jnp.zeros((128 - tok, 128), F32)], axis=0)
    return full.T[0:8, :]


def unpack_stats(tile, tok, count):
    full = jnp.concatenate([tile, jnp.zeros((120, 128), F32)], axis=0).T
    return [full[0:tok, i : i + 1] for i in range(count)]


def comm_kernel(
    dims,
    x_h, g1_h, g2_h, wg_h, wu_h, wd_h, wq_h, dx_h, dq_h,
    n1_o, n2_o, eb_o, a_o, dgu_o, dxin_o, dg_o,
    wg, wu, wd, wq, dq, x_s, dx_s, g1, g2, n1, n2, eb, e_s, x2_s,
    acc, part, r1, r2, xs, xr, xs2, xr2, gu, fb, a_f, da_f, dgu_f, y32, ys, yr, st_s, st_r, dxin_s, dg_s,
    ld, wld, out_sem, st_sem, y_sem, recvs, sends, f_sem,
):
    tok, hd, ff, qw = dims
    c_w = CHUNK
    nc = ff // c_w
    half = c_w // 2
    quart = c_w // 4
    d_model = hd * 4
    zc, yc, h = lax.axis_index("data"), lax.axis_index("ffn"), lax.axis_index("hid")
    xc = h // 2
    core = lax.rem(h, 2)
    pair = (zc, yc, xc * 2 + 1 - core)
    xnb = (zc, yc, (1 - xc) * 2 + core)
    diag = (zc, yc, 3 - h)
    ynb = (zc, 1 - yc, h)

    def peer(dy, j):
        return (zc, lax.rem(yc + dy, 2), lax.rem(h + j, 4))


    def load(src, dst, sem):
        return pltpu.make_async_copy(src, dst, sem)

    small = [
        load(x_h, x_s, ld.at[0]), load(g1_h, g1, ld.at[1]), load(dq_h, dq, ld.at[2]),
        load(g2_h, g2, ld.at[3]), load(dx_h, dx_s, ld.at[4]),
    ]
    qn = qw // 1024

    def wq_load(i):
        cols = pl.ds(pl.multiple_of(i * 1024, 1024), 1024)
        return load(wq_h.at[:, cols], wq.at[:, cols], wld.at[2, i])

    pieces = [c for c in PIECES if c < nc]

    def gu_load(i, n):
        first = pieces[n]
        last = pieces[n + 1] if n + 1 < len(pieces) else nc
        cols = pl.ds(first * c_w, (last - first) * c_w)
        src, dst = ((wg_h, wg), (wu_h, wu))[i]
        return load(src.at[:, cols], dst.at[:, cols], wld.at[i, n])

    def gu_load_wait(c):
        for n, first in enumerate(pieces):

            @pl.when(c == first)
            def _():
                gu_load(0, n).wait()
                gu_load(1, n).wait()

    wd_load = load(wd_h, wd, ld.at[5])

    def gu_load_start(n):
        gu_load(0, n).start()
        gu_load(1, n).start()

    for cp in small:
        cp.start()
    for i in range(qn):
        wq_load(i).start()

    bar = pltpu.get_barrier_semaphore()
    for dy, j in PEERS[:4]:
        pl.semaphore_signal(bar, inc=1, device_id=peer(dy, j), device_id_type=MESH_ID)
    small[0].wait()
    gu_load_start(0)
    x_f = x_s[...].astype(F32)
    sq_part = jnp.sum(x_f * x_f, axis=-1, keepdims=True)

    def qkv_step(i, carry):
        wq_load(i).wait()
        cols = pl.ds(pl.multiple_of(i * 1024, 1024), 1024)
        y32[0] += nt_dot(dq[:, cols], wq[:, cols])
        return carry

    y32[0] = jnp.zeros((tok, hd), F32)
    with jax.named_scope("barrier"):
        pl.semaphore_wait(bar, 4)

    def stat_copy(n, i):
        return pltpu.make_async_remote_copy(
            src_ref=st_s.at[n], dst_ref=st_r.at[n, yc * 4 + h], send_sem=st_sem.at[n, 0], recv_sem=st_sem.at[n, 1],
            device_id=peer(*PEERS[i]), device_id_type=MESH_ID,
        )

    def stat_send(n, cols, peers=ROW_PEERS):
        tile = pack_stats(cols)
        st_s[n] = tile
        st_r[n, yc * 4 + h] = tile
        for i in range(len(peers)):
            stat_copy(n, i).start()

    def stat_recv(n, count, peers=ROW_PEERS):
        all_tiles = st_r.at[n, pl.ds(0, len(peers))]
        whole = pltpu.make_async_remote_copy(
            src_ref=all_tiles, dst_ref=all_tiles, send_sem=st_sem.at[n, 0], recv_sem=st_sem.at[n, 1],
            device_id=peer(*PEERS[0]), device_id_type=MESH_ID,
        )
        whole.wait()
        total = jnp.zeros((8, 128), F32)
        for i in range(len(peers) + 1):
            total += st_r[n, i] if peers is PEERS else st_r[n, yc * 4 + i]
        return unpack_stats(total, tok, count)

    def y_copy(n):
        src, dst = (y32.at[0], y32.at[1]) if n == 0 else (ys.at[n - 1], yr.at[n - 1])
        return pltpu.make_async_remote_copy(
            src_ref=src, dst_ref=dst, send_sem=y_sem.at[n, 0], recv_sem=y_sem.at[n, 1],
            device_id=ynb, device_id_type=MESH_ID,
        )

    def y_sum(n):
        with jax.named_scope(f"ywait{n}"):
            y_copy(n).wait()
        if n == 0:
            return y32[0] + y32[1]
        return ys[n - 1].astype(F32) + yr[n - 1].astype(F32)

    stat_send(0, [sq_part])
    gu_load_start(1)
    small[2].wait()
    with jax.named_scope("qkv"):
        lax.fori_loop(0, qn, qkv_step, 0)
    gu_load_start(2)
    y_copy(0).start()
    small[1].wait()
    with jax.named_scope("stat0"):
        (sq,) = stat_recv(0, 1)
    inv1 = lax.rsqrt(sq / d_model + NORM_EPS)
    n1[...] = (x_s[...].astype(F32) * inv1 * g1[...]).astype(BF)
    n1_out = load(n1, n1_o, out_sem.at[0])
    n1_out.start()
    acc[...] = jnp.zeros_like(acc)

    def pair_copy(ph, c):
        slot = lax.rem(c, 2)
        src = part.at[slot, 1 - core] if ph == 0 else part.at[slot, 1 - core, 0]
        return pltpu.make_async_remote_copy(
            src_ref=src, dst_ref=(r1 if ph == 0 else r2).at[c],
            send_sem=sends.at[4 + slot], recv_sem=recvs.at[PAIR, c],
            device_id=pair, device_id_type=MESH_ID,
        )

    def x_copy(ph, c):
        src, dst = ((xs, xr), (xs2, xr2))[ph]
        return pltpu.make_async_remote_copy(
            src_ref=src.at[c], dst_ref=dst.at[c],
            send_sem=sends.at[0], recv_sem=recvs.at[XRED, c],
            device_id=xnb, device_id_type=MESH_ID,
        )

    own_q = core * 2 + xc
    xnb_q = core * 2 + 1 - xc

    def block(ph, c, q):
        cols = pl.ds(pl.multiple_of(c * c_w + q * quart, quart), quart)
        return (a_f if ph == 0 else da_f).at[:, cols]

    def g_copy(ph, c, kind):
        ref = block(ph, c, xnb_q if kind == FW else own_q)
        target = {GX: xnb, GP: pair, FW: pair, DG: diag}[kind]
        kind = FW if kind == DG else kind
        return pltpu.make_async_remote_copy(
            src_ref=ref, dst_ref=ref, send_sem=sends.at[kind - 1], recv_sem=recvs.at[kind, c],
            device_id=target, device_id_type=MESH_ID,
        )

    def wait_sends(ph):
        src = xs if ph == 0 else xs2
        pltpu.make_async_remote_copy(
            src_ref=src, dst_ref=src, send_sem=sends.at[0], recv_sem=recvs.at[XRED, 0],
            device_id=xnb, device_id_type=MESH_ID,
        ).wait_send()
        whole = (a_f if ph == 0 else da_f).at[:, pl.ds(0, ff // 4)]
        for kind in (GX, GP, FW):
            pltpu.make_async_remote_copy(
                src_ref=whole, dst_ref=whole, send_sem=sends.at[kind - 1], recv_sem=recvs.at[kind, 0],
                device_id=xnb, device_id_type=MESH_ID,
            ).wait_send()
        for c in (nc - 2, nc - 1):
            pair_copy(ph, c).wait_send()

    f_parts = ((0, nc - LATE), (nc - LATE, LATE))

    def f_copy(n):
        first, count = f_parts[n % 2] if n < 4 else (0, nc)
        ref = fb.at[xnb_q if n in (2, 3) else own_q, pl.ds(first, count)]
        return pltpu.make_async_remote_copy(
            src_ref=ref, dst_ref=ref, send_sem=f_sem.at[n, 0], recv_sem=f_sem.at[n, 1],
            device_id=xnb if n < 2 else pair, device_id_type=MESH_ID,
        )

    own_cols = pl.ds(pl.multiple_of(xc * quart, quart), quart)
    oth_cols = pl.ds(pl.multiple_of((1 - xc) * quart, quart), quart)

    def pipeline(ph, partial, activate, consume):
        lag_pair, lag_act, lag_fwd, lag_dot = LAGS[ph]

        def direct(c):
            return c >= nc - DIRECT_LAST if ph == 0 else c < DIRECT_FIRST


        def step(t, carry):
            if ph == 1:
                for n, when in enumerate(F_STEPS):

                    @pl.when(t == when)
                    def _():
                        f_copy(n).wait_recv()
                        f_copy(2 + n).start()

            if ph == 0:

                @pl.when(t == 0)
                def _():
                    for n in range(3, len(pieces)):
                        gu_load_start(n)

                @pl.when(t == 2)
                def _():
                    wd_load.start()

            @pl.when(t < nc)
            def _():
                c = t

                @pl.when(c >= 2)
                def _():
                    pair_copy(ph, c - 2).wait_send()

                with jax.named_scope(f"part{ph}"):

                    @pl.when(c == 0)
                    def _():
                        partial(c, 1 - core)
                        pair_copy(ph, c).start()
                        partial(c, core)

                    @pl.when(c > 0)
                    def _():
                        partial(c, None)
                        pair_copy(ph, c).start()

            @pl.when((t >= lag_pair) & (t < nc + lag_pair))
            def _():
                c = t - lag_pair
                slot = lax.rem(c, 2)
                with jax.named_scope(f"pairwait{ph}"):
                    pair_copy(ph, c).wait_recv()
                if ph == 0:
                    xs[c] = (part[slot, core, :, :, oth_cols] + r1[c, :, :, oth_cols]).astype(BF)
                    x_copy(ph, c).start()
                    gu[c] = part[slot, core, :, :, own_cols] + r1[c, :, :, own_cols]
                else:
                    xs2[c] = (part[slot, core, 0, :, oth_cols] + r2[c, :, oth_cols]).astype(BF)
                    x_copy(ph, c).start()
                    r2[c, :, own_cols] = part[slot, core, 0, :, own_cols] + r2[c, :, own_cols]

            @pl.when((t >= lag_act) & (t < nc + lag_act))
            def _():
                c = t - lag_act
                with jax.named_scope(f"xwait{ph}"):
                    x_copy(ph, c).wait_recv()
                with jax.named_scope(f"act{ph}"):
                    activate(c)
                g_copy(ph, c, GX).start()
                g_copy(ph, c, GP).start()

                @pl.when(direct(c))
                def _():
                    g_copy(ph, c, DG).start()

                if ph == 0:

                    @pl.when(c == nc - 1)
                    def _():
                        f_copy(0).start()

            @pl.when((t >= lag_fwd) & (t < nc + lag_fwd))
            def _():
                c = t - lag_fwd
                with jax.named_scope(f"gxwait{ph}"):
                    g_copy(ph, c, GX).wait_recv()

                @pl.when(jnp.logical_not(direct(c)))
                def _():
                    g_copy(ph, c, FW).start()

            @pl.when((t >= lag_dot) & (t < nc + lag_dot))
            def _():
                c = t - lag_dot
                with jax.named_scope(f"gpwait{ph}"):
                    g_copy(ph, c, GP).wait_recv()
                    g_copy(ph, c, FW).wait_recv()
                with jax.named_scope(f"dot{ph}"):
                    consume(c)

            return carry

        lax.fori_loop(0, nc + lag_dot, step, 0)

    def gu_partial(c, which):
        if which is not core:
            gu_load_wait(c)
        slot = lax.rem(c, 2)
        for i, w in enumerate((wg, wu)):
            if which is None:
                prod = nn_dot(n1[...], w[:, pl.ds(pl.multiple_of(c * c_w, c_w), c_w)])
                part[slot, 0, i] = prod[:, :half]
                part[slot, 1, i] = prod[:, half:]
            else:
                part[slot, which, i] = nn_dot(n1[...], w[:, pl.ds(pl.multiple_of(c * c_w + which * half, half), half)])

    def act_forward(c):
        gate = gu[c, 0] + xr[c, 0].astype(F32)
        up = gu[c, 1] + xr[c, 1].astype(F32)
        sig = jax.nn.sigmoid(gate)
        silu = gate * sig
        cols = pl.ds(pl.multiple_of(c * c_w + own_q * quart, quart), quart)
        a_f[:, cols] = (silu * up).astype(BF)
        fb[own_q, c, 0] = (up * sig * (1.0 + gate * (1.0 - sig))).astype(BF)
        fb[own_q, c, 1] = silu.astype(BF)

    def down_dot(c):
        @pl.when(c == 0)
        def _():
            wd_load.wait()

        rows = pl.ds(pl.multiple_of(c * c_w, c_w), c_w)
        acc[...] += nn_dot(a_f[:, rows], wd[rows, :])

    pipeline(0, gu_partial, act_forward, down_dot)
    ys[0] = acc[...].astype(BF)
    y_copy(1).start()
    wait_sends(0)
    f_copy(4).start()
    a_out = load(a_f, a_o, out_sem.at[1])
    a_out.start()

    small[3].wait()
    small[4].wait()
    dn2 = y_sum(0)
    acc[...] = dn2
    x2_s[...] = (x_s[...].astype(F32) + y_sum(1)).astype(BF)
    x2 = x2_s[...].astype(F32)
    stat_send(1, [
        jnp.sum(x2 * x2, axis=-1, keepdims=True),
        jnp.sum(g2[...] * acc[...] * x2, axis=-1, keepdims=True),
    ])
    f_copy(1).start()
    with jax.named_scope("stat1"):
        sq2, dot2 = stat_recv(1, 2)
    inv2 = lax.rsqrt(sq2 / d_model + NORM_EPS)
    x2 = x2_s[...].astype(F32)
    dz2 = inv2 * (g2[...] * acc[...]) - x2 * (inv2 * inv2 * inv2) * (dot2 / d_model)
    e_val = dx_s[...].astype(F32) + dz2
    e_s[...] = e_val
    eb[...] = e_val.astype(BF)
    n2[...] = (x2_s[...].astype(F32) * inv2 * g2[...]).astype(BF)
    dg_s[0:1, :] = jnp.sum(acc[...] * x2_s[...].astype(F32) * inv2, axis=0, keepdims=True)
    outs = [load(eb, eb_o, out_sem.at[2]), load(n2, n2_o, out_sem.at[3])]
    for cp in outs:
        cp.start()
    acc[...] = jnp.zeros_like(acc)

    def da_partial(c, which):
        slot = lax.rem(c, 2)
        if which is None:
            prod = nt_dot(eb[...], wd[pl.ds(pl.multiple_of(c * c_w, c_w), c_w), :])
            part[slot, 0, 0] = prod[:, :half]
            part[slot, 1, 0] = prod[:, half:]
        else:
            part[slot, which, 0] = nt_dot(eb[...], wd[pl.ds(pl.multiple_of(c * c_w + which * half, half), half), :])

    def act_backward(c):
        cols = pl.ds(pl.multiple_of(c * c_w + own_q * quart, quart), quart)
        da_f[:, cols] = (r2[c, :, own_cols] + xr2[c].astype(F32)).astype(BF)

    def dn1_dot(c):
        @pl.when(c == 0)
        def _():
            f_copy(4).wait_recv()
            f_copy(2).wait_recv()

        @pl.when(c == nc - LATE)
        def _():
            f_copy(3).wait_recv()

        for q in range(4):
            cols = pl.ds(pl.multiple_of(c * c_w + q * quart, quart), quart)
            d_act = da_f[:, cols].astype(F32)
            for i in range(2):
                dgu_f[i, :, cols] = (d_act * fb[q, c, i].astype(F32)).astype(BF)
        cols = pl.ds(pl.multiple_of(c * c_w, c_w), c_w)
        acc[...] += nt_dot(dgu_f[0, :, cols], wg[:, cols]) + nt_dot(dgu_f[1, :, cols], wu[:, cols])
    pipeline(1, da_partial, act_backward, dn1_dot)
    dgu_out = load(dgu_f, dgu_o, out_sem.at[4])

    stat_send(2, [jnp.sum(g1[...] * acc[...] * x_s[...].astype(F32), axis=-1, keepdims=True)], PEERS)
    ys[1] = acc[...].astype(BF)
    y_copy(2).start()
    dgu_out.start()
    wait_sends(1)
    for n in range(5):
        f_copy(n).wait_send()
    acc[...] = y_sum(2)
    with jax.named_scope("fin0"):
      dg_s[1:2, :] = jnp.sum(acc[...] * x_s[...].astype(F32) * inv1, axis=0, keepdims=True)
    with jax.named_scope("stat2"):
        (dot1,) = stat_recv(2, 1, PEERS)
    with jax.named_scope("fin1"):
      dz1 = inv1 * (g1[...] * acc[...]) - x_s[...].astype(F32) * (inv1 * inv1 * inv1) * (dot1 / d_model)
      dxin_s[...] = (e_s[...] + dz1).astype(BF)
    tail = [
        load(dxin_s, dxin_o, out_sem.at[5]),
        load(dg_s, dg_o, out_sem.at[6]),
    ]
    for cp in tail:
        cp.start()
    with jax.named_scope("fin2"):
      for cp in (n1_out, a_out, *outs, dgu_out, *tail):
        cp.wait()


def comm_call(x_in, gain_one, gain_two, w_gate, w_up, w_down, w_qkv, dx_out, d_qkv):
    tok, hd = x_in.shape
    ff = w_gate.shape[1]
    qw = w_qkv.shape[1]
    nc = ff // CHUNK
    half, quart = CHUNK // 2, CHUNK // 4
    out = lambda shape, dtype: jax.ShapeDtypeStruct(shape, dtype)
    vm = lambda *shape_dtype: pltpu.VMEM(shape_dtype[:-1], shape_dtype[-1])
    dma = pltpu.SemaphoreType.DMA
    return pl.pallas_call(
        functools.partial(comm_kernel, (tok, hd, ff, qw)),
        out_shape=(
            out((tok, hd), BF), out((tok, hd), BF), out((tok, hd), BF), out((tok, ff), BF), out((2, tok, ff), BF),
            out((tok, hd), BF), out((8, hd), F32),
        ),
        in_specs=[ANY] * 9,
        out_specs=[ANY] * 7,
        scratch_shapes=[
            vm(hd, ff, BF), vm(hd, ff, BF), vm(ff, hd, BF), vm(hd, qw, BF), vm(tok, qw, BF),
            vm(tok, hd, BF), vm(tok, hd, BF), vm(1, hd, F32), vm(1, hd, F32),
            vm(tok, hd, BF), vm(tok, hd, BF), vm(tok, hd, BF), vm(tok, hd, F32), vm(tok, hd, BF),
            vm(tok, hd, F32), vm(2, 2, 2, tok, half, F32), vm(nc, 2, tok, half, F32), vm(nc, tok, half, F32),
            vm(nc, 2, tok, quart, BF), vm(nc, 2, tok, quart, BF), vm(nc, tok, quart, BF), vm(nc, tok, quart, BF),
            vm(nc, 2, tok, quart, F32), vm(4, nc, 2, tok, quart, BF), vm(tok, ff, BF), vm(tok, ff, BF), vm(2, tok, ff, BF),
            vm(2, tok, hd, F32), vm(2, tok, hd, BF), vm(2, tok, hd, BF), vm(3, 8, 128, F32), vm(3, 8, 8, 128, F32),
            vm(tok, hd, BF), vm(8, hd, F32),
            dma((6,)), dma((3, 4)), dma((7,)), dma((3, 2)), dma((3, 2)), dma((5, nc)), dma((6,)), dma((5, 2)),
        ],
        compiler_params=pltpu.CompilerParams(
            collective_id=0, has_side_effects=True, vmem_limit_bytes=VMEM_LIMIT
        ),
        name="block_comm",
    )(x_in, gain_one, gain_two, w_gate, w_up, w_down, w_qkv, dx_out, d_qkv)


TILE = 512
SLOTS = 3


def grad_kernel(
    dims, n1_h, n2_h, eb_h, a_h, dgu_h, dq_h, dx_h, dg_h,
    dwg_o, dwu_o, dwd_o, dwq_o, dx_o, dg1_o, dg2_o,
    n1, n2, eb, a_f, dgu, dq, dx, dg, n1_t, n2_t, bq, bg, bu, bd, ld, sem,
):
    hd, ff, qw = dims
    nt, nq = ff // TILE, qw // TILE
    pairs = ((n2_h, n2), (dq_h, dq), (eb_h, eb), (a_h, a_f), (n1_h, n1), (dgu_h, dgu), (dx_h, dx), (dg_h, dg))
    loads = [pltpu.make_async_copy(src, dst, ld.at[i]) for i, (src, dst) in enumerate(pairs)]
    for cp in loads:
        cp.start()

    def cols_of(i):
        return pl.ds(pl.multiple_of(i * TILE, TILE), TILE)

    def out_copy(kind, i):
        slot = lax.rem(i, SLOTS)
        src = (bq, bg, bu, bd)[kind].at[slot]
        dst = (dwq_o, dwg_o, dwu_o, dwd_o)[kind]
        return pltpu.make_async_copy(src, dst.at[cols_of(i), :] if kind == 3 else dst.at[:, cols_of(i)], sem.at[kind, slot])

    with jax.named_scope("b_in0"):
      loads[0].wait()
      loads[1].wait()
    with jax.named_scope("b_t"):
      n2_t[...] = n2[...].T

    def q_step(i, carry):
        @pl.when(i >= SLOTS)
        def _():
            out_copy(0, i - SLOTS).wait()

        bq[lax.rem(i, SLOTS)] = nn_dot(n2_t[...], dq[:, cols_of(i)]).astype(BF)
        out_copy(0, i).start()
        return carry

    with jax.named_scope("b_q"):
      lax.fori_loop(0, nq, q_step, 0)
    with jax.named_scope("b_in1"):
      for cp in loads[2:]:
        cp.wait()
    finals = [
        pltpu.make_async_copy(dx, dx_o, ld.at[0]),
        pltpu.make_async_copy(dg.at[0:1, :], dg2_o, ld.at[1]),
        pltpu.make_async_copy(dg.at[1:2, :], dg1_o, ld.at[2]),
    ]
    for cp in finals:
        cp.start()
    n1_t[...] = n1[...].T

    def step(i, carry):
        slot = lax.rem(i, SLOTS)

        with jax.named_scope("b_wait"):
          @pl.when(i >= SLOTS)
          def _():
            for kind in (1, 2, 3):
                out_copy(kind, i - SLOTS).wait()

        bd[slot] = nn_dot(a_f[:, cols_of(i)].T, eb[...]).astype(BF)
        out_copy(3, i).start()
        bg[slot] = nn_dot(n1_t[...], dgu[0, :, cols_of(i)]).astype(BF)
        out_copy(1, i).start()
        bu[slot] = nn_dot(n1_t[...], dgu[1, :, cols_of(i)]).astype(BF)
        out_copy(2, i).start()
        return carry

    lax.fori_loop(0, nt, step, 0)
    for cp in finals:
        cp.wait()
    with jax.named_scope("b_end"):
     for i in range(nq - SLOTS, nq):
        out_copy(0, i).wait()
     for i in range(nt - SLOTS, nt):
        for kind in (1, 2, 3):
            out_copy(kind, i).wait()


def grad_call(n1, n2, eb, a_full, dgu, d_qkv, dx_in, dg):
    tok, hd = n1.shape
    ff, qw = a_full.shape[1], d_qkv.shape[1]
    out = lambda *shape: jax.ShapeDtypeStruct(shape, BF)
    vm = lambda *shape: pltpu.VMEM(shape, BF)
    return pl.pallas_call(
        functools.partial(grad_kernel, (hd, ff, qw)),
        out_shape=(
            out(hd, ff), out(hd, ff), out(ff, hd), out(hd, qw),
            out(tok, hd), jax.ShapeDtypeStruct((1, hd), F32), jax.ShapeDtypeStruct((1, hd), F32),
        ),
        in_specs=[ANY] * 8,
        out_specs=[ANY] * 7,
        scratch_shapes=[
            vm(tok, hd), vm(tok, hd), vm(tok, hd), vm(tok, ff), vm(2, tok, ff), vm(tok, qw), vm(tok, hd), pltpu.VMEM((8, hd), F32), vm(hd, tok), vm(hd, tok),
            vm(SLOTS, hd, TILE), vm(SLOTS, hd, TILE), vm(SLOTS, hd, TILE), vm(SLOTS, TILE, hd),
            pltpu.SemaphoreType.DMA((8,)), pltpu.SemaphoreType.DMA((4, SLOTS)),
        ],
        compiler_params=pltpu.CompilerParams(vmem_limit_bytes=VMEM_LIMIT),
        name="weight_grads",
    )(n1, n2, eb, a_full, dgu, d_qkv, dx_in, dg)


def solution(mesh):
    def local_step(x_in, gain_one, gain_two, w_gate, w_up, w_down, w_qkv, dx_out, d_qkv):
        hd = x_in.shape[1]
        n1, n2, eb, a_full, dgu, dx_in, dg = comm_call(
            x_in, gain_one.reshape(1, hd), gain_two.reshape(1, hd), w_gate, w_up, w_down, w_qkv, dx_out, d_qkv
        )
        dw_gate, dw_up, dw_down, dw_qkv, dx_in, dg1, dg2 = grad_call(
            n1, n2, eb, a_full, dgu, d_qkv, dx_in, dg
        )
        return dx_in, dw_gate, dw_up, dw_down, dw_qkv, dg1.reshape(hd), dg2.reshape(hd)

    tok_spec = P("data", "hid")
    in_specs = (tok_spec, P("hid"), P("hid"), P("hid", "ffn"), P("hid", "ffn"), P("ffn", "hid"), P("hid", "ffn"), tok_spec, P("data", "ffn"))
    out_specs = (tok_spec, P(("data", "hid"), "ffn"), P(("data", "hid"), "ffn"), P(("data", "ffn"), "hid"), P(("data", "hid"), "ffn"), P(("data", "hid")), P(("data", "hid")))
    return jax.shard_map(local_step, mesh=mesh, in_specs=in_specs, out_specs=out_specs, check_vma=False)
```

```python
import functools

import jax
import jax.numpy as jnp
from jax import lax
from jax.experimental import pallas as pl
from jax.experimental.pallas import tpu as pltpu
from jax.sharding import PartitionSpec as P

NORM_EPS = 1e-6
BF = jnp.bfloat16
F32 = jnp.float32
MESH_ID = pl.DeviceIdType.MESH
ANY = pl.BlockSpec(memory_space=pl.ANY)
VMEM_LIMIT = 67043328

CHUNK = 1024
LATE = 2
YB = 2
F_STEPS = (0, 3)
QKV_AT = 7
DIRECT_LAST = 1
DIRECT_FIRST = 0
LAGS = ((1, 4, 7, 8), (1, 3, 5, 6))

PAIR, XRED, GX, GP, FW, DG = range(6)

PEERS = tuple((dy, j) for dy in range(2) for j in range(4) if dy or j)
ROW_PEERS = PEERS[:3]


def nn_dot(a_mat, b_mat):
    return jnp.dot(a_mat, b_mat, preferred_element_type=F32)


def nt_dot(a_mat, b_mat):
    return lax.dot_general(a_mat, b_mat, (((1,), (1,)), ((), ())), preferred_element_type=F32)


def pack_stats(cols):
    tok = cols[0].shape[0]
    lane = lax.broadcasted_iota(jnp.int32, (tok, 128), 1)
    wide = jnp.zeros((tok, 128), F32)
    for i, col in enumerate(cols):
        wide = jnp.where(lane == i, col, wide)
    full = jnp.concatenate([wide, jnp.zeros((128 - tok, 128), F32)], axis=0)
    return full.T[0:8, :]


def unpack_stats(tile, tok, count):
    full = jnp.concatenate([tile, jnp.zeros((120, 128), F32)], axis=0).T
    return [full[0:tok, i : i + 1] for i in range(count)]


def comm_kernel(
    dims,
    x_h, g1_h, g2_h, wg_h, wu_h, wd_h, wq_h, dx_h, dq_h,
    n1_o, n2_o, eb_o, a_o, dgu_o, dxin_o, dg_o,
    wgu, wd, wq, dq, x_s, dx_s, g1, g2, n1, n2, eb, e_s, x2_s,
    acc, part, r1, r2, xs, xr, xs2, xr2, gu, fb, a_f, da_f, dgu_f, y32, ys, yr, st_s, st_r, dxin_s, dg_s,
    ld, wld, qld, out_sem, st_sem, y_sem, recvs, sends, f_sem,
):
    tok, hd, ff, qw = dims
    c_w = CHUNK
    nc = ff // c_w
    half = c_w // 2
    quart = c_w // 4
    d_model = hd * 4
    zc, yc, h = lax.axis_index("data"), lax.axis_index("ffn"), lax.axis_index("hid")
    xc = h // 2
    core = lax.rem(h, 2)
    pair = (zc, yc, xc * 2 + 1 - core)
    xnb = (zc, yc, (1 - xc) * 2 + core)
    diag = (zc, yc, 3 - h)
    ynb = (zc, 1 - yc, h)

    def peer(dy, j):
        return (zc, lax.rem(yc + dy, 2), lax.rem(h + j, 4))


    def load(src, dst, sem):
        return pltpu.make_async_copy(src, dst, sem)

    small = [
        load(x_h, x_s, ld.at[0]), load(g1_h, g1, ld.at[1]), load(dq_h, dq, ld.at[2]),
        load(g2_h, g2, ld.at[3]), load(dx_h, dx_s, ld.at[4]),
    ]
    qn = qw // 1024

    def wq_load(i):
        cols = pl.ds(pl.multiple_of(i * 1024, 1024), 1024)
        return load(wq_h.at[:, cols], wq.at[:, cols], qld.at[i])

    def gu_load(i, c):
        src = (wg_h, wu_h)[i].at[:, pl.ds(pl.multiple_of(c * c_w, c_w), c_w)]
        dst = wgu.at[:, pl.ds(pl.multiple_of((2 * c + i) * c_w, c_w), c_w)]
        return load(src, dst, wld.at[i, c])

    wd_load = load(wd_h, wd, ld.at[5])

    def gu_load_start(n):
        gu_load(0, n).start()
        gu_load(1, n).start()

    for cp in small:
        cp.start()

    bar = pltpu.get_barrier_semaphore()
    for dy, j in PEERS[:4]:
        pl.semaphore_signal(bar, inc=1, device_id=peer(dy, j), device_id_type=MESH_ID)
    small[0].wait()
    gu_load_start(0)
    gu_load_start(1)
    x_f = x_s[...].astype(F32)
    sq_part = jnp.sum(x_f * x_f, axis=-1, keepdims=True)

    def qkv_step(i):
        wq_load(i).wait()
        cols = pl.ds(pl.multiple_of(i * 1024, 1024), 1024)
        y32[0] += nt_dot(dq[:, cols], wq[:, cols])

    y32[0] = jnp.zeros((tok, hd), F32)
    with jax.named_scope("barrier"):
        pl.semaphore_wait(bar, 4)

    def stat_copy(n, i):
        return pltpu.make_async_remote_copy(
            src_ref=st_s.at[n], dst_ref=st_r.at[n, yc * 4 + h], send_sem=st_sem.at[n, 0], recv_sem=st_sem.at[n, 1],
            device_id=peer(*PEERS[i]), device_id_type=MESH_ID,
        )

    def stat_send(n, cols, peers=ROW_PEERS):
        tile = pack_stats(cols)
        st_s[n] = tile
        st_r[n, yc * 4 + h] = tile
        for i in range(len(peers)):
            stat_copy(n, i).start()

    def stat_recv(n, count, peers=ROW_PEERS):
        all_tiles = st_r.at[n, pl.ds(0, len(peers))]
        whole = pltpu.make_async_remote_copy(
            src_ref=all_tiles, dst_ref=all_tiles, send_sem=st_sem.at[n, 0], recv_sem=st_sem.at[n, 1],
            device_id=peer(*PEERS[0]), device_id_type=MESH_ID,
        )
        whole.wait()
        total = jnp.zeros((8, 128), F32)
        for i in range(len(peers) + 1):
            total += st_r[n, i] if peers is PEERS else st_r[n, yc * 4 + i]
        return unpack_stats(total, tok, count)

    yb = hd // YB

    def y_cols(j):
        return pl.ds(j * yb, yb)

    def y_copy(n, j=0):
        if n == 0:
            src, dst = y32.at[0], y32.at[1]
        else:
            src, dst = ys.at[n - 1, :, y_cols(j)], yr.at[n - 1, :, y_cols(j)]
        return pltpu.make_async_remote_copy(
            src_ref=src, dst_ref=dst, send_sem=y_sem.at[n, YB], recv_sem=y_sem.at[n, j],
            device_id=ynb, device_id_type=MESH_ID,
        )

    def y_send(n, j):
        ys[n - 1, :, y_cols(j)] = acc[:, y_cols(j)].astype(BF)
        y_copy(n, j).start()

    def y_sum(n, j):
        with jax.named_scope(f"ywait{n}"):
            y_copy(n, j).wait_recv()
        return ys[n - 1, :, y_cols(j)].astype(F32) + yr[n - 1, :, y_cols(j)].astype(F32)

    def y_wait_send(n):
        whole = ys.at[n - 1]
        pltpu.make_async_remote_copy(
            src_ref=whole, dst_ref=whole, send_sem=y_sem.at[n, YB], recv_sem=y_sem.at[n, 0],
            device_id=ynb, device_id_type=MESH_ID,
        ).wait_send()

    stat_send(0, [sq_part])
    gu_load_start(2)
    gu_load_start(3)
    small[2].wait()
    small[1].wait()
    with jax.named_scope("stat0"):
        (sq,) = stat_recv(0, 1)
    gu_load_start(4)
    gu_load_start(5)
    inv1 = lax.rsqrt(sq / d_model + NORM_EPS)
    n1[...] = (x_s[...].astype(F32) * inv1 * g1[...]).astype(BF)
    n1_out = load(n1, n1_o, out_sem.at[0])
    n1_out.start()
    acc[...] = jnp.zeros_like(acc)

    def pair_copy(ph, c):
        slot = lax.rem(c, 2)
        src = part.at[slot, 1 - core] if ph == 0 else part.at[slot, 1 - core, 0]
        return pltpu.make_async_remote_copy(
            src_ref=src, dst_ref=(r1 if ph == 0 else r2).at[c],
            send_sem=sends.at[4 + slot], recv_sem=recvs.at[PAIR, c],
            device_id=pair, device_id_type=MESH_ID,
        )

    def x_copy(ph, c):
        src, dst = ((xs, xr), (xs2, xr2))[ph]
        return pltpu.make_async_remote_copy(
            src_ref=src.at[c], dst_ref=dst.at[c],
            send_sem=sends.at[0], recv_sem=recvs.at[XRED, c],
            device_id=xnb, device_id_type=MESH_ID,
        )

    own_q = core * 2 + xc
    xnb_q = core * 2 + 1 - xc

    def block(ph, c, q):
        cols = pl.ds(pl.multiple_of(c * c_w + q * quart, quart), quart)
        return (a_f if ph == 0 else da_f).at[:, cols]

    def g_copy(ph, c, kind):
        ref = block(ph, c, xnb_q if kind == FW else own_q)
        target = {GX: xnb, GP: pair, FW: pair, DG: diag}[kind]
        kind = FW if kind == DG else kind
        return pltpu.make_async_remote_copy(
            src_ref=ref, dst_ref=ref, send_sem=sends.at[kind - 1], recv_sem=recvs.at[kind, c],
            device_id=target, device_id_type=MESH_ID,
        )

    def wait_sends(ph):
        src = xs if ph == 0 else xs2
        pltpu.make_async_remote_copy(
            src_ref=src, dst_ref=src, send_sem=sends.at[0], recv_sem=recvs.at[XRED, 0],
            device_id=xnb, device_id_type=MESH_ID,
        ).wait_send()
        whole = (a_f if ph == 0 else da_f).at[:, pl.ds(0, ff // 4)]
        for kind in (GX, GP, FW):
            pltpu.make_async_remote_copy(
                src_ref=whole, dst_ref=whole, send_sem=sends.at[kind - 1], recv_sem=recvs.at[kind, 0],
                device_id=xnb, device_id_type=MESH_ID,
            ).wait_send()
        for c in (nc - 2, nc - 1):
            pair_copy(ph, c).wait_send()

    f_parts = ((0, nc - LATE), (nc - LATE, LATE))

    def f_copy(n):
        first, count = f_parts[n % 2] if n < 4 else (0, nc)
        ref = fb.at[xnb_q if n in (2, 3) else own_q, pl.ds(first, count)]
        return pltpu.make_async_remote_copy(
            src_ref=ref, dst_ref=ref, send_sem=f_sem.at[n, 0], recv_sem=f_sem.at[n, 1],
            device_id=xnb if n < 2 else pair, device_id_type=MESH_ID,
        )

    own_cols = pl.ds(pl.multiple_of(xc * quart, quart), quart)
    oth_cols = pl.ds(pl.multiple_of((1 - xc) * quart, quart), quart)

    def pipeline(ph, partial, activate, consume):
        lag_pair, lag_act, lag_fwd, lag_dot = LAGS[ph]

        def direct(c):
            return c >= nc - DIRECT_LAST if ph == 0 else c < DIRECT_FIRST


        def reduce_pair(c):
            slot = lax.rem(c, 2)
            with jax.named_scope(f"pairwait{ph}"):
                pair_copy(ph, c).wait_recv()
            if ph == 0:
                xs[c] = (part[slot, core, :, :, oth_cols] + r1[c, :, :, oth_cols]).astype(BF)
                x_copy(ph, c).start()
                gu[c] = part[slot, core, :, :, own_cols] + r1[c, :, :, own_cols]
            else:
                xs2[c] = (part[slot, core, 0, :, oth_cols] + r2[c, :, oth_cols]).astype(BF)
                x_copy(ph, c).start()
                r2[c, :, own_cols] = part[slot, core, 0, :, own_cols] + r2[c, :, own_cols]

        def step(t, carry):
            if ph == 1:
                for n, when in enumerate(F_STEPS):

                    @pl.when(t == when)
                    def _():
                        f_copy(n).wait_recv()
                        f_copy(2 + n).start()

            if ph == 0:

                @pl.when(t == 0)
                def _():
                    for c in range(6, nc):
                        gu_load_start(c)

                @pl.when(t == 1)
                def _():
                    for i in range(qn):
                        wq_load(i).start()

                @pl.when(t == 2)
                def _():
                    wd_load.start()

                @pl.when((t >= QKV_AT) & (t < QKV_AT + qn))
                def _():
                    with jax.named_scope("qkv"):
                        qkv_step(t - QKV_AT)

                @pl.when(t == QKV_AT + qn - 1)
                def _():
                    y_copy(0).start()

            @pl.when(t < nc)
            def _():
                c = t

                @pl.when(c >= 2)
                def _():
                    pair_copy(ph, c - 2).wait_send()

                with jax.named_scope(f"part{ph}"):

                    @pl.when(c == 0)
                    def _():
                        partial(c, 1 - core)
                        pair_copy(ph, c).start()
                        partial(c, core)
                        reduce_pair(c)

                    @pl.when(c > 0)
                    def _():
                        partial(c, None)
                        pair_copy(ph, c).start()

            @pl.when((t > lag_pair) & (t < nc + lag_pair))
            def _():
                reduce_pair(t - lag_pair)

            @pl.when((t >= lag_act) & (t < nc + lag_act))
            def _():
                c = t - lag_act
                with jax.named_scope(f"xwait{ph}"):
                    x_copy(ph, c).wait_recv()
                with jax.named_scope(f"act{ph}"):
                    activate(c)
                g_copy(ph, c, GX).start()
                g_copy(ph, c, GP).start()

                @pl.when(direct(c))
                def _():
                    g_copy(ph, c, DG).start()

                if ph == 0:

                    @pl.when(c == nc - 1)
                    def _():
                        f_copy(0).start()

            @pl.when((t >= lag_fwd) & (t < nc + lag_fwd))
            def _():
                c = t - lag_fwd
                with jax.named_scope(f"gxwait{ph}"):
                    g_copy(ph, c, GX).wait_recv()

                @pl.when(jnp.logical_not(direct(c)))
                def _():
                    g_copy(ph, c, FW).start()

            @pl.when((t >= lag_dot) & (t < nc + lag_dot))
            def _():
                c = t - lag_dot
                with jax.named_scope(f"gpwait{ph}"):
                    g_copy(ph, c, GP).wait_recv()
                    g_copy(ph, c, FW).wait_recv()
                with jax.named_scope(f"dot{ph}"):
                    consume(c)

            return carry

        lax.fori_loop(0, nc + lag_dot, step, 0)

    def gu_partial(c, which):
        if which is not core:
            gu_load(0, c).wait()
            gu_load(1, c).wait()
        slot = lax.rem(c, 2)
        if which is None:
            prod = nn_dot(n1[...], wgu[:, pl.ds(pl.multiple_of(2 * c * c_w, 2 * c_w), 2 * c_w)])
            for i in range(2):
                part[slot, 0, i] = prod[:, i * c_w : i * c_w + half]
                part[slot, 1, i] = prod[:, i * c_w + half : (i + 1) * c_w]
        else:
            for i in range(2):
                cols = pl.ds(pl.multiple_of((2 * c + i) * c_w + which * half, half), half)
                part[slot, which, i] = nn_dot(n1[...], wgu[:, cols])

    def act_forward(c):
        gate = gu[c, 0] + xr[c, 0].astype(F32)
        up = gu[c, 1] + xr[c, 1].astype(F32)
        sig = jax.nn.sigmoid(gate)
        silu = gate * sig
        cols = pl.ds(pl.multiple_of(c * c_w + own_q * quart, quart), quart)
        a_f[:, cols] = (silu * up).astype(BF)
        fb[own_q, c, 0] = (up * sig * (1.0 + gate * (1.0 - sig))).astype(BF)
        fb[own_q, c, 1] = silu.astype(BF)

    def down_dot(c):
        @pl.when(c == 0)
        def _():
            wd_load.wait()

        rows = pl.ds(pl.multiple_of(c * c_w, c_w), c_w)

        @pl.when(c < nc - 1)
        def _():
            acc[...] += nn_dot(a_f[:, rows], wd[rows, :])

        @pl.when(c == nc - 1)
        def _():
            for j in range(YB):
                acc[:, y_cols(j)] += nn_dot(a_f[:, rows], wd[rows, y_cols(j)])
                y_send(1, j)


    pipeline(0, gu_partial, act_forward, down_dot)
    wait_sends(0)
    f_copy(4).start()
    a_out = load(a_f, a_o, out_sem.at[1])
    a_out.start()

    small[3].wait()
    small[4].wait()
    y_copy(0).wait()
    acc[...] = y32[0] + y32[1]
    sq_two = jnp.zeros((tok, 1), F32)
    dot_two = jnp.zeros((tok, 1), F32)
    for j in range(YB):
        cols = y_cols(j)
        x2_b = (x_s[:, cols].astype(F32) + y_sum(1, j)).astype(BF)
        x2_s[:, cols] = x2_b
        x2 = x2_b.astype(F32)
        sq_two += jnp.sum(x2 * x2, axis=-1, keepdims=True)
        dot_two += jnp.sum(g2[:, cols] * acc[:, cols] * x2, axis=-1, keepdims=True)
    stat_send(1, [sq_two, dot_two])
    f_copy(1).start()
    with jax.named_scope("stat1"):
        sq2, dot2 = stat_recv(1, 2)
    inv2 = lax.rsqrt(sq2 / d_model + NORM_EPS)
    x2 = x2_s[...].astype(F32)
    dz2 = inv2 * (g2[...] * acc[...]) - x2 * (inv2 * inv2 * inv2) * (dot2 / d_model)
    e_val = dx_s[...].astype(F32) + dz2
    e_s[...] = e_val
    eb[...] = e_val.astype(BF)
    n2[...] = (x2_s[...].astype(F32) * inv2 * g2[...]).astype(BF)
    dg_s[0:1, :] = jnp.sum(acc[...] * x2_s[...].astype(F32) * inv2, axis=0, keepdims=True)
    outs = [load(eb, eb_o, out_sem.at[2]), load(n2, n2_o, out_sem.at[3])]
    for cp in outs:
        cp.start()
    acc[...] = jnp.zeros_like(acc)

    def da_partial(c, which):
        slot = lax.rem(c, 2)
        if which is None:
            prod = nt_dot(eb[...], wd[pl.ds(pl.multiple_of(c * c_w, c_w), c_w), :])
            part[slot, 0, 0] = prod[:, :half]
            part[slot, 1, 0] = prod[:, half:]
        else:
            part[slot, which, 0] = nt_dot(eb[...], wd[pl.ds(pl.multiple_of(c * c_w + which * half, half), half), :])

    def act_backward(c):
        cols = pl.ds(pl.multiple_of(c * c_w + own_q * quart, quart), quart)
        da_f[:, cols] = (r2[c, :, own_cols] + xr2[c].astype(F32)).astype(BF)

    def dn1_dot(c):
        @pl.when(c == 0)
        def _():
            f_copy(4).wait_recv()
            f_copy(2).wait_recv()

        @pl.when(c == nc - LATE)
        def _():
            f_copy(3).wait_recv()

        for q in range(4):
            cols = pl.ds(pl.multiple_of(c * c_w + q * quart, quart), quart)
            d_act = da_f[:, cols].astype(F32)
            for i in range(2):
                dst = pl.ds(pl.multiple_of((2 * c + i) * c_w + q * quart, quart), quart)
                dgu_f[:, dst] = (d_act * fb[q, c, i].astype(F32)).astype(BF)
        cols = pl.ds(pl.multiple_of(2 * c * c_w, 2 * c_w), 2 * c_w)

        @pl.when(c < nc - 1)
        def _():
            acc[...] += nt_dot(dgu_f[:, cols], wgu[:, cols])

        @pl.when(c == nc - 1)
        def _():
            for j in range(YB):
                acc[:, y_cols(j)] += nt_dot(dgu_f[:, cols], wgu[y_cols(j), cols])
                y_send(2, j)

    pipeline(1, da_partial, act_backward, dn1_dot)
    dgu_out = load(dgu_f, dgu_o, out_sem.at[4])

    stat_send(2, [jnp.sum(g1[...] * acc[...] * x_s[...].astype(F32), axis=-1, keepdims=True)], PEERS)
    dgu_out.start()
    wait_sends(1)
    for n in range(5):
        f_copy(n).wait_send()
    for j in range(YB):
        acc[:, y_cols(j)] = y_sum(2, j)
    y_wait_send(1)
    y_wait_send(2)
    with jax.named_scope("fin0"):
      dg_s[1:2, :] = jnp.sum(acc[...] * x_s[...].astype(F32) * inv1, axis=0, keepdims=True)
    with jax.named_scope("stat2"):
        (dot1,) = stat_recv(2, 1, PEERS)
    with jax.named_scope("fin1"):
      dz1 = inv1 * (g1[...] * acc[...]) - x_s[...].astype(F32) * (inv1 * inv1 * inv1) * (dot1 / d_model)
      dxin_s[...] = (e_s[...] + dz1).astype(BF)
    tail = [
        load(dxin_s, dxin_o, out_sem.at[5]),
        load(dg_s, dg_o, out_sem.at[6]),
    ]
    for cp in tail:
        cp.start()
    with jax.named_scope("fin2"):
      for cp in (n1_out, a_out, *outs, dgu_out, *tail):
        cp.wait()


def comm_call(x_in, gain_one, gain_two, w_gate, w_up, w_down, w_qkv, dx_out, d_qkv):
    tok, hd = x_in.shape
    ff = w_gate.shape[1]
    qw = w_qkv.shape[1]
    nc = ff // CHUNK
    half, quart = CHUNK // 2, CHUNK // 4
    out = lambda shape, dtype: jax.ShapeDtypeStruct(shape, dtype)
    vm = lambda *shape_dtype: pltpu.VMEM(shape_dtype[:-1], shape_dtype[-1])
    dma = pltpu.SemaphoreType.DMA
    return pl.pallas_call(
        functools.partial(comm_kernel, (tok, hd, ff, qw)),
        out_shape=(
            out((tok, hd), BF), out((tok, hd), BF), out((tok, hd), BF), out((tok, ff), BF), out((tok, 2 * ff), BF),
            out((tok, hd), BF), out((8, hd), F32),
        ),
        in_specs=[ANY] * 9,
        out_specs=[ANY] * 7,
        scratch_shapes=[
            vm(hd, 2 * ff, BF), vm(ff, hd, BF), vm(hd, qw, BF), vm(tok, qw, BF),
            vm(tok, hd, BF), vm(tok, hd, BF), vm(1, hd, F32), vm(1, hd, F32),
            vm(tok, hd, BF), vm(tok, hd, BF), vm(tok, hd, BF), vm(tok, hd, F32), vm(tok, hd, BF),
            vm(tok, hd, F32), vm(2, 2, 2, tok, half, F32), vm(nc, 2, tok, half, F32), vm(nc, tok, half, F32),
            vm(nc, 2, tok, quart, BF), vm(nc, 2, tok, quart, BF), vm(nc, tok, quart, BF), vm(nc, tok, quart, BF),
            vm(nc, 2, tok, quart, F32), vm(4, nc, 2, tok, quart, BF), vm(tok, ff, BF), vm(tok, ff, BF), vm(tok, 2 * ff, BF),
            vm(2, tok, hd, F32), vm(2, tok, hd, BF), vm(2, tok, hd, BF), vm(3, 8, 128, F32), vm(3, 8, 8, 128, F32),
            vm(tok, hd, BF), vm(8, hd, F32),
            dma((6,)), dma((2, nc)), dma((qw // 1024,)), dma((7,)), dma((3, 2)), dma((3, YB + 1)), dma((5, nc)), dma((6,)), dma((5, 2)),
        ],
        compiler_params=pltpu.CompilerParams(
            collective_id=0, has_side_effects=True, vmem_limit_bytes=VMEM_LIMIT
        ),
        name="block_comm",
    )(x_in, gain_one, gain_two, w_gate, w_up, w_down, w_qkv, dx_out, d_qkv)


TILE = CHUNK
SLOTS = 2


def grad_kernel(
    dims, n1_h, n2_h, eb_h, a_h, dgu_h, dq_h, dx_h, dg_h,
    dwg_o, dwu_o, dwd_o, dwq_o, dx_o, dg1_o, dg2_o,
    n1, n2, eb, a_f, dgu, dq, dx, dg, n1_t, n2_t, bq, bg, bu, bd, ld, sem,
):
    hd, ff, qw = dims
    nt, nq = ff // TILE, qw // TILE
    pairs = ((n2_h, n2), (dq_h, dq), (eb_h, eb), (a_h, a_f), (n1_h, n1), (dgu_h, dgu), (dx_h, dx), (dg_h, dg))
    loads = [pltpu.make_async_copy(src, dst, ld.at[i]) for i, (src, dst) in enumerate(pairs)]
    for cp in loads:
        cp.start()

    def cols_of(i):
        return pl.ds(pl.multiple_of(i * TILE, TILE), TILE)

    def out_copy(kind, i):
        slot = lax.rem(i, SLOTS)
        src = (bq, bg, bu, bd)[kind].at[slot]
        dst = (dwq_o, dwg_o, dwu_o, dwd_o)[kind]
        return pltpu.make_async_copy(src, dst.at[cols_of(i), :] if kind == 3 else dst.at[:, cols_of(i)], sem.at[kind, slot])

    with jax.named_scope("b_in0"):
      loads[0].wait()
      loads[1].wait()
    with jax.named_scope("b_t"):
      n2_t[...] = n2[...].T

    def q_step(i, carry):
        @pl.when(i >= SLOTS)
        def _():
            out_copy(0, i - SLOTS).wait()

        bq[lax.rem(i, SLOTS)] = nn_dot(n2_t[...], dq[:, cols_of(i)]).astype(BF)
        out_copy(0, i).start()
        return carry

    with jax.named_scope("b_q"):
      lax.fori_loop(0, nq, q_step, 0)
    with jax.named_scope("b_in1"):
      for cp in loads[2:]:
        cp.wait()
    finals = [
        pltpu.make_async_copy(dx, dx_o, ld.at[0]),
        pltpu.make_async_copy(dg.at[0:1, :], dg2_o, ld.at[1]),
        pltpu.make_async_copy(dg.at[1:2, :], dg1_o, ld.at[2]),
    ]
    for cp in finals:
        cp.start()
    n1_t[...] = n1[...].T

    def step(i, carry):
        slot = lax.rem(i, SLOTS)

        with jax.named_scope("b_wait"):
          @pl.when(i >= SLOTS)
          def _():
            for kind in (1, 2, 3):
                out_copy(kind, i - SLOTS).wait()

        bd[slot] = nn_dot(a_f[:, cols_of(i)].T, eb[...]).astype(BF)
        out_copy(3, i).start()
        bg[slot] = nn_dot(n1_t[...], dgu[:, cols_of(2 * i)]).astype(BF)
        out_copy(1, i).start()
        bu[slot] = nn_dot(n1_t[...], dgu[:, cols_of(2 * i + 1)]).astype(BF)
        out_copy(2, i).start()
        return carry

    lax.fori_loop(0, nt, step, 0)
    for cp in finals:
        cp.wait()
    with jax.named_scope("b_end"):
     for i in range(nq - SLOTS, nq):
        out_copy(0, i).wait()
     for i in range(nt - SLOTS, nt):
        for kind in (1, 2, 3):
            out_copy(kind, i).wait()


def grad_call(n1, n2, eb, a_full, dgu, d_qkv, dx_in, dg):
    tok, hd = n1.shape
    ff, qw = a_full.shape[1], d_qkv.shape[1]
    out = lambda *shape: jax.ShapeDtypeStruct(shape, BF)
    vm = lambda *shape: pltpu.VMEM(shape, BF)
    return pl.pallas_call(
        functools.partial(grad_kernel, (hd, ff, qw)),
        out_shape=(
            out(hd, ff), out(hd, ff), out(ff, hd), out(hd, qw),
            out(tok, hd), jax.ShapeDtypeStruct((1, hd), F32), jax.ShapeDtypeStruct((1, hd), F32),
        ),
        in_specs=[ANY] * 8,
        out_specs=[ANY] * 7,
        scratch_shapes=[
            vm(tok, hd), vm(tok, hd), vm(tok, hd), vm(tok, ff), vm(tok, 2 * ff), vm(tok, qw), vm(tok, hd), pltpu.VMEM((8, hd), F32), vm(hd, tok), vm(hd, tok),
            vm(SLOTS, hd, TILE), vm(SLOTS, hd, TILE), vm(SLOTS, hd, TILE), vm(SLOTS, TILE, hd),
            pltpu.SemaphoreType.DMA((8,)), pltpu.SemaphoreType.DMA((4, SLOTS)),
        ],
        compiler_params=pltpu.CompilerParams(vmem_limit_bytes=VMEM_LIMIT),
        name="weight_grads",
    )(n1, n2, eb, a_full, dgu, d_qkv, dx_in, dg)


def solution(mesh):
    def local_step(x_in, gain_one, gain_two, w_gate, w_up, w_down, w_qkv, dx_out, d_qkv):
        hd = x_in.shape[1]
        n1, n2, eb, a_full, dgu, dx_in, dg = comm_call(
            x_in, gain_one.reshape(1, hd), gain_two.reshape(1, hd), w_gate, w_up, w_down, w_qkv, dx_out, d_qkv
        )
        dw_gate, dw_up, dw_down, dw_qkv, dx_in, dg1, dg2 = grad_call(
            n1, n2, eb, a_full, dgu, d_qkv, dx_in, dg
        )
        return dx_in, dw_gate, dw_up, dw_down, dw_qkv, dg1.reshape(hd), dg2.reshape(hd)

    tok_spec = P("data", "hid")
    in_specs = (tok_spec, P("hid"), P("hid"), P("hid", "ffn"), P("hid", "ffn"), P("ffn", "hid"), P("hid", "ffn"), tok_spec, P("data", "ffn"))
    out_specs = (tok_spec, P(("data", "hid"), "ffn"), P(("data", "hid"), "ffn"), P(("data", "ffn"), "hid"), P(("data", "hid"), "ffn"), P(("data", "hid")), P(("data", "hid")))
    return jax.shard_map(local_step, mesh=mesh, in_specs=in_specs, out_specs=out_specs, check_vma=False)
```

```python
import functools

import jax
import jax.numpy as jnp
from jax import lax
from jax.experimental import pallas as pl
from jax.experimental.pallas import tpu as pltpu
from jax.sharding import PartitionSpec as P

NORM_EPS = 1e-6
BF = jnp.bfloat16
F32 = jnp.float32
MESH_ID = pl.DeviceIdType.MESH
ANY = pl.BlockSpec(memory_space=pl.ANY)
VMEM_LIMIT = 67043328

CHUNK = 1024
LATE = 2
YB = 2
F_STEPS = (0, 3)
QKV_AT = 7
DIRECT_LAST = 1
DIRECT_FIRST = 0
LAGS = ((1, 5, 9, 10), (1, 3, 5, 6))

PAIR, XRED, GX, GP, FW, DG = range(6)

PEERS = tuple((dy, j) for dy in range(2) for j in range(4) if dy or j)
ROW_PEERS = PEERS[:3]


def nn_dot(a_mat, b_mat):
    return jnp.dot(a_mat, b_mat, preferred_element_type=F32)


def nt_dot(a_mat, b_mat):
    return lax.dot_general(a_mat, b_mat, (((1,), (1,)), ((), ())), preferred_element_type=F32)


def pack_stats(cols):
    tok = cols[0].shape[0]
    lane = lax.broadcasted_iota(jnp.int32, (tok, 128), 1)
    wide = jnp.zeros((tok, 128), F32)
    for i, col in enumerate(cols):
        wide = jnp.where(lane == i, col, wide)
    full = jnp.concatenate([wide, jnp.zeros((128 - tok, 128), F32)], axis=0)
    return full.T[0:8, :]


def unpack_stats(tile, tok, count):
    full = jnp.concatenate([tile, jnp.zeros((120, 128), F32)], axis=0).T
    return [full[0:tok, i : i + 1] for i in range(count)]


def comm_kernel(
    dims,
    x_h, g1_h, g2_h, wg_h, wu_h, wd_h, wq_h, dx_h, dq_h,
    n1_o, n2_o, eb_o, a_o, dgu_o, dxin_o, dg_o,
    wgu, wd, wq, dq, x_s, dx_s, g1, g2, n1, n2, eb, e_s, x2_s,
    acc, part, r1, r2, xs, xr, xs2, xr2, gu, fb, a_f, da_f, dgu_f, y32, ys, yr, st_s, st_r, dxin_s, dg_s,
    ld, wld, qld, st_sem, y_sem, recvs, sends, f_sem,
):
    tok, hd, ff, qw = dims
    c_w = CHUNK
    nc = ff // c_w
    half = c_w // 2
    quart = c_w // 4
    d_model = hd * 4
    zc, yc, h = lax.axis_index("data"), lax.axis_index("ffn"), lax.axis_index("hid")
    xc = h // 2
    core = lax.rem(h, 2)
    pair = (zc, yc, xc * 2 + 1 - core)
    xnb = (zc, yc, (1 - xc) * 2 + core)
    diag = (zc, yc, 3 - h)
    ynb = (zc, 1 - yc, h)

    def peer(dy, j):
        return (zc, lax.rem(yc + dy, 2), lax.rem(h + j, 4))


    def load(src, dst, sem):
        return pltpu.make_async_copy(src, dst, sem)

    small = [
        load(x_h, x_s, ld.at[0]), load(g1_h, g1, ld.at[1]), load(dq_h, dq, ld.at[2]),
        load(g2_h, g2, ld.at[3]), load(dx_h, dx_s, ld.at[4]),
    ]
    qn = qw // 1024

    wq_load = load(wq_h, wq, qld.at[0])

    def gu_load(i, c):
        src = (wg_h, wu_h)[i].at[:, pl.ds(pl.multiple_of(c * c_w, c_w), c_w)]
        dst = wgu.at[:, pl.ds(pl.multiple_of((2 * c + i) * c_w, c_w), c_w)]
        return load(src, dst, wld.at[c])

    def gu_wait(c):
        both = wgu.at[:, pl.ds(pl.multiple_of(2 * c * c_w, 2 * c_w), 2 * c_w)]
        load(wg_h.at[:, pl.ds(0, 2 * c_w)], both, wld.at[c]).wait()

    wd_load = load(wd_h, wd, ld.at[5])

    def gu_load_start(n):
        gu_load(0, n).start()
        gu_load(1, n).start()

    for cp in small:
        cp.start()

    bar = pltpu.get_barrier_semaphore()
    for dy, j in PEERS[:4]:
        pl.semaphore_signal(bar, inc=1, device_id=peer(dy, j), device_id_type=MESH_ID)
    small[0].wait()
    gu_load_start(0)
    gu_load_start(1)
    x_f = x_s[...].astype(F32)
    sq_part = jnp.sum(x_f * x_f, axis=-1, keepdims=True)

    def qkv_step(i):
        @pl.when(i == 0)
        def _():
            wq_load.wait()

        cols = pl.ds(pl.multiple_of(i * 1024, 1024), 1024)
        y32[0] += nt_dot(dq[:, cols], wq[:, cols])

    y32[0] = jnp.zeros((tok, hd), F32)
    with jax.named_scope("barrier"):
        pl.semaphore_wait(bar, 4)

    def stat_copy(n, i):
        return pltpu.make_async_remote_copy(
            src_ref=st_s.at[n], dst_ref=st_r.at[n, yc * 4 + h], send_sem=st_sem.at[n, 0], recv_sem=st_sem.at[n, 1],
            device_id=peer(*PEERS[i]), device_id_type=MESH_ID,
        )

    def stat_send(n, cols, peers=ROW_PEERS):
        tile = pack_stats(cols)
        st_s[n] = tile
        st_r[n, yc * 4 + h] = tile
        for i in range(len(peers)):
            stat_copy(n, i).start()

    def stat_recv(n, count, peers=ROW_PEERS):
        all_tiles = st_r.at[n, pl.ds(0, len(peers))]
        whole = pltpu.make_async_remote_copy(
            src_ref=all_tiles, dst_ref=all_tiles, send_sem=st_sem.at[n, 0], recv_sem=st_sem.at[n, 1],
            device_id=peer(*PEERS[0]), device_id_type=MESH_ID,
        )
        whole.wait()
        total = jnp.zeros((8, 128), F32)
        for i in range(len(peers) + 1):
            total += st_r[n, i] if peers is PEERS else st_r[n, yc * 4 + i]
        return unpack_stats(total, tok, count)

    yb = hd // YB

    def y_cols(j):
        return pl.ds(j * yb, yb)

    def y_copy(n, j=0):
        if n == 0:
            src, dst = y32.at[0], y32.at[1]
        else:
            src, dst = ys.at[n - 1, :, y_cols(j)], yr.at[n - 1, :, y_cols(j)]
        return pltpu.make_async_remote_copy(
            src_ref=src, dst_ref=dst, send_sem=y_sem.at[n, YB], recv_sem=y_sem.at[n, j],
            device_id=ynb, device_id_type=MESH_ID,
        )

    def y_send(n, j):
        ys[n - 1, :, y_cols(j)] = acc[:, y_cols(j)].astype(BF)
        y_copy(n, j).start()

    def y_sum(n, j):
        with jax.named_scope(f"ywait{n}"):
            y_copy(n, j).wait_recv()
        return ys[n - 1, :, y_cols(j)].astype(F32) + yr[n - 1, :, y_cols(j)].astype(F32)

    def y_wait_send(n):
        whole = ys.at[n - 1]
        pltpu.make_async_remote_copy(
            src_ref=whole, dst_ref=whole, send_sem=y_sem.at[n, YB], recv_sem=y_sem.at[n, 0],
            device_id=ynb, device_id_type=MESH_ID,
        ).wait_send()

    stat_send(0, [sq_part])
    gu_load_start(2)
    gu_load_start(3)
    small[2].wait()
    small[1].wait()
    with jax.named_scope("stat0"):
        (sq,) = stat_recv(0, 1)
    gu_load_start(4)
    gu_load_start(5)
    inv1 = lax.rsqrt(sq / d_model + NORM_EPS)
    n1[...] = (x_s[...].astype(F32) * inv1 * g1[...]).astype(BF)
    n1_out = load(n1, n1_o, ld.at[0])
    n1_out.start()
    acc[...] = jnp.zeros_like(acc)

    def pair_copy(ph, c):
        slot = lax.rem(c, 2)
        src = part.at[slot, 1 - core] if ph == 0 else part.at[slot, 1 - core, 0]
        return pltpu.make_async_remote_copy(
            src_ref=src, dst_ref=(r1 if ph == 0 else r2).at[c],
            send_sem=sends.at[4 + slot], recv_sem=recvs.at[PAIR, c],
            device_id=pair, device_id_type=MESH_ID,
        )

    def x_copy(ph, c):
        src, dst = ((xs, xr), (xs2, xr2))[ph]
        return pltpu.make_async_remote_copy(
            src_ref=src.at[c], dst_ref=dst.at[c],
            send_sem=sends.at[0], recv_sem=recvs.at[XRED, c],
            device_id=xnb, device_id_type=MESH_ID,
        )

    own_q = core * 2 + xc
    xnb_q = core * 2 + 1 - xc

    def block(ph, c, q):
        cols = pl.ds(pl.multiple_of(c * c_w + q * quart, quart), quart)
        return (a_f if ph == 0 else da_f).at[:, cols]

    def g_copy(ph, c, kind):
        ref = block(ph, c, xnb_q if kind == FW else own_q)
        target = {GX: xnb, GP: pair, FW: pair, DG: diag}[kind]
        kind = FW if kind == DG else kind
        return pltpu.make_async_remote_copy(
            src_ref=ref, dst_ref=ref, send_sem=sends.at[kind - 1], recv_sem=recvs.at[kind, c],
            device_id=target, device_id_type=MESH_ID,
        )

    def wait_sends(ph):
        src = xs if ph == 0 else xs2
        pltpu.make_async_remote_copy(
            src_ref=src, dst_ref=src, send_sem=sends.at[0], recv_sem=recvs.at[XRED, 0],
            device_id=xnb, device_id_type=MESH_ID,
        ).wait_send()
        whole = (a_f if ph == 0 else da_f).at[:, pl.ds(0, ff // 4)]
        for kind in (GX, GP, FW):
            pltpu.make_async_remote_copy(
                src_ref=whole, dst_ref=whole, send_sem=sends.at[kind - 1], recv_sem=recvs.at[kind, 0],
                device_id=xnb, device_id_type=MESH_ID,
            ).wait_send()
        for c in (nc - 2, nc - 1):
            pair_copy(ph, c).wait_send()

    f_parts = ((0, nc - LATE), (nc - LATE, LATE))

    def f_copy(n):
        first, count = f_parts[n % 2] if n < 4 else (0, nc)
        ref = fb.at[xnb_q if n in (2, 3) else own_q, pl.ds(first, count)]
        return pltpu.make_async_remote_copy(
            src_ref=ref, dst_ref=ref, send_sem=f_sem.at[5], recv_sem=f_sem.at[n],
            device_id=xnb if n < 2 else pair, device_id_type=MESH_ID,
        )

    own_cols = pl.ds(pl.multiple_of(xc * quart, quart), quart)
    oth_cols = pl.ds(pl.multiple_of((1 - xc) * quart, quart), quart)

    def pipeline(ph, partial, activate, consume):
        lag_pair, lag_act, lag_fwd, lag_dot = LAGS[ph]

        def direct(c):
            return c >= nc - DIRECT_LAST if ph == 0 else c < DIRECT_FIRST

        def reduce_pair(c):
            slot = lax.rem(c, 2)
            with jax.named_scope(f"pairwait{ph}"):
                pair_copy(ph, c).wait_recv()
            if ph == 0:
                xs[c] = (part[slot, core, :, :, oth_cols] + r1[c, :, :, oth_cols]).astype(BF)
                x_copy(ph, c).start()
                gu[c] = part[slot, core, :, :, own_cols] + r1[c, :, :, own_cols]
            else:
                xs2[c] = (part[slot, core, 0, :, oth_cols] + r2[c, :, oth_cols]).astype(BF)
                x_copy(ph, c).start()
                r2[c, :, own_cols] = part[slot, core, 0, :, own_cols] + r2[c, :, own_cols]

        def step(t, carry):
            if ph == 1:
                for n, when in enumerate(F_STEPS):

                    @pl.when(t == when)
                    def _():
                        f_copy(n).wait_recv()
                        f_copy(2 + n).start()

            if ph == 0:

                @pl.when(t == 0)
                def _():
                    for c in range(6, nc):
                        gu_load_start(c)

                @pl.when(t == 1)
                def _():
                    wq_load.start()

                @pl.when(t == 2)
                def _():
                    wd_load.start()

                @pl.when((t >= QKV_AT) & (t < QKV_AT + qn))
                def _():
                    with jax.named_scope("qkv"):
                        qkv_step(t - QKV_AT)

                @pl.when(t == QKV_AT + qn - 1)
                def _():
                    y_copy(0).start()

            @pl.when(t < nc)
            def _():
                c = t

                @pl.when(c >= 2)
                def _():
                    pair_copy(ph, c - 2).wait_send()

                with jax.named_scope(f"part{ph}"):

                    @pl.when(c == 0)
                    def _():
                        partial(c, 1 - core)
                        pair_copy(ph, c).start()
                        partial(c, core)
                        reduce_pair(c)

                    @pl.when(c > 0)
                    def _():
                        partial(c, None)
                        pair_copy(ph, c).start()

            @pl.when((t > lag_pair) & (t < nc + lag_pair))
            def _():
                reduce_pair(t - lag_pair)

            @pl.when((t >= lag_act) & (t < nc + lag_act))
            def _():
                c = t - lag_act
                with jax.named_scope(f"xwait{ph}"):
                    x_copy(ph, c).wait_recv()
                with jax.named_scope(f"act{ph}"):
                    activate(c)
                g_copy(ph, c, GX).start()
                g_copy(ph, c, GP).start()

                @pl.when(direct(c))
                def _():
                    g_copy(ph, c, DG).start()

                if ph == 0:

                    @pl.when(c == nc - 1)
                    def _():
                        f_copy(0).start()

            @pl.when((t >= lag_fwd) & (t < nc + lag_fwd))
            def _():
                c = t - lag_fwd
                with jax.named_scope(f"gxwait{ph}"):
                    g_copy(ph, c, GX).wait_recv()

                @pl.when(jnp.logical_not(direct(c)))
                def _():
                    g_copy(ph, c, FW).start()

            @pl.when((t >= lag_dot) & (t < nc + lag_dot))
            def _():
                c = t - lag_dot
                with jax.named_scope(f"gpwait{ph}"):
                    g_copy(ph, c, GP).wait_recv()
                    g_copy(ph, c, FW).wait_recv()
                with jax.named_scope(f"dot{ph}"):
                    consume(c)

            return carry

        lax.fori_loop(0, nc + lag_dot, step, 0)

    def gu_partial(c, which):
        if which is not core:
            gu_wait(c)
        slot = lax.rem(c, 2)
        if which is None:
            prod = nn_dot(n1[...], wgu[:, pl.ds(pl.multiple_of(2 * c * c_w, 2 * c_w), 2 * c_w)])
            for i in range(2):
                part[slot, 0, i] = prod[:, i * c_w : i * c_w + half]
                part[slot, 1, i] = prod[:, i * c_w + half : (i + 1) * c_w]
        else:
            for i in range(2):
                cols = pl.ds(pl.multiple_of((2 * c + i) * c_w + which * half, half), half)
                part[slot, which, i] = nn_dot(n1[...], wgu[:, cols])

    def act_forward(c):
        gate = gu[c, 0] + xr[c, 0].astype(F32)
        up = gu[c, 1] + xr[c, 1].astype(F32)
        sig = jax.nn.sigmoid(gate)
        silu = gate * sig
        cols = pl.ds(pl.multiple_of(c * c_w + own_q * quart, quart), quart)
        a_f[:, cols] = (silu * up).astype(BF)
        fb[own_q, c, 0] = (up * sig * (1.0 + gate * (1.0 - sig))).astype(BF)
        fb[own_q, c, 1] = silu.astype(BF)

    def down_dot(c):
        @pl.when(c == 0)
        def _():
            wd_load.wait()

        rows = pl.ds(pl.multiple_of(c * c_w, c_w), c_w)

        @pl.when(c < nc - 1)
        def _():
            acc[...] += nn_dot(a_f[:, rows], wd[rows, :])

        @pl.when(c == nc - 1)
        def _():
            for j in range(YB):
                acc[:, y_cols(j)] += nn_dot(a_f[:, rows], wd[rows, y_cols(j)])
                y_send(1, j)


    pipeline(0, gu_partial, act_forward, down_dot)
    wait_sends(0)
    f_copy(4).start()
    a_out = load(a_f, a_o, ld.at[1])
    a_out.start()

    small[3].wait()
    small[4].wait()
    y_copy(0).wait()
    acc[...] = y32[0] + y32[1]
    sq_two = jnp.zeros((tok, 1), F32)
    dot_two = jnp.zeros((tok, 1), F32)
    for j in range(YB):
        cols = y_cols(j)
        x2_b = (x_s[:, cols].astype(F32) + y_sum(1, j)).astype(BF)
        x2_s[:, cols] = x2_b
        x2 = x2_b.astype(F32)
        sq_two += jnp.sum(x2 * x2, axis=-1, keepdims=True)
        dot_two += jnp.sum(g2[:, cols] * acc[:, cols] * x2, axis=-1, keepdims=True)
    stat_send(1, [sq_two, dot_two])
    f_copy(1).start()
    with jax.named_scope("stat1"):
        sq2, dot2 = stat_recv(1, 2)
    inv2 = lax.rsqrt(sq2 / d_model + NORM_EPS)
    x2 = x2_s[...].astype(F32)
    dz2 = inv2 * (g2[...] * acc[...]) - x2 * (inv2 * inv2 * inv2) * (dot2 / d_model)
    e_val = dx_s[...].astype(F32) + dz2
    e_s[...] = e_val
    eb[...] = e_val.astype(BF)
    n2[...] = (x2_s[...].astype(F32) * inv2 * g2[...]).astype(BF)
    dg_s[0:1, :] = jnp.sum(acc[...] * x2_s[...].astype(F32) * inv2, axis=0, keepdims=True)
    outs = [load(eb, eb_o, ld.at[2]), load(n2, n2_o, ld.at[3])]
    for cp in outs:
        cp.start()
    acc[...] = jnp.zeros_like(acc)

    def da_partial(c, which):
        slot = lax.rem(c, 2)
        if which is None:
            prod = nt_dot(eb[...], wd[pl.ds(pl.multiple_of(c * c_w, c_w), c_w), :])
            part[slot, 0, 0] = prod[:, :half]
            part[slot, 1, 0] = prod[:, half:]
        else:
            part[slot, which, 0] = nt_dot(eb[...], wd[pl.ds(pl.multiple_of(c * c_w + which * half, half), half), :])

    def act_backward(c):
        cols = pl.ds(pl.multiple_of(c * c_w + own_q * quart, quart), quart)
        da_f[:, cols] = (r2[c, :, own_cols] + xr2[c].astype(F32)).astype(BF)

    def dn1_dot(c):
        @pl.when(c == 0)
        def _():
            f_copy(4).wait_recv()
            f_copy(2).wait_recv()

        @pl.when(c == nc - LATE)
        def _():
            f_copy(3).wait_recv()

        for q in range(4):
            cols = pl.ds(pl.multiple_of(c * c_w + q * quart, quart), quart)
            d_act = da_f[:, cols].astype(F32)
            for i in range(2):
                dst = pl.ds(pl.multiple_of((2 * c + i) * c_w + q * quart, quart), quart)
                dgu_f[:, dst] = (d_act * fb[q, c, i].astype(F32)).astype(BF)
        cols = pl.ds(pl.multiple_of(2 * c * c_w, 2 * c_w), 2 * c_w)

        @pl.when(c < nc - 1)
        def _():
            acc[...] += nt_dot(dgu_f[:, cols], wgu[:, cols])

        @pl.when(c == nc - 1)
        def _():
            for j in range(YB):
                acc[:, y_cols(j)] += nt_dot(dgu_f[:, cols], wgu[y_cols(j), cols])
                y_send(2, j)

    pipeline(1, da_partial, act_backward, dn1_dot)
    dgu_out = load(dgu_f, dgu_o, ld.at[4])

    stat_send(2, [jnp.sum(g1[...] * acc[...] * x_s[...].astype(F32), axis=-1, keepdims=True)], PEERS)
    dgu_out.start()
    wait_sends(1)
    sent = fb.at[pl.ds(0, 3)]
    pltpu.make_async_remote_copy(
        src_ref=sent, dst_ref=sent, send_sem=f_sem.at[5], recv_sem=f_sem.at[0], device_id=pair, device_id_type=MESH_ID
    ).wait_send()
    for j in range(YB):
        acc[:, y_cols(j)] = y_sum(2, j)
    y_wait_send(1)
    y_wait_send(2)
    dg_s[1:2, :] = jnp.sum(acc[...] * x_s[...].astype(F32) * inv1, axis=0, keepdims=True)
    with jax.named_scope("stat2"):
        (dot1,) = stat_recv(2, 1, PEERS)
    dz1 = inv1 * (g1[...] * acc[...]) - x_s[...].astype(F32) * (inv1 * inv1 * inv1) * (dot1 / d_model)
    dxin_s[...] = (e_s[...] + dz1).astype(BF)
    tail = [
        load(dxin_s, dxin_o, ld.at[5]),
        load(dg_s, dg_o, qld.at[0]),
    ]
    for cp in tail:
        cp.start()
    for cp in (n1_out, a_out, *outs, dgu_out, *tail):
        cp.wait()


def comm_call(x_in, gain_one, gain_two, w_gate, w_up, w_down, w_qkv, dx_out, d_qkv):
    tok, hd = x_in.shape
    ff = w_gate.shape[1]
    qw = w_qkv.shape[1]
    nc = ff // CHUNK
    half, quart = CHUNK // 2, CHUNK // 4
    out = lambda shape, dtype: jax.ShapeDtypeStruct(shape, dtype)
    vm = lambda *shape_dtype: pltpu.VMEM(shape_dtype[:-1], shape_dtype[-1])
    dma = pltpu.SemaphoreType.DMA
    return pl.pallas_call(
        functools.partial(comm_kernel, (tok, hd, ff, qw)),
        out_shape=(
            out((tok, hd), BF), out((tok, hd), BF), out((tok, hd), BF), out((tok, ff), BF), out((tok, 2 * ff), BF),
            out((tok, hd), BF), out((8, hd), F32),
        ),
        in_specs=[ANY] * 9,
        out_specs=[ANY] * 7,
        scratch_shapes=[
            vm(hd, 2 * ff, BF), vm(ff, hd, BF), vm(hd, qw, BF), vm(tok, qw, BF),
            vm(tok, hd, BF), vm(tok, hd, BF), vm(1, hd, F32), vm(1, hd, F32),
            vm(tok, hd, BF), vm(tok, hd, BF), vm(tok, hd, BF), vm(tok, hd, F32), vm(tok, hd, BF),
            vm(tok, hd, F32), vm(2, 2, 2, tok, half, F32), vm(nc, 2, tok, half, F32), vm(nc, tok, half, F32),
            vm(nc, 2, tok, quart, BF), vm(nc, 2, tok, quart, BF), vm(nc, tok, quart, BF), vm(nc, tok, quart, BF),
            vm(nc, 2, tok, quart, F32), vm(4, nc, 2, tok, quart, BF), vm(tok, ff, BF), vm(tok, ff, BF), vm(tok, 2 * ff, BF),
            vm(2, tok, hd, F32), vm(2, tok, hd, BF), vm(2, tok, hd, BF), vm(3, 8, 128, F32), vm(3, 8, 8, 128, F32),
            vm(tok, hd, BF), vm(8, hd, F32),
            dma((6,)), dma((nc,)), dma((1,)), dma((3, 2)), dma((3, YB + 1)), dma((5, nc)), dma((6,)), dma((6,)),
        ],
        compiler_params=pltpu.CompilerParams(
            collective_id=0, has_side_effects=True, vmem_limit_bytes=VMEM_LIMIT
        ),
        name="block_comm",
    )(x_in, gain_one, gain_two, w_gate, w_up, w_down, w_qkv, dx_out, d_qkv)


TILE = CHUNK
SLOTS = 3


def grad_kernel(
    dims, n1_h, n2_h, eb_h, a_h, dgu_h, dq_h, dx_h, dg_h,
    dwg_o, dwu_o, dwd_o, dwq_o, dx_o, dg1_o, dg2_o,
    n1, n2, eb, a_f, dgu, dq, dx, dg, n1_t, n2_t, bq, bg, bu, bd, ld, sem,
):
    hd, ff, qw = dims
    nt, nq = ff // TILE, qw // TILE
    pairs = ((n2_h, n2), (dq_h, dq), (eb_h, eb), (a_h, a_f), (n1_h, n1), (dgu_h, dgu), (dx_h, dx), (dg_h, dg))
    loads = [pltpu.make_async_copy(src, dst, ld.at[i]) for i, (src, dst) in enumerate(pairs)]
    for cp in loads:
        cp.start()

    def cols_of(i):
        return pl.ds(pl.multiple_of(i * TILE, TILE), TILE)

    def out_copy(kind, i):
        slot = lax.rem(i, SLOTS)
        src = (bq, bg, bu, bd)[kind].at[slot]
        dst = (dwq_o, dwg_o, dwu_o, dwd_o)[kind]
        return pltpu.make_async_copy(src, dst.at[cols_of(i), :] if kind == 3 else dst.at[:, cols_of(i)], sem.at[kind, slot])

    with jax.named_scope("b_in0"):
      loads[0].wait()
      loads[1].wait()
    with jax.named_scope("b_t"):
      n2_t[...] = n2[...].T

    def q_step(i, carry):
        @pl.when(i >= SLOTS)
        def _():
            out_copy(0, i - SLOTS).wait()

        bq[lax.rem(i, SLOTS)] = nn_dot(n2_t[...], dq[:, cols_of(i)]).astype(BF)
        out_copy(0, i).start()
        return carry

    with jax.named_scope("b_q"):
      lax.fori_loop(0, nq, q_step, 0)
    with jax.named_scope("b_in1"):
      for cp in loads[2:]:
        cp.wait()
    finals = [
        pltpu.make_async_copy(dx, dx_o, ld.at[0]),
        pltpu.make_async_copy(dg.at[0:1, :], dg2_o, ld.at[1]),
        pltpu.make_async_copy(dg.at[1:2, :], dg1_o, ld.at[2]),
    ]
    for cp in finals:
        cp.start()
    n1_t[...] = n1[...].T

    def step(i, carry):
        slot = lax.rem(i, SLOTS)

        @pl.when(i >= SLOTS)
        def _():
            for kind in (1, 2, 3):
                out_copy(kind, i - SLOTS).wait()

        bd[slot] = nn_dot(a_f[:, cols_of(i)].T, eb[...]).astype(BF)
        out_copy(3, i).start()
        bg[slot] = nn_dot(n1_t[...], dgu[:, cols_of(2 * i)]).astype(BF)
        out_copy(1, i).start()
        bu[slot] = nn_dot(n1_t[...], dgu[:, cols_of(2 * i + 1)]).astype(BF)
        out_copy(2, i).start()
        return carry

    lax.fori_loop(0, nt, step, 0)
    for cp in finals:
        cp.wait()
    for i in range(max(nq - SLOTS, 0), nq):
        out_copy(0, i).wait()
    for i in range(nt - SLOTS, nt):
        for kind in (1, 2, 3):
            out_copy(kind, i).wait()


def grad_call(n1, n2, eb, a_full, dgu, d_qkv, dx_in, dg):
    tok, hd = n1.shape
    ff, qw = a_full.shape[1], d_qkv.shape[1]
    out = lambda *shape: jax.ShapeDtypeStruct(shape, BF)
    vm = lambda *shape: pltpu.VMEM(shape, BF)
    return pl.pallas_call(
        functools.partial(grad_kernel, (hd, ff, qw)),
        out_shape=(
            out(hd, ff), out(hd, ff), out(ff, hd), out(hd, qw),
            out(tok, hd), jax.ShapeDtypeStruct((1, hd), F32), jax.ShapeDtypeStruct((1, hd), F32),
        ),
        in_specs=[ANY] * 8,
        out_specs=[ANY] * 7,
        scratch_shapes=[
            vm(tok, hd), vm(tok, hd), vm(tok, hd), vm(tok, ff), vm(tok, 2 * ff), vm(tok, qw), vm(tok, hd), pltpu.VMEM((8, hd), F32), vm(hd, tok), vm(hd, tok),
            vm(SLOTS, hd, TILE), vm(SLOTS, hd, TILE), vm(SLOTS, hd, TILE), vm(SLOTS, TILE, hd),
            pltpu.SemaphoreType.DMA((8,)), pltpu.SemaphoreType.DMA((4, SLOTS)),
        ],
        compiler_params=pltpu.CompilerParams(vmem_limit_bytes=VMEM_LIMIT),
        name="weight_grads",
    )(n1, n2, eb, a_full, dgu, d_qkv, dx_in, dg)


def solution(mesh):
    def local_step(x_in, gain_one, gain_two, w_gate, w_up, w_down, w_qkv, dx_out, d_qkv):
        hd = x_in.shape[1]
        n1, n2, eb, a_full, dgu, dx_in, dg = comm_call(
            x_in, gain_one.reshape(1, hd), gain_two.reshape(1, hd), w_gate, w_up, w_down, w_qkv, dx_out, d_qkv
        )
        dw_gate, dw_up, dw_down, dw_qkv, dx_in, dg1, dg2 = grad_call(
            n1, n2, eb, a_full, dgu, d_qkv, dx_in, dg
        )
        return dx_in, dw_gate, dw_up, dw_down, dw_qkv, dg1.reshape(hd), dg2.reshape(hd)

    tok_spec = P("data", "hid")
    in_specs = (tok_spec, P("hid"), P("hid"), P("hid", "ffn"), P("hid", "ffn"), P("ffn", "hid"), P("hid", "ffn"), tok_spec, P("data", "ffn"))
    out_specs = (tok_spec, P(("data", "hid"), "ffn"), P(("data", "hid"), "ffn"), P(("data", "ffn"), "hid"), P(("data", "hid"), "ffn"), P(("data", "hid")), P(("data", "hid")))
    return jax.shard_map(local_step, mesh=mesh, in_specs=in_specs, out_specs=out_specs, check_vma=False)
```

```python
import functools

import jax
import jax.numpy as jnp
from jax import lax
from jax.experimental import pallas as pl
from jax.experimental.pallas import tpu as pltpu
from jax.sharding import PartitionSpec as P

NORM_EPS = 1e-6
BF = jnp.bfloat16
F32 = jnp.float32
MESH_ID = pl.DeviceIdType.MESH
ANY = pl.BlockSpec(memory_space=pl.ANY)
VMEM_LIMIT = 67043328

CHUNK = 1024
LATE = 2
YB = 2
F_STEPS = (0, 3)
QKV_AT = 7
DIRECT_LAST = 1
DIRECT_FIRST = 0
LAGS = ((1, 5, 9, 10), (1, 3, 5, 6))

PAIR, XRED, GX, GP, FW, DG = range(6)

PEERS = tuple((dy, j) for dy in range(2) for j in range(4) if dy or j)
ROW_PEERS = PEERS[:3]


def nn_dot(a_mat, b_mat):
    return jnp.dot(a_mat, b_mat, preferred_element_type=F32)


def nt_dot(a_mat, b_mat):
    return lax.dot_general(a_mat, b_mat, (((1,), (1,)), ((), ())), preferred_element_type=F32)


def pack_stats(cols):
    tok = cols[0].shape[0]
    lane = lax.broadcasted_iota(jnp.int32, (tok, 128), 1)
    wide = jnp.zeros((tok, 128), F32)
    for i, col in enumerate(cols):
        wide = jnp.where(lane == i, col, wide)
    full = jnp.concatenate([wide, jnp.zeros((128 - tok, 128), F32)], axis=0)
    return full.T[0:8, :]


def unpack_stats(tile, tok, count):
    full = jnp.concatenate([tile, jnp.zeros((120, 128), F32)], axis=0).T
    return [full[0:tok, i : i + 1] for i in range(count)]


def comm_kernel(
    dims,
    x_h, g1_h, g2_h, wg_h, wu_h, wd_h, wq_h, dx_h, dq_h,
    n1_o, n2_o, eb_o, a_o, dgu_o, dxin_o, dg_o,
    wgu, wd, wq, dq, x_s, dx_s, g1, g2, n1, n2, eb, e_s, x2_s,
    acc, part, r1, r2, xs, xr, xs2, xr2, gu, fb, a_f, da_f, dgu_f, y32, ys, yr, st_s, st_r, dxin_s, dg_s,
    ld, wld, qld, st_sem, y_sem, recvs, sends, f_sem,
):
    tok, hd, ff, qw = dims
    c_w = CHUNK
    nc = ff // c_w
    half = c_w // 2
    quart = c_w // 4
    d_model = hd * 4
    zc, yc, h = lax.axis_index("data"), lax.axis_index("ffn"), lax.axis_index("hid")
    xc = h // 2
    core = lax.rem(h, 2)
    pair = (zc, yc, xc * 2 + 1 - core)
    xnb = (zc, yc, (1 - xc) * 2 + core)
    diag = (zc, yc, 3 - h)
    ynb = (zc, 1 - yc, h)

    def peer(dy, j):
        return (zc, lax.rem(yc + dy, 2), lax.rem(h + j, 4))


    def load(src, dst, sem):
        return pltpu.make_async_copy(src, dst, sem)

    small = [
        load(x_h, x_s, ld.at[0]), load(g1_h, g1, ld.at[1]), load(dq_h, dq, ld.at[2]),
        load(g2_h, g2, ld.at[3]), load(dx_h, dx_s, ld.at[4]),
    ]
    qn = qw // 1024

    wq_load = load(wq_h, wq, qld.at[0])

    def gu_load(i, c):
        src = (wg_h, wu_h)[i].at[:, pl.ds(pl.multiple_of(c * c_w, c_w), c_w)]
        dst = wgu.at[:, pl.ds(pl.multiple_of((2 * c + i) * c_w, c_w), c_w)]
        return load(src, dst, wld.at[c])

    def gu_wait(c):
        both = wgu.at[:, pl.ds(pl.multiple_of(2 * c * c_w, 2 * c_w), 2 * c_w)]
        load(wg_h.at[:, pl.ds(0, 2 * c_w)], both, wld.at[c]).wait()

    wd_load = load(wd_h, wd, ld.at[5])

    def gu_load_start(n):
        gu_load(0, n).start()
        gu_load(1, n).start()

    for cp in small:
        cp.start()

    bar = pltpu.get_barrier_semaphore()
    for dy, j in PEERS[:4]:
        pl.semaphore_signal(bar, inc=1, device_id=peer(dy, j), device_id_type=MESH_ID)
    small[0].wait()
    gu_load_start(0)
    gu_load_start(1)
    x_f = x_s[...].astype(F32)
    sq_part = jnp.sum(x_f * x_f, axis=-1, keepdims=True)

    def qkv_step(i):
        @pl.when(i == 0)
        def _():
            wq_load.wait()

        cols = pl.ds(pl.multiple_of(i * 1024, 1024), 1024)
        y32[0] += nt_dot(dq[:, cols], wq[:, cols])

    y32[0] = jnp.zeros((tok, hd), F32)
    with jax.named_scope("barrier"):
        pl.semaphore_wait(bar, 4)

    def stat_copy(n, i):
        return pltpu.make_async_remote_copy(
            src_ref=st_s.at[n], dst_ref=st_r.at[n, yc * 4 + h], send_sem=st_sem.at[n, 0], recv_sem=st_sem.at[n, 1],
            device_id=peer(*PEERS[i]), device_id_type=MESH_ID,
        )

    def stat_send(n, cols, peers=ROW_PEERS):
        tile = pack_stats(cols)
        st_s[n] = tile
        st_r[n, yc * 4 + h] = tile
        for i in range(len(peers)):
            stat_copy(n, i).start()

    def stat_recv(n, count, peers=ROW_PEERS):
        all_tiles = st_r.at[n, pl.ds(0, len(peers))]
        whole = pltpu.make_async_remote_copy(
            src_ref=all_tiles, dst_ref=all_tiles, send_sem=st_sem.at[n, 0], recv_sem=st_sem.at[n, 1],
            device_id=peer(*PEERS[0]), device_id_type=MESH_ID,
        )
        whole.wait()
        total = jnp.zeros((8, 128), F32)
        for i in range(len(peers) + 1):
            total += st_r[n, i] if peers is PEERS else st_r[n, yc * 4 + i]
        return unpack_stats(total, tok, count)

    yb = hd // YB

    def y_cols(j):
        return pl.ds(j * yb, yb)

    def y_copy(n, j=0):
        if n == 0:
            src, dst = y32.at[0], y32.at[1]
        else:
            src, dst = ys.at[n - 1, :, y_cols(j)], yr.at[n - 1, :, y_cols(j)]
        return pltpu.make_async_remote_copy(
            src_ref=src, dst_ref=dst, send_sem=y_sem.at[n, YB], recv_sem=y_sem.at[n, j],
            device_id=ynb, device_id_type=MESH_ID,
        )

    def y_send(n, j):
        ys[n - 1, :, y_cols(j)] = acc[:, y_cols(j)].astype(BF)
        y_copy(n, j).start()

    def y_sum(n, j):
        with jax.named_scope(f"ywait{n}"):
            y_copy(n, j).wait_recv()
        return ys[n - 1, :, y_cols(j)].astype(F32) + yr[n - 1, :, y_cols(j)].astype(F32)

    def y_wait_send(n):
        whole = ys.at[n - 1]
        pltpu.make_async_remote_copy(
            src_ref=whole, dst_ref=whole, send_sem=y_sem.at[n, YB], recv_sem=y_sem.at[n, 0],
            device_id=ynb, device_id_type=MESH_ID,
        ).wait_send()

    stat_send(0, [sq_part])
    gu_load_start(2)
    gu_load_start(3)
    small[2].wait()
    small[1].wait()
    with jax.named_scope("stat0"):
        (sq,) = stat_recv(0, 1)
    gu_load_start(4)
    gu_load_start(5)
    inv1 = lax.rsqrt(sq / d_model + NORM_EPS)
    n1[...] = (x_s[...].astype(F32) * inv1 * g1[...]).astype(BF)
    n1_out = load(n1, n1_o, ld.at[0])
    n1_out.start()
    acc[...] = jnp.zeros_like(acc)

    def pair_copy(ph, c):
        slot = lax.rem(c, 2)
        src = part.at[slot, 1 - core] if ph == 0 else part.at[slot, 1 - core, 0]
        return pltpu.make_async_remote_copy(
            src_ref=src, dst_ref=(r1 if ph == 0 else r2).at[c],
            send_sem=sends.at[4 + slot], recv_sem=recvs.at[PAIR, c],
            device_id=pair, device_id_type=MESH_ID,
        )

    def x_copy(ph, c):
        src, dst = ((xs, xr), (xs2, xr2))[ph]
        return pltpu.make_async_remote_copy(
            src_ref=src.at[c], dst_ref=dst.at[c],
            send_sem=sends.at[0], recv_sem=recvs.at[XRED, c],
            device_id=xnb, device_id_type=MESH_ID,
        )

    own_q = core * 2 + xc
    xnb_q = core * 2 + 1 - xc

    def block(ph, c, q):
        cols = pl.ds(pl.multiple_of(c * c_w + q * quart, quart), quart)
        return (a_f if ph == 0 else da_f).at[:, cols]

    def g_copy(ph, c, kind):
        ref = block(ph, c, xnb_q if kind == FW else own_q)
        target = {GX: xnb, GP: pair, FW: pair, DG: diag}[kind]
        kind = FW if kind == DG else kind
        return pltpu.make_async_remote_copy(
            src_ref=ref, dst_ref=ref, send_sem=sends.at[kind - 1], recv_sem=recvs.at[kind, c],
            device_id=target, device_id_type=MESH_ID,
        )

    def wait_sends(ph):
        src = xs if ph == 0 else xs2
        pltpu.make_async_remote_copy(
            src_ref=src, dst_ref=src, send_sem=sends.at[0], recv_sem=recvs.at[XRED, 0],
            device_id=xnb, device_id_type=MESH_ID,
        ).wait_send()
        whole = (a_f if ph == 0 else da_f).at[:, pl.ds(0, ff // 4)]
        for kind in (GX, GP, FW):
            pltpu.make_async_remote_copy(
                src_ref=whole, dst_ref=whole, send_sem=sends.at[kind - 1], recv_sem=recvs.at[kind, 0],
                device_id=xnb, device_id_type=MESH_ID,
            ).wait_send()
        for c in (nc - 2, nc - 1):
            pair_copy(ph, c).wait_send()

    f_parts = ((0, nc - LATE), (nc - LATE, LATE))

    def f_copy(n):
        first, count = f_parts[n % 2] if n < 4 else (0, nc)
        ref = fb.at[xnb_q if n in (2, 3) else own_q, pl.ds(first, count)]
        return pltpu.make_async_remote_copy(
            src_ref=ref, dst_ref=ref, send_sem=f_sem.at[5], recv_sem=f_sem.at[n],
            device_id=xnb if n < 2 else pair, device_id_type=MESH_ID,
        )

    own_cols = pl.ds(pl.multiple_of(xc * quart, quart), quart)
    oth_cols = pl.ds(pl.multiple_of((1 - xc) * quart, quart), quart)

    def pipeline(ph, partial, activate, consume):
        lag_pair, lag_act, lag_fwd, lag_dot = LAGS[ph]

        def direct(c):
            return c >= nc - DIRECT_LAST if ph == 0 else c < DIRECT_FIRST

        def reduce_pair(c):
            slot = lax.rem(c, 2)
            with jax.named_scope(f"pairwait{ph}"):
                pair_copy(ph, c).wait_recv()
            if ph == 0:
                xs[c] = (part[slot, core, :, :, oth_cols] + r1[c, :, :, oth_cols]).astype(BF)
                x_copy(ph, c).start()
                gu[c] = part[slot, core, :, :, own_cols] + r1[c, :, :, own_cols]
            else:
                xs2[c] = (part[slot, core, 0, :, oth_cols] + r2[c, :, oth_cols]).astype(BF)
                x_copy(ph, c).start()
                r2[c, :, own_cols] = part[slot, core, 0, :, own_cols] + r2[c, :, own_cols]

        def step(t, carry):
            if ph == 1:
                for n, when in enumerate(F_STEPS):

                    @pl.when(t == when)
                    def _():
                        f_copy(n).wait_recv()
                        f_copy(2 + n).start()

            if ph == 0:

                @pl.when(t == 0)
                def _():
                    for c in range(6, nc):
                        gu_load_start(c)

                @pl.when(t == 1)
                def _():
                    wq_load.start()

                @pl.when(t == 2)
                def _():
                    wd_load.start()

                @pl.when((t >= QKV_AT) & (t < QKV_AT + qn))
                def _():
                    with jax.named_scope("qkv"):
                        qkv_step(t - QKV_AT)

                @pl.when(t == QKV_AT + qn - 1)
                def _():
                    y_copy(0).start()

            @pl.when(t < nc)
            def _():
                c = t

                @pl.when(c >= 2)
                def _():
                    pair_copy(ph, c - 2).wait_send()

                with jax.named_scope(f"part{ph}"):

                    partial(c)
                    pair_copy(ph, c).start()

            @pl.when((t >= lag_pair) & (t < nc + lag_pair))
            def _():
                reduce_pair(t - lag_pair)

            @pl.when((t >= lag_act) & (t < nc + lag_act))
            def _():
                c = t - lag_act
                with jax.named_scope(f"xwait{ph}"):
                    x_copy(ph, c).wait_recv()
                with jax.named_scope(f"act{ph}"):
                    activate(c)
                g_copy(ph, c, GX).start()
                g_copy(ph, c, GP).start()

                @pl.when(direct(c))
                def _():
                    g_copy(ph, c, DG).start()

                if ph == 0:

                    @pl.when(c == nc - 1)
                    def _():
                        f_copy(0).start()

            @pl.when((t >= lag_fwd) & (t < nc + lag_fwd))
            def _():
                c = t - lag_fwd
                with jax.named_scope(f"gxwait{ph}"):
                    g_copy(ph, c, GX).wait_recv()

                @pl.when(jnp.logical_not(direct(c)))
                def _():
                    g_copy(ph, c, FW).start()

            @pl.when((t >= lag_dot) & (t < nc + lag_dot))
            def _():
                c = t - lag_dot
                with jax.named_scope(f"gpwait{ph}"):
                    g_copy(ph, c, GP).wait_recv()
                    g_copy(ph, c, FW).wait_recv()
                with jax.named_scope(f"dot{ph}"):
                    consume(c)

            return carry

        lax.fori_loop(0, nc + lag_dot, step, 0)

    def gu_partial(c):
        gu_wait(c)
        slot = lax.rem(c, 2)
        prod = nn_dot(n1[...], wgu[:, pl.ds(pl.multiple_of(2 * c * c_w, 2 * c_w), 2 * c_w)])
        for i in range(2):
            part[slot, 0, i] = prod[:, i * c_w : i * c_w + half]
            part[slot, 1, i] = prod[:, i * c_w + half : (i + 1) * c_w]

    def act_forward(c):
        gate = gu[c, 0] + xr[c, 0].astype(F32)
        up = gu[c, 1] + xr[c, 1].astype(F32)
        sig = jax.nn.sigmoid(gate)
        silu = gate * sig
        cols = pl.ds(pl.multiple_of(c * c_w + own_q * quart, quart), quart)
        a_f[:, cols] = (silu * up).astype(BF)
        fb[own_q, c, 0] = (up * sig * (1.0 + gate * (1.0 - sig))).astype(BF)
        fb[own_q, c, 1] = silu.astype(BF)

    def down_dot(c):
        @pl.when(c == 0)
        def _():
            wd_load.wait()

        rows = pl.ds(pl.multiple_of(c * c_w, c_w), c_w)

        @pl.when(c < nc - 1)
        def _():
            acc[...] += nn_dot(a_f[:, rows], wd[rows, :])

        @pl.when(c == nc - 1)
        def _():
            for j in range(YB):
                acc[:, y_cols(j)] += nn_dot(a_f[:, rows], wd[rows, y_cols(j)])
                y_send(1, j)


    pipeline(0, gu_partial, act_forward, down_dot)
    wait_sends(0)
    f_copy(4).start()
    a_out = load(a_f, a_o, ld.at[1])
    a_out.start()

    small[3].wait()
    small[4].wait()
    y_copy(0).wait()
    acc[...] = y32[0] + y32[1]
    sq_two = jnp.zeros((tok, 1), F32)
    dot_two = jnp.zeros((tok, 1), F32)
    for j in range(YB):
        cols = y_cols(j)
        x2_b = (x_s[:, cols].astype(F32) + y_sum(1, j)).astype(BF)
        x2_s[:, cols] = x2_b
        x2 = x2_b.astype(F32)
        sq_two += jnp.sum(x2 * x2, axis=-1, keepdims=True)
        dot_two += jnp.sum(g2[:, cols] * acc[:, cols] * x2, axis=-1, keepdims=True)
    stat_send(1, [sq_two, dot_two])
    f_copy(1).start()
    with jax.named_scope("stat1"):
        sq2, dot2 = stat_recv(1, 2)
    inv2 = lax.rsqrt(sq2 / d_model + NORM_EPS)
    x2 = x2_s[...].astype(F32)
    dz2 = inv2 * (g2[...] * acc[...]) - x2 * (inv2 * inv2 * inv2) * (dot2 / d_model)
    e_val = dx_s[...].astype(F32) + dz2
    e_s[...] = e_val
    eb[...] = e_val.astype(BF)
    n2[...] = (x2_s[...].astype(F32) * inv2 * g2[...]).astype(BF)
    dg_s[0:1, :] = jnp.sum(acc[...] * x2_s[...].astype(F32) * inv2, axis=0, keepdims=True)
    outs = [load(eb, eb_o, ld.at[2]), load(n2, n2_o, ld.at[3])]
    for cp in outs:
        cp.start()
    acc[...] = jnp.zeros_like(acc)

    def da_partial(c):
        slot = lax.rem(c, 2)
        prod = nt_dot(eb[...], wd[pl.ds(pl.multiple_of(c * c_w, c_w), c_w), :])
        part[slot, 0, 0] = prod[:, :half]
        part[slot, 1, 0] = prod[:, half:]

    def act_backward(c):
        cols = pl.ds(pl.multiple_of(c * c_w + own_q * quart, quart), quart)
        da_f[:, cols] = (r2[c, :, own_cols] + xr2[c].astype(F32)).astype(BF)

    def dn1_dot(c):
        @pl.when(c == 0)
        def _():
            f_copy(4).wait_recv()
            f_copy(2).wait_recv()

        @pl.when(c == nc - LATE)
        def _():
            f_copy(3).wait_recv()

        for q in range(4):
            cols = pl.ds(pl.multiple_of(c * c_w + q * quart, quart), quart)
            d_act = da_f[:, cols].astype(F32)
            for i in range(2):
                dst = pl.ds(pl.multiple_of((2 * c + i) * c_w + q * quart, quart), quart)
                dgu_f[:, dst] = (d_act * fb[q, c, i].astype(F32)).astype(BF)
        cols = pl.ds(pl.multiple_of(2 * c * c_w, 2 * c_w), 2 * c_w)

        @pl.when(c < nc - 1)
        def _():
            acc[...] += nt_dot(dgu_f[:, cols], wgu[:, cols])

        @pl.when(c == nc - 1)
        def _():
            for j in range(YB):
                acc[:, y_cols(j)] += nt_dot(dgu_f[:, cols], wgu[y_cols(j), cols])
                y_send(2, j)

    pipeline(1, da_partial, act_backward, dn1_dot)
    dgu_out = load(dgu_f, dgu_o, ld.at[4])

    stat_send(2, [jnp.sum(g1[...] * acc[...] * x_s[...].astype(F32), axis=-1, keepdims=True)], PEERS)
    dgu_out.start()
    wait_sends(1)
    sent = fb.at[pl.ds(0, 3)]
    pltpu.make_async_remote_copy(
        src_ref=sent, dst_ref=sent, send_sem=f_sem.at[5], recv_sem=f_sem.at[0], device_id=pair, device_id_type=MESH_ID
    ).wait_send()
    for j in range(YB):
        acc[:, y_cols(j)] = y_sum(2, j)
    y_wait_send(1)
    y_wait_send(2)
    dg_s[1:2, :] = jnp.sum(acc[...] * x_s[...].astype(F32) * inv1, axis=0, keepdims=True)
    with jax.named_scope("stat2"):
        (dot1,) = stat_recv(2, 1, PEERS)
    dz1 = inv1 * (g1[...] * acc[...]) - x_s[...].astype(F32) * (inv1 * inv1 * inv1) * (dot1 / d_model)
    dxin_s[...] = (e_s[...] + dz1).astype(BF)
    tail = [
        load(dxin_s, dxin_o, ld.at[5]),
        load(dg_s, dg_o, qld.at[0]),
    ]
    for cp in tail:
        cp.start()
    for cp in (n1_out, a_out, *outs, dgu_out, *tail):
        cp.wait()


def comm_call(x_in, gain_one, gain_two, w_gate, w_up, w_down, w_qkv, dx_out, d_qkv):
    tok, hd = x_in.shape
    ff = w_gate.shape[1]
    qw = w_qkv.shape[1]
    nc = ff // CHUNK
    half, quart = CHUNK // 2, CHUNK // 4
    out = lambda shape, dtype: jax.ShapeDtypeStruct(shape, dtype)
    vm = lambda *shape_dtype: pltpu.VMEM(shape_dtype[:-1], shape_dtype[-1])
    dma = pltpu.SemaphoreType.DMA
    return pl.pallas_call(
        functools.partial(comm_kernel, (tok, hd, ff, qw)),
        out_shape=(
            out((tok, hd), BF), out((tok, hd), BF), out((tok, hd), BF), out((tok, ff), BF), out((tok, 2 * ff), BF),
            out((tok, hd), BF), out((8, hd), F32),
        ),
        in_specs=[ANY] * 9,
        out_specs=[ANY] * 7,
        scratch_shapes=[
            vm(hd, 2 * ff, BF), vm(ff, hd, BF), vm(hd, qw, BF), vm(tok, qw, BF),
            vm(tok, hd, BF), vm(tok, hd, BF), vm(1, hd, F32), vm(1, hd, F32),
            vm(tok, hd, BF), vm(tok, hd, BF), vm(tok, hd, BF), vm(tok, hd, F32), vm(tok, hd, BF),
            vm(tok, hd, F32), vm(2, 2, 2, tok, half, F32), vm(nc, 2, tok, half, F32), vm(nc, tok, half, F32),
            vm(nc, 2, tok, quart, BF), vm(nc, 2, tok, quart, BF), vm(nc, tok, quart, BF), vm(nc, tok, quart, BF),
            vm(nc, 2, tok, quart, F32), vm(4, nc, 2, tok, quart, BF), vm(tok, ff, BF), vm(tok, ff, BF), vm(tok, 2 * ff, BF),
            vm(2, tok, hd, F32), vm(2, tok, hd, BF), vm(2, tok, hd, BF), vm(3, 8, 128, F32), vm(3, 8, 8, 128, F32),
            vm(tok, hd, BF), vm(8, hd, F32),
            dma((6,)), dma((nc,)), dma((1,)), dma((3, 2)), dma((3, YB + 1)), dma((5, nc)), dma((6,)), dma((6,)),
        ],
        compiler_params=pltpu.CompilerParams(
            collective_id=0, has_side_effects=True, vmem_limit_bytes=VMEM_LIMIT
        ),
        name="block_comm",
    )(x_in, gain_one, gain_two, w_gate, w_up, w_down, w_qkv, dx_out, d_qkv)


TILE = CHUNK
SLOTS = 3


def grad_kernel(
    dims, n1_h, n2_h, eb_h, a_h, dgu_h, dq_h, dx_h, dg_h,
    dwg_o, dwu_o, dwd_o, dwq_o, dx_o, dg1_o, dg2_o,
    n1, n2, eb, a_f, dgu, dq, dx, dg, n1_t, n2_t, bq, bg, bu, bd, ld, sem,
):
    hd, ff, qw = dims
    nt, nq = ff // TILE, qw // TILE
    pairs = ((n2_h, n2), (dq_h, dq), (eb_h, eb), (a_h, a_f), (n1_h, n1), (dgu_h, dgu), (dx_h, dx), (dg_h, dg))
    loads = [pltpu.make_async_copy(src, dst, ld.at[i]) for i, (src, dst) in enumerate(pairs)]
    for cp in loads:
        cp.start()

    def cols_of(i):
        return pl.ds(pl.multiple_of(i * TILE, TILE), TILE)

    def out_copy(kind, i):
        slot = lax.rem(i, SLOTS)
        src = (bq, bg, bu, bd)[kind].at[slot]
        dst = (dwq_o, dwg_o, dwu_o, dwd_o)[kind]
        return pltpu.make_async_copy(src, dst.at[cols_of(i), :] if kind == 3 else dst.at[:, cols_of(i)], sem.at[kind, slot])

    with jax.named_scope("b_in0"):
      loads[0].wait()
      loads[1].wait()
    with jax.named_scope("b_t"):
      n2_t[...] = n2[...].T

    def q_step(i, carry):
        @pl.when(i >= SLOTS)
        def _():
            out_copy(0, i - SLOTS).wait()

        bq[lax.rem(i, SLOTS)] = nn_dot(n2_t[...], dq[:, cols_of(i)]).astype(BF)
        out_copy(0, i).start()
        return carry

    with jax.named_scope("b_q"):
      lax.fori_loop(0, nq, q_step, 0)
    with jax.named_scope("b_in1"):
      for cp in loads[2:]:
        cp.wait()
    finals = [
        pltpu.make_async_copy(dx, dx_o, ld.at[0]),
        pltpu.make_async_copy(dg.at[0:1, :], dg2_o, ld.at[1]),
        pltpu.make_async_copy(dg.at[1:2, :], dg1_o, ld.at[2]),
    ]
    for cp in finals:
        cp.start()
    n1_t[...] = n1[...].T

    def step(i, carry):
        slot = lax.rem(i, SLOTS)

        @pl.when(i >= SLOTS)
        def _():
            for kind in (1, 2, 3):
                out_copy(kind, i - SLOTS).wait()

        bd[slot] = nn_dot(a_f[:, cols_of(i)].T, eb[...]).astype(BF)
        out_copy(3, i).start()
        bg[slot] = nn_dot(n1_t[...], dgu[:, cols_of(2 * i)]).astype(BF)
        out_copy(1, i).start()
        bu[slot] = nn_dot(n1_t[...], dgu[:, cols_of(2 * i + 1)]).astype(BF)
        out_copy(2, i).start()
        return carry

    lax.fori_loop(0, nt, step, 0)
    for cp in finals:
        cp.wait()
    for i in range(max(nq - SLOTS, 0), nq):
        out_copy(0, i).wait()
    for i in range(nt - SLOTS, nt):
        for kind in (1, 2, 3):
            out_copy(kind, i).wait()


def grad_call(n1, n2, eb, a_full, dgu, d_qkv, dx_in, dg):
    tok, hd = n1.shape
    ff, qw = a_full.shape[1], d_qkv.shape[1]
    out = lambda *shape: jax.ShapeDtypeStruct(shape, BF)
    vm = lambda *shape: pltpu.VMEM(shape, BF)
    return pl.pallas_call(
        functools.partial(grad_kernel, (hd, ff, qw)),
        out_shape=(
            out(hd, ff), out(hd, ff), out(ff, hd), out(hd, qw),
            out(tok, hd), jax.ShapeDtypeStruct((1, hd), F32), jax.ShapeDtypeStruct((1, hd), F32),
        ),
        in_specs=[ANY] * 8,
        out_specs=[ANY] * 7,
        scratch_shapes=[
            vm(tok, hd), vm(tok, hd), vm(tok, hd), vm(tok, ff), vm(tok, 2 * ff), vm(tok, qw), vm(tok, hd), pltpu.VMEM((8, hd), F32), vm(hd, tok), vm(hd, tok),
            vm(SLOTS, hd, TILE), vm(SLOTS, hd, TILE), vm(SLOTS, hd, TILE), vm(SLOTS, TILE, hd),
            pltpu.SemaphoreType.DMA((8,)), pltpu.SemaphoreType.DMA((4, SLOTS)),
        ],
        compiler_params=pltpu.CompilerParams(vmem_limit_bytes=VMEM_LIMIT),
        name="weight_grads",
    )(n1, n2, eb, a_full, dgu, d_qkv, dx_in, dg)


def solution(mesh):
    def local_step(x_in, gain_one, gain_two, w_gate, w_up, w_down, w_qkv, dx_out, d_qkv):
        hd = x_in.shape[1]
        n1, n2, eb, a_full, dgu, dx_in, dg = comm_call(
            x_in, gain_one.reshape(1, hd), gain_two.reshape(1, hd), w_gate, w_up, w_down, w_qkv, dx_out, d_qkv
        )
        dw_gate, dw_up, dw_down, dw_qkv, dx_in, dg1, dg2 = grad_call(
            n1, n2, eb, a_full, dgu, d_qkv, dx_in, dg
        )
        return dx_in, dw_gate, dw_up, dw_down, dw_qkv, dg1.reshape(hd), dg2.reshape(hd)

    tok_spec = P("data", "hid")
    in_specs = (tok_spec, P("hid"), P("hid"), P("hid", "ffn"), P("hid", "ffn"), P("ffn", "hid"), P("hid", "ffn"), tok_spec, P("data", "ffn"))
    out_specs = (tok_spec, P(("data", "hid"), "ffn"), P(("data", "hid"), "ffn"), P(("data", "ffn"), "hid"), P(("data", "hid"), "ffn"), P(("data", "hid")), P(("data", "hid")))
    return jax.shard_map(local_step, mesh=mesh, in_specs=in_specs, out_specs=out_specs, check_vma=False)
```

```python
import functools

import jax
import jax.numpy as jnp
from jax import lax
from jax.experimental import pallas as pl
from jax.experimental.pallas import tpu as pltpu
from jax.sharding import PartitionSpec as P

NORM_EPS = 1e-6
BF = jnp.bfloat16
F32 = jnp.float32
MESH_ID = pl.DeviceIdType.MESH
ANY = pl.BlockSpec(memory_space=pl.ANY)
VMEM_LIMIT = 67043328

CHUNK = 1024
LATE = 2
YB = 2
F_STEPS = (0, 3)
QKV_AT = 7
DIRECT_LAST = 1
DIRECT_FIRST = 0
LAGS = ((1, 5, 9, 10), (1, 3, 5, 6))

PAIR, XRED, GX, GP, FW, DG = range(6)

PEERS = tuple((dy, j) for dy in range(2) for j in range(4) if dy or j)
ROW_PEERS = PEERS[:3]


def nn_dot(a_mat, b_mat):
    return jnp.dot(a_mat, b_mat, preferred_element_type=F32)


def nt_dot(a_mat, b_mat):
    return lax.dot_general(a_mat, b_mat, (((1,), (1,)), ((), ())), preferred_element_type=F32)


def pack_stats(cols):
    tok = cols[0].shape[0]
    lane = lax.broadcasted_iota(jnp.int32, (tok, 128), 1)
    wide = jnp.zeros((tok, 128), F32)
    for i, col in enumerate(cols):
        wide = jnp.where(lane == i, col, wide)
    full = jnp.concatenate([wide, jnp.zeros((128 - tok, 128), F32)], axis=0)
    return full.T[0:8, :]


def unpack_stats(tile, tok, count):
    full = jnp.concatenate([tile, jnp.zeros((120, 128), F32)], axis=0).T
    return [full[0:tok, i : i + 1] for i in range(count)]


def comm_kernel(
    dims,
    x_h, g1_h, g2_h, wg_h, wu_h, wd_h, wq_h, dx_h, dq_h,
    n1_o, n2_o, eb_o, a_o, dgu_o, dxin_o, dg_o,
    wgu, wd, wq, dq, x_s, dx_s, g1, g2, n1, n2, eb, e_s, x2_s,
    acc, part, r1, r2, xs, xr, xs2, xr2, gu, fb, a_f, da_f, dgu_f, y32, ys, yr, st_s, st_r, dxin_s, dg_s,
    ld, wld, qld, st_sem, y_sem, recvs, sends, f_sem,
):
    tok, hd, ff, qw = dims
    c_w = CHUNK
    nc = ff // c_w
    half = c_w // 2
    quart = c_w // 4
    d_model = hd * 4
    zc, yc, h = lax.axis_index("data"), lax.axis_index("ffn"), lax.axis_index("hid")
    xc = h // 2
    core = lax.rem(h, 2)
    pair = (zc, yc, xc * 2 + 1 - core)
    xnb = (zc, yc, (1 - xc) * 2 + core)
    diag = (zc, yc, 3 - h)
    ynb = (zc, 1 - yc, h)

    def peer(dy, j):
        return (zc, lax.rem(yc + dy, 2), lax.rem(h + j, 4))


    def load(src, dst, sem):
        return pltpu.make_async_copy(src, dst, sem)

    small = [
        load(x_h, x_s, ld.at[0]), load(g1_h, g1, ld.at[1]), load(dq_h, dq, ld.at[2]),
        load(g2_h, g2, ld.at[3]), load(dx_h, dx_s, ld.at[4]),
    ]
    qn = qw // 1024

    wq_load = load(wq_h, wq, qld.at[0])

    def gu_load(i, c):
        src = (wg_h, wu_h)[i].at[:, pl.ds(pl.multiple_of(c * c_w, c_w), c_w)]
        dst = wgu.at[:, pl.ds(pl.multiple_of((2 * c + i) * c_w, c_w), c_w)]
        return load(src, dst, wld.at[c])

    def gu_wait(c):
        both = wgu.at[:, pl.ds(pl.multiple_of(2 * c * c_w, 2 * c_w), 2 * c_w)]
        load(wg_h.at[:, pl.ds(0, 2 * c_w)], both, wld.at[c]).wait()

    wd_load = load(wd_h, wd, ld.at[5])

    def gu_load_start(n):
        gu_load(0, n).start()
        gu_load(1, n).start()

    for cp in small:
        cp.start()

    bar = pltpu.get_barrier_semaphore()
    for dy, j in PEERS[:4]:
        pl.semaphore_signal(bar, inc=1, device_id=peer(dy, j), device_id_type=MESH_ID)
    small[0].wait()
    gu_load_start(0)
    gu_load_start(1)
    x_f = x_s[...].astype(F32)
    sq_part = jnp.sum(x_f * x_f, axis=-1, keepdims=True)

    def qkv_step(i):
        @pl.when(i == 0)
        def _():
            wq_load.wait()

        cols = pl.ds(pl.multiple_of(i * 1024, 1024), 1024)
        y32[0] += nt_dot(dq[:, cols], wq[:, cols])

    y32[0] = jnp.zeros((tok, hd), F32)
    with jax.named_scope("barrier"):
        pl.semaphore_wait(bar, 4)

    def stat_copy(n, i):
        return pltpu.make_async_remote_copy(
            src_ref=st_s.at[n], dst_ref=st_r.at[n, yc * 4 + h], send_sem=st_sem.at[n, 0], recv_sem=st_sem.at[n, 1],
            device_id=peer(*PEERS[i]), device_id_type=MESH_ID,
        )

    def stat_send(n, cols, peers=ROW_PEERS):
        tile = pack_stats(cols)
        st_s[n] = tile
        st_r[n, yc * 4 + h] = tile
        for i in range(len(peers)):
            stat_copy(n, i).start()

    def stat_recv(n, count, peers=ROW_PEERS):
        all_tiles = st_r.at[n, pl.ds(0, len(peers))]
        whole = pltpu.make_async_remote_copy(
            src_ref=all_tiles, dst_ref=all_tiles, send_sem=st_sem.at[n, 0], recv_sem=st_sem.at[n, 1],
            device_id=peer(*PEERS[0]), device_id_type=MESH_ID,
        )
        whole.wait()
        total = jnp.zeros((8, 128), F32)
        for i in range(len(peers) + 1):
            total += st_r[n, i] if peers is PEERS else st_r[n, yc * 4 + i]
        return unpack_stats(total, tok, count)

    yb = hd // YB

    def y_cols(j):
        return pl.ds(j * yb, yb)

    def y_copy(n, j=0):
        if n == 0:
            src, dst = y32.at[0], y32.at[1]
        else:
            src, dst = ys.at[n - 1, :, y_cols(j)], yr.at[n - 1, :, y_cols(j)]
        return pltpu.make_async_remote_copy(
            src_ref=src, dst_ref=dst, send_sem=y_sem.at[n, YB], recv_sem=y_sem.at[n, j],
            device_id=ynb, device_id_type=MESH_ID,
        )

    def y_send(n, j):
        ys[n - 1, :, y_cols(j)] = acc[:, y_cols(j)].astype(BF)
        y_copy(n, j).start()

    def y_sum(n, j):
        with jax.named_scope(f"ywait{n}"):
            y_copy(n, j).wait_recv()
        return ys[n - 1, :, y_cols(j)].astype(F32) + yr[n - 1, :, y_cols(j)].astype(F32)

    def y_wait_send(n):
        whole = ys.at[n - 1]
        pltpu.make_async_remote_copy(
            src_ref=whole, dst_ref=whole, send_sem=y_sem.at[n, YB], recv_sem=y_sem.at[n, 0],
            device_id=ynb, device_id_type=MESH_ID,
        ).wait_send()

    stat_send(0, [sq_part])
    gu_load_start(2)
    gu_load_start(3)
    small[2].wait()
    small[1].wait()
    with jax.named_scope("stat0"):
        (sq,) = stat_recv(0, 1)
    gu_load_start(4)
    gu_load_start(5)
    inv1 = lax.rsqrt(sq / d_model + NORM_EPS)
    n1[...] = (x_s[...].astype(F32) * inv1 * g1[...]).astype(BF)
    n1_out = load(n1, n1_o, ld.at[0])
    n1_out.start()
    acc[...] = jnp.zeros_like(acc)

    def pair_copy(ph, c):
        slot = lax.rem(c, 2)
        src = part.at[slot, 1 - core] if ph == 0 else part.at[slot, 1 - core, 0]
        return pltpu.make_async_remote_copy(
            src_ref=src, dst_ref=(r1 if ph == 0 else r2).at[c],
            send_sem=sends.at[4 + slot], recv_sem=recvs.at[PAIR, c],
            device_id=pair, device_id_type=MESH_ID,
        )

    def x_copy(ph, c):
        src, dst = ((xs, xr), (xs2, xr2))[ph]
        return pltpu.make_async_remote_copy(
            src_ref=src.at[c], dst_ref=dst.at[c],
            send_sem=sends.at[0], recv_sem=recvs.at[XRED, c],
            device_id=xnb, device_id_type=MESH_ID,
        )

    own_q = core * 2 + xc
    xnb_q = core * 2 + 1 - xc

    def block(ph, c, q):
        cols = pl.ds(pl.multiple_of(c * c_w + q * quart, quart), quart)
        return (a_f if ph == 0 else da_f).at[:, cols]

    def g_copy(ph, c, kind):
        ref = block(ph, c, xnb_q if kind == FW else own_q)
        target = {GX: xnb, GP: pair, FW: pair, DG: diag}[kind]
        kind = FW if kind == DG else kind
        return pltpu.make_async_remote_copy(
            src_ref=ref, dst_ref=ref, send_sem=sends.at[kind - 1], recv_sem=recvs.at[kind, c],
            device_id=target, device_id_type=MESH_ID,
        )

    def wait_sends(ph):
        src = xs if ph == 0 else xs2
        pltpu.make_async_remote_copy(
            src_ref=src, dst_ref=src, send_sem=sends.at[0], recv_sem=recvs.at[XRED, 0],
            device_id=xnb, device_id_type=MESH_ID,
        ).wait_send()
        whole = (a_f if ph == 0 else da_f).at[:, pl.ds(0, ff // 4)]
        for kind in (GX, GP, FW):
            pltpu.make_async_remote_copy(
                src_ref=whole, dst_ref=whole, send_sem=sends.at[kind - 1], recv_sem=recvs.at[kind, 0],
                device_id=xnb, device_id_type=MESH_ID,
            ).wait_send()
        for c in (nc - 2, nc - 1):
            pair_copy(ph, c).wait_send()

    f_parts = ((0, nc - LATE), (nc - LATE, LATE))

    def f_copy(n):
        first, count = f_parts[n % 2] if n < 4 else (0, nc)
        ref = fb.at[xnb_q if n in (2, 3) else own_q, pl.ds(first, count)]
        return pltpu.make_async_remote_copy(
            src_ref=ref, dst_ref=ref, send_sem=f_sem.at[5], recv_sem=f_sem.at[n],
            device_id=xnb if n < 2 else pair, device_id_type=MESH_ID,
        )

    own_cols = pl.ds(pl.multiple_of(xc * quart, quart), quart)
    oth_cols = pl.ds(pl.multiple_of((1 - xc) * quart, quart), quart)

    def pipeline(ph, partial, activate, consume):
        lag_pair, lag_act, lag_fwd, lag_dot = LAGS[ph]

        def direct(c):
            return c >= nc - DIRECT_LAST if ph == 0 else c < DIRECT_FIRST

        def reduce_pair(c):
            slot = lax.rem(c, 2)
            with jax.named_scope(f"pairwait{ph}"):
                pair_copy(ph, c).wait_recv()
            if ph == 0:
                xs[c] = (part[slot, core, :, :, oth_cols] + r1[c, :, :, oth_cols]).astype(BF)
                x_copy(ph, c).start()
                gu[c] = part[slot, core, :, :, own_cols] + r1[c, :, :, own_cols]
            else:
                xs2[c] = (part[slot, core, 0, :, oth_cols] + r2[c, :, oth_cols]).astype(BF)
                x_copy(ph, c).start()
                r2[c, :, own_cols] = part[slot, core, 0, :, own_cols] + r2[c, :, own_cols]

        def step(t, carry):
            if ph == 1:
                for n, when in enumerate(F_STEPS):

                    @pl.when(t == when)
                    def _():
                        f_copy(n).wait_recv()
                        f_copy(2 + n).start()

            if ph == 0:

                @pl.when(t == 0)
                def _():
                    for c in range(6, nc):
                        gu_load_start(c)

                @pl.when(t == 1)
                def _():
                    wq_load.start()

                @pl.when(t == 2)
                def _():
                    wd_load.start()

                @pl.when((t >= QKV_AT) & (t < QKV_AT + qn))
                def _():
                    with jax.named_scope("qkv"):
                        qkv_step(t - QKV_AT)

                @pl.when(t == QKV_AT + qn - 1)
                def _():
                    y_copy(0).start()

            @pl.when(t < nc)
            def _():
                c = t

                @pl.when(c >= 2)
                def _():
                    pair_copy(ph, c - 2).wait_send()

                with jax.named_scope(f"part{ph}"):

                    partial(c)
                    pair_copy(ph, c).start()

            @pl.when((t >= lag_pair) & (t < nc + lag_pair))
            def _():
                reduce_pair(t - lag_pair)

            @pl.when((t >= lag_act) & (t < nc + lag_act))
            def _():
                c = t - lag_act
                with jax.named_scope(f"xwait{ph}"):
                    x_copy(ph, c).wait_recv()
                with jax.named_scope(f"act{ph}"):
                    activate(c)
                g_copy(ph, c, GP).start()
                g_copy(ph, c, GX).start()

                @pl.when(direct(c))
                def _():
                    g_copy(ph, c, DG).start()

                if ph == 0:

                    @pl.when(c == nc - 1)
                    def _():
                        f_copy(0).start()

            @pl.when((t >= lag_fwd) & (t < nc + lag_fwd))
            def _():
                c = t - lag_fwd
                with jax.named_scope(f"gxwait{ph}"):
                    g_copy(ph, c, GX).wait_recv()

                @pl.when(jnp.logical_not(direct(c)))
                def _():
                    g_copy(ph, c, FW).start()

            @pl.when((t >= lag_dot) & (t < nc + lag_dot))
            def _():
                c = t - lag_dot
                with jax.named_scope(f"gpwait{ph}"):
                    g_copy(ph, c, GP).wait_recv()
                    g_copy(ph, c, FW).wait_recv()
                with jax.named_scope(f"dot{ph}"):
                    consume(c)

            return carry

        lax.fori_loop(0, nc + lag_dot, step, 0)

    def gu_partial(c):
        gu_wait(c)
        slot = lax.rem(c, 2)
        prod = nn_dot(n1[...], wgu[:, pl.ds(pl.multiple_of(2 * c * c_w, 2 * c_w), 2 * c_w)])
        for i in range(2):
            part[slot, 0, i] = prod[:, i * c_w : i * c_w + half]
            part[slot, 1, i] = prod[:, i * c_w + half : (i + 1) * c_w]

    def act_forward(c):
        gate = gu[c, 0] + xr[c, 0].astype(F32)
        up = gu[c, 1] + xr[c, 1].astype(F32)
        sig = jax.nn.sigmoid(gate)
        silu = gate * sig
        cols = pl.ds(pl.multiple_of(c * c_w + own_q * quart, quart), quart)
        a_f[:, cols] = (silu * up).astype(BF)
        fb[own_q, c, 0] = (up * sig * (1.0 + gate * (1.0 - sig))).astype(BF)
        fb[own_q, c, 1] = silu.astype(BF)

    def down_dot(c):
        @pl.when(c == 0)
        def _():
            wd_load.wait()

        rows = pl.ds(pl.multiple_of(c * c_w, c_w), c_w)

        @pl.when(c < nc - 1)
        def _():
            acc[...] += nn_dot(a_f[:, rows], wd[rows, :])

        @pl.when(c == nc - 1)
        def _():
            for j in range(YB):
                acc[:, y_cols(j)] += nn_dot(a_f[:, rows], wd[rows, y_cols(j)])
                y_send(1, j)


    pipeline(0, gu_partial, act_forward, down_dot)
    wait_sends(0)
    f_copy(4).start()
    a_out = load(a_f, a_o, ld.at[1])
    a_out.start()

    small[3].wait()
    small[4].wait()
    y_copy(0).wait()
    acc[...] = y32[0] + y32[1]
    sq_two = jnp.zeros((tok, 1), F32)
    dot_two = jnp.zeros((tok, 1), F32)
    for j in range(YB):
        cols = y_cols(j)
        x2_b = (x_s[:, cols].astype(F32) + y_sum(1, j)).astype(BF)
        x2_s[:, cols] = x2_b
        x2 = x2_b.astype(F32)
        sq_two += jnp.sum(x2 * x2, axis=-1, keepdims=True)
        dot_two += jnp.sum(g2[:, cols] * acc[:, cols] * x2, axis=-1, keepdims=True)
    stat_send(1, [sq_two, dot_two])
    f_copy(1).start()
    acc[...] = g2[...] * acc[...]
    with jax.named_scope("stat1"):
        sq2, dot2 = stat_recv(1, 2)
    inv2 = lax.rsqrt(sq2 / d_model + NORM_EPS)
    x2 = x2_s[...].astype(F32)
    dz2 = inv2 * acc[...] - x2 * (inv2 * inv2 * inv2) * (dot2 / d_model)
    e_val = dx_s[...].astype(F32) + dz2
    e_s[...] = e_val
    eb[...] = e_val.astype(BF)
    eb_out = load(eb, eb_o, ld.at[2])
    eb_out.start()
    acc[...] = jnp.zeros_like(acc)

    def da_partial(c):
        slot = lax.rem(c, 2)
        prod = nt_dot(eb[...], wd[pl.ds(pl.multiple_of(c * c_w, c_w), c_w), :])
        part[slot, 0, 0] = prod[:, :half]
        part[slot, 1, 0] = prod[:, half:]

    def act_backward(c):
        cols = pl.ds(pl.multiple_of(c * c_w + own_q * quart, quart), quart)
        da_f[:, cols] = (r2[c, :, own_cols] + xr2[c].astype(F32)).astype(BF)

    def dn1_dot(c):
        @pl.when(c == 0)
        def _():
            f_copy(4).wait_recv()
            f_copy(2).wait_recv()

        @pl.when(c == nc - LATE)
        def _():
            f_copy(3).wait_recv()

        for q in range(4):
            cols = pl.ds(pl.multiple_of(c * c_w + q * quart, quart), quart)
            d_act = da_f[:, cols].astype(F32)
            for i in range(2):
                dst = pl.ds(pl.multiple_of((2 * c + i) * c_w + q * quart, quart), quart)
                dgu_f[:, dst] = (d_act * fb[q, c, i].astype(F32)).astype(BF)
        cols = pl.ds(pl.multiple_of(2 * c * c_w, 2 * c_w), 2 * c_w)

        @pl.when(c < nc - 1)
        def _():
            acc[...] += nt_dot(dgu_f[:, cols], wgu[:, cols])

        @pl.when(c == nc - 1)
        def _():
            for j in range(YB):
                acc[:, y_cols(j)] += nt_dot(dgu_f[:, cols], wgu[y_cols(j), cols])
                y_send(2, j)

    pipeline(1, da_partial, act_backward, dn1_dot)
    dgu_out = load(dgu_f, dgu_o, ld.at[4])

    stat_send(2, [jnp.sum(g1[...] * acc[...] * x_s[...].astype(F32), axis=-1, keepdims=True)], PEERS)
    dgu_out.start()
    wait_sends(1)
    xr2_f = x2_s[...].astype(F32) * inv2
    n2[...] = (xr2_f * g2[...]).astype(BF)
    dg_s[0:1, :] = jnp.sum((y32[0] + y32[1]) * xr2_f, axis=0, keepdims=True)
    n2_out = load(n2, n2_o, ld.at[3])
    n2_out.start()
    sent = fb.at[pl.ds(0, 3)]
    pltpu.make_async_remote_copy(
        src_ref=sent, dst_ref=sent, send_sem=f_sem.at[5], recv_sem=f_sem.at[0], device_id=pair, device_id_type=MESH_ID
    ).wait_send()
    for j in range(YB):
        acc[:, y_cols(j)] = y_sum(2, j)
    y_wait_send(1)
    y_wait_send(2)
    dg_s[1:2, :] = jnp.sum(acc[...] * x_s[...].astype(F32) * inv1, axis=0, keepdims=True)
    with jax.named_scope("stat2"):
        (dot1,) = stat_recv(2, 1, PEERS)
    dz1 = inv1 * (g1[...] * acc[...]) - x_s[...].astype(F32) * (inv1 * inv1 * inv1) * (dot1 / d_model)
    dxin_s[...] = (e_s[...] + dz1).astype(BF)
    tail = [
        load(dxin_s, dxin_o, ld.at[5]),
        load(dg_s, dg_o, qld.at[0]),
    ]
    for cp in tail:
        cp.start()
    for cp in (n1_out, a_out, eb_out, n2_out, dgu_out, *tail):
        cp.wait()


def comm_call(x_in, gain_one, gain_two, w_gate, w_up, w_down, w_qkv, dx_out, d_qkv):
    tok, hd = x_in.shape
    ff = w_gate.shape[1]
    qw = w_qkv.shape[1]
    nc = ff // CHUNK
    half, quart = CHUNK // 2, CHUNK // 4
    out = lambda shape, dtype: jax.ShapeDtypeStruct(shape, dtype)
    vm = lambda *shape_dtype: pltpu.VMEM(shape_dtype[:-1], shape_dtype[-1])
    dma = pltpu.SemaphoreType.DMA
    return pl.pallas_call(
        functools.partial(comm_kernel, (tok, hd, ff, qw)),
        out_shape=(
            out((tok, hd), BF), out((tok, hd), BF), out((tok, hd), BF), out((tok, ff), BF), out((tok, 2 * ff), BF),
            out((tok, hd), BF), out((8, hd), F32),
        ),
        in_specs=[ANY] * 9,
        out_specs=[ANY] * 7,
        scratch_shapes=[
            vm(hd, 2 * ff, BF), vm(ff, hd, BF), vm(hd, qw, BF), vm(tok, qw, BF),
            vm(tok, hd, BF), vm(tok, hd, BF), vm(1, hd, F32), vm(1, hd, F32),
            vm(tok, hd, BF), vm(tok, hd, BF), vm(tok, hd, BF), vm(tok, hd, F32), vm(tok, hd, BF),
            vm(tok, hd, F32), vm(2, 2, 2, tok, half, F32), vm(nc, 2, tok, half, F32), vm(nc, tok, half, F32),
            vm(nc, 2, tok, quart, BF), vm(nc, 2, tok, quart, BF), vm(nc, tok, quart, BF), vm(nc, tok, quart, BF),
            vm(nc, 2, tok, quart, F32), vm(4, nc, 2, tok, quart, BF), vm(tok, ff, BF), vm(tok, ff, BF), vm(tok, 2 * ff, BF),
            vm(2, tok, hd, F32), vm(2, tok, hd, BF), vm(2, tok, hd, BF), vm(3, 8, 128, F32), vm(3, 8, 8, 128, F32),
            vm(tok, hd, BF), vm(8, hd, F32),
            dma((6,)), dma((nc,)), dma((1,)), dma((3, 2)), dma((3, YB + 1)), dma((5, nc)), dma((6,)), dma((6,)),
        ],
        compiler_params=pltpu.CompilerParams(
            collective_id=0, has_side_effects=True, vmem_limit_bytes=VMEM_LIMIT
        ),
        name="block_comm",
    )(x_in, gain_one, gain_two, w_gate, w_up, w_down, w_qkv, dx_out, d_qkv)


TILE = CHUNK
SLOTS = 3


def grad_kernel(
    dims, n1_h, n2_h, eb_h, a_h, dgu_h, dq_h, dx_h, dg_h,
    dwg_o, dwu_o, dwd_o, dwq_o, dx_o, dg1_o, dg2_o,
    n1, n2, eb, a_f, dgu, dq, dx, dg, n1_t, n2_t, bq, bg, bu, bd, ld, sem,
):
    hd, ff, qw = dims
    nt, nq = ff // TILE, qw // TILE
    pairs = ((n2_h, n2), (dq_h, dq), (eb_h, eb), (a_h, a_f), (n1_h, n1), (dgu_h, dgu), (dx_h, dx), (dg_h, dg))
    loads = [pltpu.make_async_copy(src, dst, ld.at[i]) for i, (src, dst) in enumerate(pairs)]
    for cp in loads:
        cp.start()

    def cols_of(i):
        return pl.ds(pl.multiple_of(i * TILE, TILE), TILE)

    def out_copy(kind, i):
        slot = lax.rem(i, SLOTS)
        src = (bq, bg, bu, bd)[kind].at[slot]
        dst = (dwq_o, dwg_o, dwu_o, dwd_o)[kind]
        return pltpu.make_async_copy(src, dst.at[cols_of(i), :] if kind == 3 else dst.at[:, cols_of(i)], sem.at[kind, slot])

    with jax.named_scope("b_in0"):
      loads[0].wait()
      loads[1].wait()
    with jax.named_scope("b_t"):
      n2_t[...] = n2[...].T

    def q_step(i, carry):
        @pl.when(i >= SLOTS)
        def _():
            out_copy(0, i - SLOTS).wait()

        bq[lax.rem(i, SLOTS)] = nn_dot(n2_t[...], dq[:, cols_of(i)]).astype(BF)
        out_copy(0, i).start()
        return carry

    with jax.named_scope("b_q"):
      lax.fori_loop(0, nq, q_step, 0)
    with jax.named_scope("b_in1"):
      for cp in loads[2:]:
        cp.wait()
    finals = [
        pltpu.make_async_copy(dx, dx_o, ld.at[0]),
        pltpu.make_async_copy(dg.at[0:1, :], dg2_o, ld.at[1]),
        pltpu.make_async_copy(dg.at[1:2, :], dg1_o, ld.at[2]),
    ]
    for cp in finals:
        cp.start()
    n1_t[...] = n1[...].T

    def step(i, carry):
        slot = lax.rem(i, SLOTS)

        @pl.when(i >= SLOTS)
        def _():
            for kind in (1, 2, 3):
                out_copy(kind, i - SLOTS).wait()

        bd[slot] = nn_dot(a_f[:, cols_of(i)].T, eb[...]).astype(BF)
        out_copy(3, i).start()
        bg[slot] = nn_dot(n1_t[...], dgu[:, cols_of(2 * i)]).astype(BF)
        out_copy(1, i).start()
        bu[slot] = nn_dot(n1_t[...], dgu[:, cols_of(2 * i + 1)]).astype(BF)
        out_copy(2, i).start()
        return carry

    lax.fori_loop(0, nt, step, 0)
    for cp in finals:
        cp.wait()
    for i in range(max(nq - SLOTS, 0), nq):
        out_copy(0, i).wait()
    for i in range(nt - SLOTS, nt):
        for kind in (1, 2, 3):
            out_copy(kind, i).wait()


def grad_call(n1, n2, eb, a_full, dgu, d_qkv, dx_in, dg):
    tok, hd = n1.shape
    ff, qw = a_full.shape[1], d_qkv.shape[1]
    out = lambda *shape: jax.ShapeDtypeStruct(shape, BF)
    vm = lambda *shape: pltpu.VMEM(shape, BF)
    return pl.pallas_call(
        functools.partial(grad_kernel, (hd, ff, qw)),
        out_shape=(
            out(hd, ff), out(hd, ff), out(ff, hd), out(hd, qw),
            out(tok, hd), jax.ShapeDtypeStruct((1, hd), F32), jax.ShapeDtypeStruct((1, hd), F32),
        ),
        in_specs=[ANY] * 8,
        out_specs=[ANY] * 7,
        scratch_shapes=[
            vm(tok, hd), vm(tok, hd), vm(tok, hd), vm(tok, ff), vm(tok, 2 * ff), vm(tok, qw), vm(tok, hd), pltpu.VMEM((8, hd), F32), vm(hd, tok), vm(hd, tok),
            vm(SLOTS, hd, TILE), vm(SLOTS, hd, TILE), vm(SLOTS, hd, TILE), vm(SLOTS, TILE, hd),
            pltpu.SemaphoreType.DMA((8,)), pltpu.SemaphoreType.DMA((4, SLOTS)),
        ],
        compiler_params=pltpu.CompilerParams(vmem_limit_bytes=VMEM_LIMIT),
        name="weight_grads",
    )(n1, n2, eb, a_full, dgu, d_qkv, dx_in, dg)


def solution(mesh):
    def local_step(x_in, gain_one, gain_two, w_gate, w_up, w_down, w_qkv, dx_out, d_qkv):
        hd = x_in.shape[1]
        n1, n2, eb, a_full, dgu, dx_in, dg = comm_call(
            x_in, gain_one.reshape(1, hd), gain_two.reshape(1, hd), w_gate, w_up, w_down, w_qkv, dx_out, d_qkv
        )
        dw_gate, dw_up, dw_down, dw_qkv, dx_in, dg1, dg2 = grad_call(
            n1, n2, eb, a_full, dgu, d_qkv, dx_in, dg
        )
        return dx_in, dw_gate, dw_up, dw_down, dw_qkv, dg1.reshape(hd), dg2.reshape(hd)

    tok_spec = P("data", "hid")
    in_specs = (tok_spec, P("hid"), P("hid"), P("hid", "ffn"), P("hid", "ffn"), P("ffn", "hid"), P("hid", "ffn"), tok_spec, P("data", "ffn"))
    out_specs = (tok_spec, P(("data", "hid"), "ffn"), P(("data", "hid"), "ffn"), P(("data", "ffn"), "hid"), P(("data", "hid"), "ffn"), P(("data", "hid")), P(("data", "hid")))
    return jax.shard_map(local_step, mesh=mesh, in_specs=in_specs, out_specs=out_specs, check_vma=False)
```

```python
import functools

import jax
import jax.numpy as jnp
from jax import lax
from jax.experimental import pallas as pl
from jax.experimental.pallas import tpu as pltpu
from jax.sharding import PartitionSpec as P

NORM_EPS = 1e-6
BF = jnp.bfloat16
F32 = jnp.float32
MESH_ID = pl.DeviceIdType.MESH
ANY = pl.BlockSpec(memory_space=pl.ANY)
VMEM_LIMIT = 67043328

CHUNK = 1024
LATE = 2
YB = 2
F_STEPS = (0, 3)
QKV_AT = 7
DIRECT_LAST = 1
DIRECT_FIRST = 0
LAGS = ((1, 5, 9, 10), (1, 3, 5, 6))

PAIR, XRED, GX, GP, FW, DG = range(6)

PEERS = tuple((dy, j) for dy in range(2) for j in range(4) if dy or j)
ROW_PEERS = PEERS[:3]


def nn_dot(a_mat, b_mat):
    return jnp.dot(a_mat, b_mat, preferred_element_type=F32)


def nt_dot(a_mat, b_mat):
    return lax.dot_general(a_mat, b_mat, (((1,), (1,)), ((), ())), preferred_element_type=F32)


def pack_stats(cols):
    tok = cols[0].shape[0]
    lane = lax.broadcasted_iota(jnp.int32, (tok, 128), 1)
    wide = jnp.zeros((tok, 128), F32)
    for i, col in enumerate(cols):
        wide = jnp.where(lane == i, col, wide)
    full = jnp.concatenate([wide, jnp.zeros((128 - tok, 128), F32)], axis=0)
    return full.T[0:8, :]


def unpack_stats(tile, tok, count):
    full = jnp.concatenate([tile, jnp.zeros((120, 128), F32)], axis=0).T
    return [full[0:tok, i : i + 1] for i in range(count)]


def comm_kernel(
    dims,
    x_h, g1_h, g2_h, wg_h, wu_h, wd_h, wq_h, dx_h, dq_h,
    n1_o, n2_o, eb_o, a_o, dgu_o, dxin_o, dg_o,
    wgu, wd, wq, dq, x_s, dx_s, g1, g2, n1, n2, eb, e_s, x2_s,
    acc, part, r1, r2, xs, xr, xs2, xr2, gu, fb, a_f, da_f, dgu_f, y32, ys, yr, st_s, st_r, dxin_s, dg_s,
    ld, wld, qld, st_sem, y_sem, recvs, sends, f_sem,
):
    tok, hd, ff, qw = dims
    c_w = CHUNK
    nc = ff // c_w
    half = c_w // 2
    quart = c_w // 4
    d_model = hd * 4
    zc, yc, h = lax.axis_index("data"), lax.axis_index("ffn"), lax.axis_index("hid")
    xc = h // 2
    core = lax.rem(h, 2)
    pair = (zc, yc, xc * 2 + 1 - core)
    xnb = (zc, yc, (1 - xc) * 2 + core)
    diag = (zc, yc, 3 - h)
    ynb = (zc, 1 - yc, h)

    def peer(dy, j):
        return (zc, lax.rem(yc + dy, 2), lax.rem(h + j, 4))


    def load(src, dst, sem):
        return pltpu.make_async_copy(src, dst, sem)

    small = [
        load(x_h, x_s, ld.at[0]), load(g1_h, g1, ld.at[1]), load(dq_h, dq, ld.at[2]),
        load(g2_h, g2, ld.at[3]), load(dx_h, dx_s, ld.at[4]),
    ]
    qn = qw // 1024

    wq_load = load(wq_h, wq, qld.at[0])

    def gu_load(i, c):
        src = (wg_h, wu_h)[i].at[:, pl.ds(pl.multiple_of(c * c_w, c_w), c_w)]
        dst = wgu.at[:, pl.ds(pl.multiple_of((2 * c + i) * c_w, c_w), c_w)]
        return load(src, dst, wld.at[c])

    def gu_wait(c):
        both = wgu.at[:, pl.ds(pl.multiple_of(2 * c * c_w, 2 * c_w), 2 * c_w)]
        load(wg_h.at[:, pl.ds(0, 2 * c_w)], both, wld.at[c]).wait()

    wd_load = load(wd_h, wd, ld.at[5])

    def gu_load_start(n):
        gu_load(0, n).start()
        gu_load(1, n).start()

    for cp in small:
        cp.start()

    bar = pltpu.get_barrier_semaphore()
    for dy, j in PEERS[:4]:
        pl.semaphore_signal(bar, inc=1, device_id=peer(dy, j), device_id_type=MESH_ID)
    small[0].wait()
    gu_load_start(0)
    gu_load_start(1)
    x_f = x_s[...].astype(F32)
    sq_part = jnp.sum(x_f * x_f, axis=-1, keepdims=True)

    def qkv_step(i):
        @pl.when(i == 0)
        def _():
            wq_load.wait()

        cols = pl.ds(pl.multiple_of(i * 1024, 1024), 1024)
        y32[0] += nt_dot(dq[:, cols], wq[:, cols])

    y32[0] = jnp.zeros((tok, hd), F32)
    with jax.named_scope("barrier"):
        pl.semaphore_wait(bar, 4)

    def stat_copy(n, i):
        return pltpu.make_async_remote_copy(
            src_ref=st_s.at[n], dst_ref=st_r.at[n, yc * 4 + h], send_sem=st_sem.at[n, 0], recv_sem=st_sem.at[n, 1],
            device_id=peer(*PEERS[i]), device_id_type=MESH_ID,
        )

    def stat_send(n, cols, peers=ROW_PEERS):
        tile = pack_stats(cols)
        st_s[n] = tile
        st_r[n, yc * 4 + h] = tile
        for i in range(len(peers)):
            stat_copy(n, i).start()

    def stat_recv(n, count, peers=ROW_PEERS):
        all_tiles = st_r.at[n, pl.ds(0, len(peers))]
        whole = pltpu.make_async_remote_copy(
            src_ref=all_tiles, dst_ref=all_tiles, send_sem=st_sem.at[n, 0], recv_sem=st_sem.at[n, 1],
            device_id=peer(*PEERS[0]), device_id_type=MESH_ID,
        )
        whole.wait()
        total = jnp.zeros((8, 128), F32)
        for i in range(len(peers) + 1):
            total += st_r[n, i] if peers is PEERS else st_r[n, yc * 4 + i]
        return unpack_stats(total, tok, count)

    yb = hd // YB

    def y_cols(j):
        return pl.ds(j * yb, yb)

    def y_copy(n, j=0):
        if n == 0:
            src, dst = y32.at[0], y32.at[1]
        else:
            src, dst = ys.at[n - 1, :, y_cols(j)], yr.at[n - 1, :, y_cols(j)]
        return pltpu.make_async_remote_copy(
            src_ref=src, dst_ref=dst, send_sem=y_sem.at[n, YB], recv_sem=y_sem.at[n, j],
            device_id=ynb, device_id_type=MESH_ID,
        )

    def y_send(n, j):
        ys[n - 1, :, y_cols(j)] = acc[:, y_cols(j)].astype(BF)
        y_copy(n, j).start()

    def y_sum(n, j):
        with jax.named_scope(f"ywait{n}"):
            y_copy(n, j).wait_recv()
        return ys[n - 1, :, y_cols(j)].astype(F32) + yr[n - 1, :, y_cols(j)].astype(F32)

    def y_wait_send(n):
        whole = ys.at[n - 1]
        pltpu.make_async_remote_copy(
            src_ref=whole, dst_ref=whole, send_sem=y_sem.at[n, YB], recv_sem=y_sem.at[n, 0],
            device_id=ynb, device_id_type=MESH_ID,
        ).wait_send()

    stat_send(0, [sq_part])
    gu_load_start(2)
    gu_load_start(3)
    small[2].wait()
    small[1].wait()
    with jax.named_scope("stat0"):
        (sq,) = stat_recv(0, 1)
    gu_load_start(4)
    gu_load_start(5)
    inv1 = lax.rsqrt(sq / d_model + NORM_EPS)
    n1[...] = (x_s[...].astype(F32) * inv1 * g1[...]).astype(BF)
    n1_out = load(n1, n1_o, ld.at[0])
    n1_out.start()
    acc[...] = jnp.zeros_like(acc)

    def pair_copy(ph, c):
        slot = lax.rem(c, 2)
        src = part.at[slot, 1 - core] if ph == 0 else part.at[slot, 1 - core, 0]
        return pltpu.make_async_remote_copy(
            src_ref=src, dst_ref=(r1 if ph == 0 else r2).at[c],
            send_sem=sends.at[4 + slot], recv_sem=recvs.at[PAIR, c],
            device_id=pair, device_id_type=MESH_ID,
        )

    def x_copy(ph, c):
        src, dst = ((xs, xr), (xs2, xr2))[ph]
        return pltpu.make_async_remote_copy(
            src_ref=src.at[c], dst_ref=dst.at[c],
            send_sem=sends.at[0], recv_sem=recvs.at[XRED, c],
            device_id=xnb, device_id_type=MESH_ID,
        )

    own_q = core * 2 + xc
    xnb_q = core * 2 + 1 - xc

    def block(ph, c, q):
        cols = pl.ds(pl.multiple_of(c * c_w + q * quart, quart), quart)
        return (a_f if ph == 0 else da_f).at[:, cols]

    def g_copy(ph, c, kind):
        ref = block(ph, c, xnb_q if kind == FW else own_q)
        target = {GX: xnb, GP: pair, FW: pair, DG: diag}[kind]
        kind = FW if kind == DG else kind
        return pltpu.make_async_remote_copy(
            src_ref=ref, dst_ref=ref, send_sem=sends.at[kind - 1], recv_sem=recvs.at[kind, c],
            device_id=target, device_id_type=MESH_ID,
        )

    def wait_sends(ph):
        src = xs if ph == 0 else xs2
        pltpu.make_async_remote_copy(
            src_ref=src, dst_ref=src, send_sem=sends.at[0], recv_sem=recvs.at[XRED, 0],
            device_id=xnb, device_id_type=MESH_ID,
        ).wait_send()
        whole = (a_f if ph == 0 else da_f).at[:, pl.ds(0, ff // 4)]
        for kind in (GX, GP, FW):
            pltpu.make_async_remote_copy(
                src_ref=whole, dst_ref=whole, send_sem=sends.at[kind - 1], recv_sem=recvs.at[kind, 0],
                device_id=xnb, device_id_type=MESH_ID,
            ).wait_send()
        for c in (nc - 2, nc - 1):
            pair_copy(ph, c).wait_send()

    f_parts = ((0, nc - LATE), (nc - LATE, LATE))

    def f_copy(n):
        first, count = f_parts[n % 2] if n < 4 else (0, nc)
        ref = fb.at[xnb_q if n in (2, 3) else own_q, pl.ds(first, count)]
        return pltpu.make_async_remote_copy(
            src_ref=ref, dst_ref=ref, send_sem=f_sem.at[5], recv_sem=f_sem.at[n],
            device_id=xnb if n < 2 else pair, device_id_type=MESH_ID,
        )

    own_cols = pl.ds(pl.multiple_of(xc * quart, quart), quart)
    oth_cols = pl.ds(pl.multiple_of((1 - xc) * quart, quart), quart)

    def pipeline(ph, partial, activate, consume):
        lag_pair, lag_act, lag_fwd, lag_dot = LAGS[ph]

        def direct(c):
            return c >= nc - DIRECT_LAST if ph == 0 else c < DIRECT_FIRST

        def reduce_pair(c):
            slot = lax.rem(c, 2)
            with jax.named_scope(f"pairwait{ph}"):
                pair_copy(ph, c).wait_recv()
            if ph == 0:
                xs[c] = (part[slot, core, :, :, oth_cols] + r1[c, :, :, oth_cols]).astype(BF)
                x_copy(ph, c).start()
                gu[c] = part[slot, core, :, :, own_cols] + r1[c, :, :, own_cols]
            else:
                xs2[c] = (part[slot, core, 0, :, oth_cols] + r2[c, :, oth_cols]).astype(BF)
                x_copy(ph, c).start()
                r2[c, :, own_cols] = part[slot, core, 0, :, own_cols] + r2[c, :, own_cols]

        def step(t, carry):
            if ph == 1:
                for n, when in enumerate(F_STEPS):

                    @pl.when(t == when)
                    def _():
                        f_copy(n).wait_recv()
                        f_copy(2 + n).start()

            if ph == 0:

                @pl.when(t == 0)
                def _():
                    for c in range(6, nc):
                        gu_load_start(c)

                @pl.when(t == 1)
                def _():
                    wq_load.start()

                @pl.when(t == 2)
                def _():
                    wd_load.start()

                @pl.when((t >= QKV_AT) & (t < QKV_AT + qn))
                def _():
                    with jax.named_scope("qkv"):
                        qkv_step(t - QKV_AT)

                @pl.when(t == QKV_AT + qn - 1)
                def _():
                    y_copy(0).start()

            @pl.when(t < nc)
            def _():
                c = t

                @pl.when(c >= 2)
                def _():
                    pair_copy(ph, c - 2).wait_send()

                with jax.named_scope(f"part{ph}"):

                    partial(c)
                    pair_copy(ph, c).start()

            @pl.when((t >= lag_pair) & (t < nc + lag_pair))
            def _():
                reduce_pair(t - lag_pair)

            @pl.when((t >= lag_act) & (t < nc + lag_act))
            def _():
                c = t - lag_act
                with jax.named_scope(f"xwait{ph}"):
                    x_copy(ph, c).wait_recv()
                with jax.named_scope(f"act{ph}"):
                    activate(c)
                g_copy(ph, c, GP).start()
                g_copy(ph, c, GX).start()

                @pl.when(direct(c))
                def _():
                    g_copy(ph, c, DG).start()

                if ph == 0:

                    @pl.when(c == nc - 1)
                    def _():
                        f_copy(0).start()

            @pl.when((t >= lag_fwd) & (t < nc + lag_fwd))
            def _():
                c = t - lag_fwd
                with jax.named_scope(f"gxwait{ph}"):
                    g_copy(ph, c, GX).wait_recv()

                @pl.when(jnp.logical_not(direct(c)))
                def _():
                    g_copy(ph, c, FW).start()

            @pl.when((t >= lag_dot) & (t < nc + lag_dot))
            def _():
                c = t - lag_dot
                with jax.named_scope(f"gpwait{ph}"):
                    g_copy(ph, c, GP).wait_recv()
                    g_copy(ph, c, FW).wait_recv()
                with jax.named_scope(f"dot{ph}"):
                    consume(c)

            return carry

        lax.fori_loop(0, nc + lag_dot, step, 0)

    def gu_partial(c):
        gu_wait(c)
        slot = lax.rem(c, 2)
        prod = nn_dot(n1[...], wgu[:, pl.ds(pl.multiple_of(2 * c * c_w, 2 * c_w), 2 * c_w)])
        for i in range(2):
            part[slot, 0, i] = prod[:, i * c_w : i * c_w + half]
            part[slot, 1, i] = prod[:, i * c_w + half : (i + 1) * c_w]

    def act_forward(c):
        gate = gu[c, 0] + xr[c, 0].astype(F32)
        up = gu[c, 1] + xr[c, 1].astype(F32)
        sig = jax.nn.sigmoid(gate)
        silu = gate * sig
        cols = pl.ds(pl.multiple_of(c * c_w + own_q * quart, quart), quart)
        a_f[:, cols] = (silu * up).astype(BF)
        fb[own_q, c, 0] = (up * sig * (1.0 + gate * (1.0 - sig))).astype(BF)
        fb[own_q, c, 1] = silu.astype(BF)

    def down_dot(c):
        @pl.when(c == 0)
        def _():
            wd_load.wait()

        rows = pl.ds(pl.multiple_of(c * c_w, c_w), c_w)

        @pl.when(c < nc - 1)
        def _():
            acc[...] += nn_dot(a_f[:, rows], wd[rows, :])

        @pl.when(c == nc - 1)
        def _():
            for j in range(YB):
                acc[:, y_cols(j)] += nn_dot(a_f[:, rows], wd[rows, y_cols(j)])
                y_send(1, j)


    pipeline(0, gu_partial, act_forward, down_dot)
    wait_sends(0)
    f_copy(4).start()
    a_out = load(a_f, a_o, ld.at[1])
    a_out.start()

    small[3].wait()
    small[4].wait()
    y_copy(0).wait()
    acc[...] = y32[0] + y32[1]
    sq_two = jnp.zeros((tok, 1), F32)
    dot_two = jnp.zeros((tok, 1), F32)
    for j in range(YB):
        cols = y_cols(j)
        x2_b = (x_s[:, cols].astype(F32) + y_sum(1, j)).astype(BF)
        x2_s[:, cols] = x2_b
        x2 = x2_b.astype(F32)
        sq_two += jnp.sum(x2 * x2, axis=-1, keepdims=True)
        dot_two += jnp.sum(g2[:, cols] * acc[:, cols] * x2, axis=-1, keepdims=True)
    stat_send(1, [sq_two, dot_two])
    f_copy(1).start()
    acc[...] = g2[...] * acc[...]
    with jax.named_scope("stat1"):
        sq2, dot2 = stat_recv(1, 2)
    inv2 = lax.rsqrt(sq2 / d_model + NORM_EPS)
    x2 = x2_s[...].astype(F32)
    dz2 = inv2 * acc[...] - x2 * (inv2 * inv2 * inv2) * (dot2 / d_model)
    e_val = dx_s[...].astype(F32) + dz2
    e_s[...] = e_val
    eb[...] = e_val.astype(BF)
    eb_out = load(eb, eb_o, ld.at[2])
    eb_out.start()
    acc[...] = jnp.zeros_like(acc)

    def da_partial(c):
        slot = lax.rem(c, 2)
        prod = nt_dot(eb[...], wd[pl.ds(pl.multiple_of(c * c_w, c_w), c_w), :])
        part[slot, 0, 0] = prod[:, :half]
        part[slot, 1, 0] = prod[:, half:]

    def act_backward(c):
        cols = pl.ds(pl.multiple_of(c * c_w + own_q * quart, quart), quart)
        da_f[:, cols] = (r2[c, :, own_cols] + xr2[c].astype(F32)).astype(BF)

    def dn1_dot(c):
        @pl.when(c == 0)
        def _():
            f_copy(4).wait_recv()
            f_copy(2).wait_recv()

        @pl.when(c == nc - LATE)
        def _():
            f_copy(3).wait_recv()

        for q in range(4):
            cols = pl.ds(pl.multiple_of(c * c_w + q * quart, quart), quart)
            d_act = da_f[:, cols].astype(F32)
            for i in range(2):
                dst = pl.ds(pl.multiple_of((2 * c + i) * c_w + q * quart, quart), quart)
                dgu_f[:, dst] = (d_act * fb[q, c, i].astype(F32)).astype(BF)
        cols = pl.ds(pl.multiple_of(2 * c * c_w, 2 * c_w), 2 * c_w)

        @pl.when(c < nc - 1)
        def _():
            acc[...] += nt_dot(dgu_f[:, cols], wgu[:, cols])

        @pl.when(c == nc - 1)
        def _():
            for j in range(YB):
                acc[:, y_cols(j)] += nt_dot(dgu_f[:, cols], wgu[y_cols(j), cols])
                y_send(2, j)

    pipeline(1, da_partial, act_backward, dn1_dot)
    dgu_out = load(dgu_f, dgu_o, ld.at[4])

    stat_send(2, [jnp.sum(g1[...] * acc[...] * x_s[...].astype(F32), axis=-1, keepdims=True)], PEERS)
    dgu_out.start()
    wait_sends(1)
    xr2_f = x2_s[...].astype(F32) * inv2
    n2[...] = (xr2_f * g2[...]).astype(BF)
    dg_s[0:1, :] = jnp.sum((y32[0] + y32[1]) * xr2_f, axis=0, keepdims=True)
    n2_out = load(n2, n2_o, ld.at[3])
    n2_out.start()
    y32[0] = x_s[...].astype(F32) * (inv1 * inv1 * inv1)
    y32[1] = inv1 * g1[...]
    sent = fb.at[pl.ds(0, 3)]
    pltpu.make_async_remote_copy(
        src_ref=sent, dst_ref=sent, send_sem=f_sem.at[5], recv_sem=f_sem.at[0], device_id=pair, device_id_type=MESH_ID
    ).wait_send()
    for j in range(YB):
        acc[:, y_cols(j)] = y_sum(2, j)
    y_wait_send(1)
    y_wait_send(2)
    dg_s[1:2, :] = jnp.sum(acc[...] * x_s[...].astype(F32) * inv1, axis=0, keepdims=True)
    with jax.named_scope("stat2"):
        (dot1,) = stat_recv(2, 1, PEERS)
    dz1 = y32[1] * acc[...] - y32[0] * (dot1 / d_model)
    dxin_s[...] = (e_s[...] + dz1).astype(BF)
    tail = [
        load(dxin_s, dxin_o, ld.at[5]),
        load(dg_s, dg_o, qld.at[0]),
    ]
    for cp in tail:
        cp.start()
    for cp in (n1_out, a_out, eb_out, n2_out, dgu_out, *tail):
        cp.wait()


def comm_call(x_in, gain_one, gain_two, w_gate, w_up, w_down, w_qkv, dx_out, d_qkv):
    tok, hd = x_in.shape
    ff = w_gate.shape[1]
    qw = w_qkv.shape[1]
    nc = ff // CHUNK
    half, quart = CHUNK // 2, CHUNK // 4
    out = lambda shape, dtype: jax.ShapeDtypeStruct(shape, dtype)
    vm = lambda *shape_dtype: pltpu.VMEM(shape_dtype[:-1], shape_dtype[-1])
    dma = pltpu.SemaphoreType.DMA
    return pl.pallas_call(
        functools.partial(comm_kernel, (tok, hd, ff, qw)),
        out_shape=(
            out((tok, hd), BF), out((tok, hd), BF), out((tok, hd), BF), out((tok, ff), BF), out((tok, 2 * ff), BF),
            out((tok, hd), BF), out((8, hd), F32),
        ),
        in_specs=[ANY] * 9,
        out_specs=[ANY] * 7,
        scratch_shapes=[
            vm(hd, 2 * ff, BF), vm(ff, hd, BF), vm(hd, qw, BF), vm(tok, qw, BF),
            vm(tok, hd, BF), vm(tok, hd, BF), vm(1, hd, F32), vm(1, hd, F32),
            vm(tok, hd, BF), vm(tok, hd, BF), vm(tok, hd, BF), vm(tok, hd, F32), vm(tok, hd, BF),
            vm(tok, hd, F32), vm(2, 2, 2, tok, half, F32), vm(nc, 2, tok, half, F32), vm(nc, tok, half, F32),
            vm(nc, 2, tok, quart, BF), vm(nc, 2, tok, quart, BF), vm(nc, tok, quart, BF), vm(nc, tok, quart, BF),
            vm(nc, 2, tok, quart, F32), vm(4, nc, 2, tok, quart, BF), vm(tok, ff, BF), vm(tok, ff, BF), vm(tok, 2 * ff, BF),
            vm(2, tok, hd, F32), vm(2, tok, hd, BF), vm(2, tok, hd, BF), vm(3, 8, 128, F32), vm(3, 8, 8, 128, F32),
            vm(tok, hd, BF), vm(8, hd, F32),
            dma((6,)), dma((nc,)), dma((1,)), dma((3, 2)), dma((3, YB + 1)), dma((5, nc)), dma((6,)), dma((6,)),
        ],
        compiler_params=pltpu.CompilerParams(
            collective_id=0, has_side_effects=True, vmem_limit_bytes=VMEM_LIMIT
        ),
        name="block_comm",
    )(x_in, gain_one, gain_two, w_gate, w_up, w_down, w_qkv, dx_out, d_qkv)


TILE = CHUNK
SLOTS = 3


def grad_kernel(
    dims, n1_h, n2_h, eb_h, a_h, dgu_h, dq_h, dx_h, dg_h,
    dwg_o, dwu_o, dwd_o, dwq_o, dx_o, dg1_o, dg2_o,
    n1, n2, eb, a_f, dgu, dq, dx, dg, n1_t, n2_t, bq, bg, bu, bd, ld, sem,
):
    hd, ff, qw = dims
    nt, nq = ff // TILE, qw // TILE
    pairs = ((n2_h, n2), (dq_h, dq), (eb_h, eb), (a_h, a_f), (n1_h, n1), (dgu_h, dgu), (dx_h, dx), (dg_h, dg))
    loads = [pltpu.make_async_copy(src, dst, ld.at[i]) for i, (src, dst) in enumerate(pairs)]
    for cp in loads:
        cp.start()

    def cols_of(i):
        return pl.ds(pl.multiple_of(i * TILE, TILE), TILE)

    def out_copy(kind, i):
        slot = lax.rem(i, SLOTS)
        src = (bq, bg, bu, bd)[kind].at[slot]
        dst = (dwq_o, dwg_o, dwu_o, dwd_o)[kind]
        return pltpu.make_async_copy(src, dst.at[cols_of(i), :] if kind == 3 else dst.at[:, cols_of(i)], sem.at[kind, slot])

    with jax.named_scope("b_in0"):
      loads[0].wait()
      loads[1].wait()
    with jax.named_scope("b_t"):
      n2_t[...] = n2[...].T

    def q_step(i, carry):
        @pl.when(i >= SLOTS)
        def _():
            out_copy(0, i - SLOTS).wait()

        bq[lax.rem(i, SLOTS)] = nn_dot(n2_t[...], dq[:, cols_of(i)]).astype(BF)
        out_copy(0, i).start()
        return carry

    with jax.named_scope("b_q"):
      lax.fori_loop(0, nq, q_step, 0)
    with jax.named_scope("b_in1"):
      for cp in loads[2:]:
        cp.wait()
    finals = [
        pltpu.make_async_copy(dx, dx_o, ld.at[0]),
        pltpu.make_async_copy(dg.at[0:1, :], dg2_o, ld.at[1]),
        pltpu.make_async_copy(dg.at[1:2, :], dg1_o, ld.at[2]),
    ]
    for cp in finals:
        cp.start()
    n1_t[...] = n1[...].T

    def step(i, carry):
        slot = lax.rem(i, SLOTS)

        @pl.when(i >= SLOTS)
        def _():
            for kind in (1, 2, 3):
                out_copy(kind, i - SLOTS).wait()

        bd[slot] = nn_dot(a_f[:, cols_of(i)].T, eb[...]).astype(BF)
        out_copy(3, i).start()
        bg[slot] = nn_dot(n1_t[...], dgu[:, cols_of(2 * i)]).astype(BF)
        out_copy(1, i).start()
        bu[slot] = nn_dot(n1_t[...], dgu[:, cols_of(2 * i + 1)]).astype(BF)
        out_copy(2, i).start()
        return carry

    lax.fori_loop(0, nt, step, 0)
    for cp in finals:
        cp.wait()
    for i in range(max(nq - SLOTS, 0), nq):
        out_copy(0, i).wait()
    for i in range(nt - SLOTS, nt):
        for kind in (1, 2, 3):
            out_copy(kind, i).wait()


def grad_call(n1, n2, eb, a_full, dgu, d_qkv, dx_in, dg):
    tok, hd = n1.shape
    ff, qw = a_full.shape[1], d_qkv.shape[1]
    out = lambda *shape: jax.ShapeDtypeStruct(shape, BF)
    vm = lambda *shape: pltpu.VMEM(shape, BF)
    return pl.pallas_call(
        functools.partial(grad_kernel, (hd, ff, qw)),
        out_shape=(
            out(hd, ff), out(hd, ff), out(ff, hd), out(hd, qw),
            out(tok, hd), jax.ShapeDtypeStruct((1, hd), F32), jax.ShapeDtypeStruct((1, hd), F32),
        ),
        in_specs=[ANY] * 8,
        out_specs=[ANY] * 7,
        scratch_shapes=[
            vm(tok, hd), vm(tok, hd), vm(tok, hd), vm(tok, ff), vm(tok, 2 * ff), vm(tok, qw), vm(tok, hd), pltpu.VMEM((8, hd), F32), vm(hd, tok), vm(hd, tok),
            vm(SLOTS, hd, TILE), vm(SLOTS, hd, TILE), vm(SLOTS, hd, TILE), vm(SLOTS, TILE, hd),
            pltpu.SemaphoreType.DMA((8,)), pltpu.SemaphoreType.DMA((4, SLOTS)),
        ],
        compiler_params=pltpu.CompilerParams(vmem_limit_bytes=VMEM_LIMIT),
        name="weight_grads",
    )(n1, n2, eb, a_full, dgu, d_qkv, dx_in, dg)


def solution(mesh):
    def local_step(x_in, gain_one, gain_two, w_gate, w_up, w_down, w_qkv, dx_out, d_qkv):
        hd = x_in.shape[1]
        n1, n2, eb, a_full, dgu, dx_in, dg = comm_call(
            x_in, gain_one.reshape(1, hd), gain_two.reshape(1, hd), w_gate, w_up, w_down, w_qkv, dx_out, d_qkv
        )
        dw_gate, dw_up, dw_down, dw_qkv, dx_in, dg1, dg2 = grad_call(
            n1, n2, eb, a_full, dgu, d_qkv, dx_in, dg
        )
        return dx_in, dw_gate, dw_up, dw_down, dw_qkv, dg1.reshape(hd), dg2.reshape(hd)

    tok_spec = P("data", "hid")
    in_specs = (tok_spec, P("hid"), P("hid"), P("hid", "ffn"), P("hid", "ffn"), P("ffn", "hid"), P("hid", "ffn"), tok_spec, P("data", "ffn"))
    out_specs = (tok_spec, P(("data", "hid"), "ffn"), P(("data", "hid"), "ffn"), P(("data", "ffn"), "hid"), P(("data", "hid"), "ffn"), P(("data", "hid")), P(("data", "hid")))
    return jax.shard_map(local_step, mesh=mesh, in_specs=in_specs, out_specs=out_specs, check_vma=False)
```
